32 devices in a mesh: tile: 8 (over y, x, core), head: 4 (over z).
Axes of the slice: x: 2, y: 2, z: 4, core: 2. Of those that a mesh axis runs over, the one named last changes fastest.
Arguments:
- latent: bfloat16 [16, 512, 512], P('tile', 'head'), may hold values from -6 to 6
- norm1_gain: float32 [512], replicated, may hold values from 0.25 to 1.75
- norm1_shift: float32 [512], replicated, may hold values from -1.75 to 1.75
- conv1_weight: bfloat16 [3, 3, 512, 512], replicated, may hold values from -0.09375 to 0.09375
- conv1_bias: float32 [512], replicated, may hold values from -1.75 to 1.75
- norm2_gain: float32 [512], replicated, may hold values from 0.25 to 1.75
- norm2_shift: float32 [512], replicated, may hold values from -1.75 to 1.75
- conv2_weight: bfloat16 [3, 3, 512, 512], replicated, may hold values from -0.09375 to 0.09375
- conv2_bias: float32 [512], replicated, may hold values from -1.75 to 1.75
- norm3_gain: float32 [512], replicated, may hold values from 0.25 to 1.75
- norm3_shift: float32 [512], replicated, may hold values from -1.75 to 1.75
- query_weight: bfloat16 [512, 512], replicated, may hold values from -2 to 2
- query_bias: float32 [512], replicated, may hold values from -3 to 3
- key_weight: bfloat16 [512, 512], replicated, may hold values from -2 to 2
- value_weight: bfloat16 [512, 512], replicated, may hold values from -0.25 to 0.25
- value_bias: float32 [512], replicated, may hold values from -3 to 3
- out_weight: bfloat16 [512, 512], replicated, may hold values from -0.5 to 0.5
- out_bias: float32 [512], replicated, may hold values from -1.75 to 1.75
Outputs:
- block_out: bfloat16 [16, 512, 512], P('tile', 'head')
The draws below stay inside these ranges and needn't reach their ends.
All inputs are finite; a program needn't handle non-finite values.
Results may differ from the reference program's by a relative error of at most 0.01615.
Values may be sent and summed in bfloat16 or wider, within the bound.
A program may use at most 128 MiB of HBM per device.

```python
import jax
import jax.numpy as jnp
from jax import lax

C = 512
GROUPS = 32
W = 512
H = 16


def base_projection(key, salt):
    entries = jax.random.normal(jax.random.fold_in(key, salt), (C, C), jnp.float32)
    return jnp.clip(entries, -4.0, 4.0) * (1.0 / jnp.sqrt(jnp.float32(C // 4)))


def draw_query_weight(key, part):
    weight = base_projection(key, 311)
    return weight.astype(jnp.bfloat16)


def draw_key_weight(key, part):
    weight = base_projection(key, 523)
    return weight.astype(jnp.bfloat16)


def smooth_field(key):
    freq_rows = jax.random.randint(jax.random.fold_in(key, 7101), (4,), 1, 4).astype(jnp.float32)
    freq_cols = jax.random.randint(jax.random.fold_in(key, 7102), (4,), 0, 4).astype(jnp.float32)
    phases = jax.random.uniform(jax.random.fold_in(key, 7103), (4,), jnp.float32, -jnp.pi, jnp.pi)
    amplitudes = jax.random.uniform(jax.random.fold_in(key, 7104), (4,), jnp.float32, 0.5, 0.9)
    row_pos = jnp.arange(H, dtype=jnp.float32) / jnp.float32(H)
    col_pos = jnp.arange(W, dtype=jnp.float32) / jnp.float32(W)
    phase_grid = 2.0 * jnp.pi * (freq_rows[:, None, None] * row_pos[None, :, None] + freq_cols[:, None, None] * col_pos[None, None, :]) + phases[:, None, None]
    return jnp.sum(amplitudes[:, None, None] * jnp.cos(phase_grid), axis=0) + 0.4


def draw_latent(key, part):
    field = smooth_field(key)
    loading = jax.random.normal(jax.random.fold_in(key, 7105), (C,), jnp.float32)
    noise = 0.7 * jax.random.normal(jax.random.fold_in(key, 7106), (H, W, C), jnp.float32)
    values = noise + field[:, :, None] * loading[None, None, :]
    return jnp.clip(values, -6.0, 6.0).astype(jnp.bfloat16)


def gaussian(key, dims, scale, most, kind=jnp.bfloat16):
    return jnp.clip(scale * jax.random.normal(key, dims, jnp.float32), -most, most).astype(kind)


def setup_inputs(seed: int = 0) -> dict:
    arg_keys = jax.random.split(jax.random.key(seed), 19)
    latent = draw_latent(jax.random.fold_in(arg_keys[18], 71), 0)
    norm1_gain = jnp.clip(1.0 + 0.15 * jax.random.normal(arg_keys[1], (C,), jnp.float32), 0.25, 1.75)
    norm1_shift = gaussian(arg_keys[2], (C,), 0.3, 1.75, jnp.float32)
    conv1_weight = gaussian(arg_keys[3], (3, 3, C, C), (9 * C) ** -0.5, 0.09375)
    conv1_bias = gaussian(arg_keys[4], (C,), 0.3, 1.75, jnp.float32)
    norm2_gain = jnp.clip(1.0 + 0.15 * jax.random.normal(arg_keys[5], (C,), jnp.float32), 0.25, 1.75)
    norm2_shift = gaussian(arg_keys[6], (C,), 0.3, 1.75, jnp.float32)
    conv2_weight = gaussian(arg_keys[7], (3, 3, C, C), (9 * C) ** -0.5, 0.09375)
    conv2_bias = gaussian(arg_keys[8], (C,), 0.3, 1.75, jnp.float32)
    norm3_gain = jnp.clip(1.0 + 0.15 * jax.random.normal(arg_keys[9], (C,), jnp.float32), 0.25, 1.75)
    norm3_shift = gaussian(arg_keys[10], (C,), 0.3, 1.75, jnp.float32)
    query_weight = draw_query_weight(jax.random.fold_in(arg_keys[18], 71), 0)
    query_bias = gaussian(arg_keys[12], (C,), 0.5, 3.0, jnp.float32)
    key_weight = draw_key_weight(jax.random.fold_in(arg_keys[18], 71), 0)
    value_weight = gaussian(arg_keys[14], (C, C), C ** -0.5, 0.25)
    value_bias = gaussian(arg_keys[15], (C,), 0.5, 3.0, jnp.float32)
    out_weight = gaussian(arg_keys[16], (C, C), (C // 4) ** -0.5, 0.5)
    out_bias = gaussian(arg_keys[17], (C,), 0.3, 1.75, jnp.float32)
    return dict(latent=latent, norm1_gain=norm1_gain, norm1_shift=norm1_shift, conv1_weight=conv1_weight, conv1_bias=conv1_bias, norm2_gain=norm2_gain, norm2_shift=norm2_shift, conv2_weight=conv2_weight, conv2_bias=conv2_bias, norm3_gain=norm3_gain, norm3_shift=norm3_shift, query_weight=query_weight, query_bias=query_bias, key_weight=key_weight, value_weight=value_weight, value_bias=value_bias, out_weight=out_weight, out_bias=out_bias)


def group_norm(values, gain, shift):
    grouped = values.reshape(-1, GROUPS, C // GROUPS)
    mean = lax.optimization_barrier(jnp.mean(grouped, axis=(0, 2)))
    deviation = grouped - mean[None, :, None]
    variance = lax.optimization_barrier(jnp.mean(deviation * deviation, axis=(0, 2)))
    normalized = deviation * lax.rsqrt(variance + 1e-06)[None, :, None]
    return normalized.reshape(values.shape) * gain + shift

def conv_three(act, weight, bias):
    result = lax.conv_general_dilated(act[None], weight, (1, 1), ((1, 1), (1, 1)), dimension_numbers=('NHWC', 'HWIO', 'NHWC'), preferred_element_type=jnp.float32)[0]
    return result + bias

def reference(latent, norm1_gain, norm1_shift, conv1_weight, conv1_bias, norm2_gain, norm2_shift, conv2_weight, conv2_bias, norm3_gain, norm3_shift, query_weight, query_bias, key_weight, value_weight, value_bias, out_weight, out_bias):
    latent32 = latent.astype(jnp.float32)
    act1 = jax.nn.silu(group_norm(latent32, norm1_gain, norm1_shift)).astype(jnp.bfloat16)
    hidden = conv_three(act1, conv1_weight, conv1_bias)
    act2 = jax.nn.silu(group_norm(hidden, norm2_gain, norm2_shift)).astype(jnp.bfloat16)
    resid = (latent32 + conv_three(act2, conv2_weight, conv2_bias)).astype(jnp.bfloat16)
    flat_res = resid.reshape(-1, C)
    normed = group_norm(flat_res.astype(jnp.float32), norm3_gain, norm3_shift).astype(jnp.bfloat16)
    queries = (jnp.dot(normed, query_weight, preferred_element_type=jnp.float32) + query_bias).astype(jnp.bfloat16)
    keys = jnp.dot(normed, key_weight, preferred_element_type=jnp.float32).astype(jnp.bfloat16)
    values = (jnp.dot(normed, value_weight, preferred_element_type=jnp.float32) + value_bias).astype(jnp.bfloat16)
    total_rows = queries.shape[0]
    block_rows = 1024 if total_rows % 1024 == 0 else total_rows
    softmax_scale = 1.0 / C ** 0.5

    def attend(query_block):
        scores = jnp.dot(query_block, keys.T, preferred_element_type=jnp.float32) * softmax_scale
        top = lax.optimization_barrier(jnp.max(scores, axis=1, keepdims=True))
        expo = jnp.exp(scores - top)
        row_sum = lax.optimization_barrier(jnp.sum(expo, axis=1, keepdims=True))
        weighted = jnp.dot(expo.astype(jnp.bfloat16), values, preferred_element_type=jnp.float32)
        return (weighted / row_sum).astype(jnp.bfloat16)
    attended = lax.map(attend, queries.reshape(total_rows // block_rows, block_rows, C)).reshape(total_rows, C)
    mixed = flat_res.astype(jnp.float32) + jnp.dot(attended, out_weight, preferred_element_type=jnp.float32) + out_bias
    return mixed.astype(jnp.bfloat16).reshape(latent.shape)
```

```python
import functools
import math

import jax
import jax.numpy as jnp
from jax import lax
from jax.experimental import pallas as pl
from jax.experimental.pallas import tpu as pltpu
from jax.sharding import PartitionSpec as P

C = 512
GROUPS = 32
WIDTH = C // GROUPS
EPS = 1e-06
LANES = 128
PARTS = C // LANES
SHARE = WIDTH // PARTS
PAD = 8
LOG2E = math.log2(math.e)
MESH = pl.DeviceIdType.MESH
VMEM = pl.BlockSpec(memory_space=pltpu.VMEM)
ANY = pl.BlockSpec(memory_space=pl.ANY)


def nt_dot(a, b):
    return lax.dot_general(a, b, (((1,), (1,)), ((), ())), preferred_element_type=jnp.float32)


def nn_dot(a, b):
    return jnp.dot(a, b, preferred_element_type=jnp.float32)


def lane_index(rows):
    return lax.broadcasted_iota(jnp.int32, (rows, LANES), 1)


def group_sum(values):
    lane = lane_index(values.shape[0])
    step = 1
    while step < WIDTH:
        below = pltpu.roll(values, step, 1)
        above = pltpu.roll(values, LANES - step, 1)
        values = values + jnp.where(lane % (2 * step) >= step, below, above)
        step *= 2
    return values


def fold(row):
    return jnp.concatenate([row[:, i * LANES : (i + 1) * LANES] for i in range(PARTS)], axis=0)


def unfold(rows):
    return jnp.concatenate([rows[i : i + 1] for i in range(PARTS)], axis=1)


def local_stats(values):
    count = values.shape[0]
    mean = jnp.sum(values, axis=0, keepdims=True) / count
    deviation = values - mean
    square = jnp.sum(deviation * deviation, axis=0, keepdims=True)
    mean, square = fold(mean), fold(square)
    group_mean = group_sum(mean) / WIDTH
    gap = mean - group_mean
    square = group_sum(square + count * gap * gap)
    lane = lane_index(1)
    packed = jnp.zeros((1, LANES), jnp.float32)
    for i in range(PARTS):
        one = jnp.where(lane % 2 == 0, group_mean[i : i + 1], square[i : i + 1])
        packed = jnp.where((lane % WIDTH) // SHARE == i, one, packed)
    return packed


def merged_stats(slots, count):
    total = slots.shape[0]
    sums = jnp.sum(slots, axis=0)
    mean = sums / total
    gap = slots - mean[None]
    spread = jnp.sum(gap * gap, axis=0)
    variance = (sums + count * pltpu.roll(spread, 1, 1)) / (total * count)
    lane = lane_index(1)
    both = jnp.where(lane % 2 == 0, mean, lax.rsqrt(variance + EPS))
    row = lax.broadcasted_iota(jnp.int32, (2 * PARTS, LANES), 0)
    want = (row % PARTS) * SHARE + row // PARTS
    wide = jnp.where(lane_index(2 * PARTS) % WIDTH == want, both, 0.0)
    wide = group_sum(wide)
    return unfold(wide[:PARTS]), unfold(wide[PARTS:])


def silu(values):
    return values / (1.0 + jnp.exp(-values))


def block_kernel(
    tiles,
    heads,
    lat_ref,
    n1g,
    n1s,
    c1b,
    n2g,
    n2s,
    c2b,
    n3g,
    n3s,
    qb,
    vb,
    ob,
    w1_hbm,
    w2_hbm,
    wq_hbm,
    wk_hbm,
    wv_hbm,
    wo_hbm,
    out_ref,
    w1,
    w2,
    wp,
    act,
    shifted,
    hid,
    row_in,
    row_out,
    col_in,
    col_out,
    corner_in,
    stat_out,
    stat_in,
    norm,
    res,
    kv,
    kn,
    qn,
    qp,
    acc,
    top,
    low,
    o_out,
    o_in,
    l_out,
    l_in,
    w_sem,
    s_send,
    s_recv,
    h_send,
    h_recv,
    z_send,
    z_recv,
    c_send,
    c_recv,
    q_send,
    q_recv,
    o_send,
    o_recv,
    l_send,
    l_recv,
):
    rows, cols, _ = lat_ref.shape
    n = rows * cols
    total = tiles * heads
    half = tiles // 2
    tile, head = lax.axis_index("tile"), lax.axis_index("head")
    me = tile * heads + head
    partner = (tile + 1 - 2 * lax.rem(tile, 2), head)

    weights = [
        pltpu.make_async_copy(src, dst, w_sem.at[i])
        for i, (src, dst) in enumerate(
            (
                (w1_hbm, w1),
                (w2_hbm, w2),
                (wq_hbm, wp.at[0]),
                (wk_hbm, wp.at[1]),
                (wv_hbm, wp.at[2]),
                (wo_hbm, wp.at[3]),
            )
        )
    ]
    for copy in weights:
        copy.start()

    barrier = pltpu.get_barrier_semaphore()

    def greet(k, carry):
        peer = lax.rem(me + k, total)
        pl.semaphore_signal(
            barrier, inc=1, device_id=(peer // heads, lax.rem(peer, heads)), device_id_type=MESH
        )
        return carry

    lax.fori_loop(1, total, greet, 0)

    def remote(src, dst, send, recv, device):
        return pltpu.make_async_remote_copy(
            src_ref=src,
            dst_ref=dst,
            send_sem=send,
            recv_sem=recv,
            device_id=device,
            device_id_type=MESH,
        )

    def stat_copy(phase, k):
        peer = lax.rem(me + k, total)
        return remote(
            stat_out.at[phase],
            stat_in.at[phase, k],
            s_send.at[phase, k],
            s_recv.at[phase, k],
            (peer // heads, lax.rem(peer, heads)),
        )

    def stats_start(phase):
        def begin(k, carry):
            stat_copy(phase, k).start()
            return carry

        lax.fori_loop(1, total, begin, 0)

    def stats_finish(phase, gain, shift):
        def finish(k, carry):
            stat_copy(phase, k).wait()
            return carry

        lax.fori_loop(1, total, finish, 0)
        mean, inverse = merged_stats(stat_in[phase], n * WIDTH)
        norm[0:1] = mean
        norm[1:2] = inverse * gain[...]
        norm[2:3] = shift[...]

    def put_stats(phase, values):
        packed = local_stats(values)
        stat_out[phase] = packed
        stat_in[phase, 0] = packed

    def normalize(values):
        return (values - norm[0:1]) * norm[1:2] + norm[2:3]

    def halo_plan(phase, first_row, last_row):
        first, last = col_out.at[phase, 0], col_out.at[phase, 1]
        plan = [
            (first_row, row_in.at[phase, 1], -1, 0),
            (last_row, row_in.at[phase, 0], 1, 0),
            (first, col_in.at[phase, 1], 0, -1),
            (last, col_in.at[phase, 0], 0, 1),
            (first.at[0], corner_in.at[phase, 3], -1, -1),
            (last.at[0], corner_in.at[phase, 2], -1, 1),
            (first.at[rows - 1], corner_in.at[phase, 1], 1, -1),
            (last.at[rows - 1], corner_in.at[phase, 0], 1, 1),
        ]
        return plan

    def there(dt, dh):
        inside = None
        for place, delta, size in ((tile, dt, tiles), (head, dh, heads)):
            if delta:
                one = place + delta < size if delta > 0 else place + delta >= 0
                inside = one if inside is None else jnp.logical_and(inside, one)
        return inside

    def halo_copy(phase, i, src, dst, dt, dh):
        return remote(
            src, dst, h_send.at[phase, i], h_recv.at[phase, i], (tile + dt, head + dh)
        )

    def halo_start(phase, plan):
        for i, (src, dst, dt, dh) in enumerate(plan):

            @pl.when(there(dt, dh))
            def _(i=i, src=src, dst=dst, dt=dt, dh=dh):
                halo_copy(phase, i, src, dst, dt, dh).start()

    def halo_finish(phase, plan):
        for i, (src, dst, dt, dh) in enumerate(plan):

            @pl.when(there(dt, dh))
            def _(i=i, src=src, dst=dst, dt=dt, dh=dh):
                halo_copy(phase, i, src, dst, dt, dh).wait_send()

            @pl.when(there(-dt, -dh))
            def _(i=i, src=src, dst=dst, dt=dt, dh=dh):
                halo_copy(phase, i, src, dst, dt, dh).wait_recv()

    def put_columns(phase, values):
        for r in range(rows):
            col_out[phase, 0, r] = values[r, 0:1]
            col_out[phase, 1, r] = values[r, cols - 1 : cols]

    def activate(phase, values):
        left, right = head > 0, head < heads - 1
        up, down = tile > 0, tile < tiles - 1

        def active(x):
            return silu(normalize(x))

        for r in range(rows):
            act[1 + r, PAD : PAD + cols] = active(values(r))
            for side, at, inside in ((0, PAD - 1, left), (1, PAD + cols, right)):
                one = active(col_in[phase, side, r])
                act[1 + r, at : at + 1] = jnp.where(inside, one, 0.0)
        for side, at, inside in ((0, 0, up), (1, rows + 1, down)):
            one = active(row_in[phase, side].astype(jnp.float32))
            act[at, PAD : PAD + cols] = jnp.where(inside, one, 0.0)
            for k, place, beside in ((0, PAD - 1, left), (1, PAD + cols, right)):
                one = active(corner_in[phase, 2 * side + k])
                both = jnp.logical_and(inside, beside)
                act[at, place : place + 1] = jnp.where(both, one, 0.0)
        for dj in range(3):
            start = PAD - 1 + dj
            for r in range(rows + 2):
                shifted[dj, r] = act[r, start : start + cols].astype(jnp.bfloat16)

    def conv(weight):
        result = None
        for di in range(3):
            for dj in range(3):
                tap = 3 * di + dj
                lhs = shifted[dj, di : di + rows].reshape(n, C)
                one = nn_dot(lhs, weight[tap * C : (tap + 1) * C])
                result = one if result is None else result + one
        return result

    put_columns(0, lat_ref[...].astype(jnp.float32))
    put_stats(0, lat_ref[...].astype(jnp.float32).reshape(n, C))
    pl.semaphore_wait(barrier, total - 1)
    plan = halo_plan(0, lat_ref.at[0], lat_ref.at[rows - 1])
    stats_start(0)
    halo_start(0, plan)
    halo_finish(0, plan)
    stats_finish(0, n1g, n1s)
    activate(0, lambda r: lat_ref[r].astype(jnp.float32))
    weights[0].wait()
    hid[...] = (conv(w1) + c1b[...]).reshape(rows, cols, C)

    put_stats(1, hid[...].reshape(n, C))
    put_columns(1, hid[...])
    row_out[0] = hid[0].astype(jnp.bfloat16)
    row_out[1] = hid[rows - 1].astype(jnp.bfloat16)
    plan = halo_plan(1, row_out.at[0], row_out.at[1])
    stats_start(1)
    halo_start(1, plan)
    halo_finish(1, plan)
    stats_finish(1, n2g, n2s)
    activate(1, lambda r: hid[r])
    weights[1].wait()
    res[...] = (
        lat_ref[...].astype(jnp.float32).reshape(n, C) + (conv(w2) + c2b[...])
    ).astype(jnp.bfloat16)

    put_stats(2, res[...].astype(jnp.float32))
    stats_start(2)

    def z_copy(k):
        return remote(
            res,
            kv.at[0, k],
            z_send.at[k],
            z_recv.at[k],
            (tile, lax.rem(head + k, heads)),
        )

    def c_copy(k, src):
        return remote(src, kv.at[1, k], c_send.at[k], c_recv.at[k], partner)

    def q_copy(j):
        return remote(
            res, qn.at[j], q_send.at[j], q_recv.at[j], (lax.rem(tile + 2 * j, tiles), head)
        )

    c_copy(0, res).start()
    for k in range(1, heads):
        z_copy(k).start()

    def q_begin(j, carry):
        q_copy(j).start()
        return carry

    lax.fori_loop(1, half, q_begin, 0)
    stats_finish(2, n3g, n3s)
    for copy in weights[2:]:
        copy.wait()

    def normed(values):
        return normalize(values.astype(jnp.float32)).astype(jnp.bfloat16)

    scale = LOG2E / C**0.5

    def make_query(j, source):
        query = (nn_dot(normed(source), wp[0]) + qb[...]).astype(jnp.bfloat16)
        qp[j] = (nt_dot(query, wp[1]) * scale).astype(jnp.bfloat16)
        top[j] = jnp.full((n, LANES), -jnp.inf, jnp.float32)
        low[j] = jnp.zeros((n, LANES), jnp.float32)
        acc[j] = jnp.zeros((n, C), jnp.float32)

    make_query(0, res[...])

    def attend(j):
        scores = nt_dot(qp[j], kn[...])
        before = top[j][:, :1]
        peak = jnp.maximum(before, jnp.max(scores, axis=1, keepdims=True))
        expo = jnp.exp2(scores - peak).astype(jnp.bfloat16)
        fade = jnp.exp2(before - peak)
        sums = low[j][:, :1] * fade + jnp.sum(expo.astype(jnp.float32), axis=1, keepdims=True)
        top[j] = jnp.broadcast_to(peak, (n, LANES))
        low[j] = jnp.broadcast_to(sums, (n, LANES))
        acc[j] = acc[j] * fade + nn_dot(expo, kn[...])

    c_copy(0, res).wait()
    kn[0:n] = normed(res[...])
    kn[n : 2 * n] = normed(kv[1, 0])
    attend(0)

    def q_finish(j, carry):
        q_copy(j).wait()
        make_query(j, qn[j])
        attend(j)
        return carry

    lax.fori_loop(1, half, q_finish, 0)

    def column(k, carry):
        z_copy(k).wait()
        c_copy(k, kv.at[0, k]).start()
        kn[0:n] = normed(kv[0, k])
        c_copy(k, kv.at[0, k]).wait()
        kn[n : 2 * n] = normed(kv[1, k])

        def one(j, inner):
            attend(j)
            return inner

        lax.fori_loop(0, half, one, 0)
        return carry

    lax.fori_loop(1, heads, column, 0)

    def give_copies(j):
        owner = (lax.rem(tile + tiles - 2 * j, tiles), head)
        return [
            remote(o_out.at[j], o_in.at[j], o_send.at[j], o_recv.at[j], owner),
            remote(l_out.at[j], l_in.at[j], l_send.at[j], l_recv.at[j], owner),
        ]

    def finish(j, o_to, l_to):
        level = top[j] + jnp.log2(low[j])
        l_to[j] = jnp.transpose(level)[:8]
        o_to[j] = (acc[j] / low[j][:, :1]).astype(jnp.bfloat16)

    def give(j, carry):
        finish(j, o_out, l_out)
        for copy in give_copies(j):
            copy.start()
        return carry

    lax.fori_loop(1, half, give, 0)
    finish(0, o_in, l_in)

    def take(j, carry):
        for copy in give_copies(j):
            copy.wait()
        return carry

    lax.fori_loop(1, half, take, 0)
    peak = l_in[0]
    for j in range(1, half):
        peak = jnp.maximum(peak, l_in[j])
    shares = [jnp.exp2(l_in[j] - peak) for j in range(half)]
    whole = shares[0]
    for j in range(1, half):
        whole = whole + shares[j]
    mixed = jnp.zeros((n, C), jnp.float32)
    for j in range(half):
        share = jnp.transpose(jnp.broadcast_to((shares[j] / whole)[:1], (LANES, n)))[:, :1]
        mixed = mixed + share * o_in[j].astype(jnp.float32)
    attended = (nn_dot(mixed.astype(jnp.bfloat16), wp[2]) + vb[...]).astype(jnp.bfloat16)
    out = nn_dot(attended, wp[3]) + ob[...]
    out_ref[...] = (res[...].astype(jnp.float32) + out).astype(jnp.bfloat16)


def per_device(
    latent,
    norm1_gain,
    norm1_shift,
    conv1_weight,
    conv1_bias,
    norm2_gain,
    norm2_shift,
    conv2_weight,
    conv2_bias,
    norm3_gain,
    norm3_shift,
    query_weight,
    query_bias,
    key_weight,
    value_weight,
    value_bias,
    out_weight,
    out_bias,
):
    rows, cols, _ = latent.shape
    tiles, heads = lax.axis_size("tile"), lax.axis_size("head")
    n = rows * cols
    total = tiles * heads
    half = tiles // 2
    vectors = [
        v.reshape(1, C)
        for v in (
            norm1_gain,
            norm1_shift,
            conv1_bias,
            norm2_gain,
            norm2_shift,
            conv2_bias,
            norm3_gain,
            norm3_shift,
            query_bias,
            value_bias,
            out_bias,
        )
    ]
    matrices = [
        conv1_weight.reshape(9 * C, C),
        conv2_weight.reshape(9 * C, C),
        query_weight,
        key_weight,
        value_weight,
        out_weight,
    ]
    bf16, f32 = jnp.bfloat16, jnp.float32
    dma = pltpu.SemaphoreType.DMA
    out = pl.pallas_call(
        functools.partial(block_kernel, tiles, heads),
        out_shape=jax.ShapeDtypeStruct((n, C), bf16),
        in_specs=[VMEM] * (1 + len(vectors)) + [ANY] * len(matrices),
        out_specs=VMEM,
        scratch_shapes=[
            pltpu.VMEM((9 * C, C), bf16),
            pltpu.VMEM((9 * C, C), bf16),
            pltpu.VMEM((4, C, C), bf16),
            pltpu.VMEM((rows + 2, cols + 2 * PAD, C), f32),
            pltpu.VMEM((3, rows + 2, cols, C), bf16),
            pltpu.VMEM((rows, cols, C), f32),
            pltpu.VMEM((2, 2, cols, C), bf16),
            pltpu.VMEM((2, cols, C), bf16),
            pltpu.VMEM((2, 2, rows, 1, C), f32),
            pltpu.VMEM((2, 2, rows, 1, C), f32),
            pltpu.VMEM((2, 4, 1, C), f32),
            pltpu.VMEM((3, 1, LANES), f32),
            pltpu.VMEM((3, total, 1, LANES), f32),
            pltpu.VMEM((8, C), f32),
            pltpu.VMEM((n, C), bf16),
            pltpu.VMEM((2, heads, n, C), bf16),
            pltpu.VMEM((2 * n, C), bf16),
            pltpu.VMEM((half, n, C), bf16),
            pltpu.VMEM((half, n, C), bf16),
            pltpu.VMEM((half, n, C), f32),
            pltpu.VMEM((half, n, LANES), f32),
            pltpu.VMEM((half, n, LANES), f32),
            pltpu.VMEM((half, n, C), bf16),
            pltpu.VMEM((half, n, C), bf16),
            pltpu.VMEM((half, 8, n), f32),
            pltpu.VMEM((half, 8, n), f32),
            dma((6,)),
            dma((3, total)),
            dma((3, total)),
            dma((2, 8)),
            dma((2, 8)),
            dma((heads,)),
            dma((heads,)),
            dma((heads,)),
            dma((heads,)),
            dma((half,)),
            dma((half,)),
            dma((half,)),
            dma((half,)),
            dma((half,)),
            dma((half,)),
        ],
        compiler_params=pltpu.CompilerParams(collective_id=1, has_side_effects=True),
        name="middle_block",
    )(latent, *vectors, *matrices)
    return out.reshape(rows, cols, C)


def solution(mesh):
    return jax.shard_map(
        per_device,
        mesh=mesh,
        in_specs=(P("tile", "head", None),) + (P(),) * 17,
        out_specs=P("tile", "head", None),
        check_vma=False,
    )
```

```python
import functools
import math

import jax
import jax.numpy as jnp
from jax import lax
from jax.experimental import pallas as pl
from jax.experimental.pallas import tpu as pltpu
from jax.sharding import PartitionSpec as P

C = 512
GROUPS = 32
WIDTH = C // GROUPS
EPS = 1e-06
LANES = 128
PARTS = C // LANES
SHARE = WIDTH // PARTS
PAD = 8
LOG2E = math.log2(math.e)
MESH = pl.DeviceIdType.MESH
VMEM = pl.BlockSpec(memory_space=pltpu.VMEM)
HBM = pl.BlockSpec(memory_space=pltpu.HBM)
VECTORS = 11
CHUNKS = 2
DIRECT = 2
VMEM_LIMIT = 56 * 1024 * 1024


def nt_dot(a, b):
    return lax.dot_general(a, b, (((1,), (1,)), ((), ())), preferred_element_type=jnp.float32)


def nn_dot(a, b):
    return jnp.dot(a, b, preferred_element_type=jnp.float32)


def lane_index(rows):
    return lax.broadcasted_iota(jnp.int32, (rows, LANES), 1)


def group_sum(values):
    lane = lane_index(values.shape[0])
    step = 1
    while step < WIDTH:
        below = pltpu.roll(values, step, 1)
        above = pltpu.roll(values, LANES - step, 1)
        values = values + jnp.where(lane % (2 * step) >= step, below, above)
        step *= 2
    return values


def fold(row):
    return jnp.concatenate([row[:, i * LANES : (i + 1) * LANES] for i in range(PARTS)], axis=0)


def unfold(rows):
    return jnp.concatenate([rows[i : i + 1] for i in range(PARTS)], axis=1)


def local_stats(values):
    count = values.shape[0]
    mean = jnp.sum(values, axis=0, keepdims=True) / count
    deviation = values - mean
    square = jnp.sum(deviation * deviation, axis=0, keepdims=True)
    mean, square = fold(mean), fold(square)
    group_mean = group_sum(mean) / WIDTH
    gap = mean - group_mean
    square = group_sum(square + count * gap * gap)
    lane = lane_index(1)
    packed = jnp.zeros((1, LANES), jnp.float32)
    for i in range(PARTS):
        one = jnp.where(lane % 2 == 0, group_mean[i : i + 1], square[i : i + 1])
        packed = jnp.where((lane % WIDTH) // SHARE == i, one, packed)
    return packed


def merged_stats(slots, count):
    total = slots.shape[0]
    sums = jnp.sum(slots, axis=0)
    mean = sums / total
    gap = slots - mean[None]
    spread = jnp.sum(gap * gap, axis=0)
    variance = (sums + count * pltpu.roll(spread, 1, 1)) / (total * count)
    lane = lane_index(1)
    both = jnp.where(lane % 2 == 0, mean, lax.rsqrt(variance + EPS))
    row = lax.broadcasted_iota(jnp.int32, (2 * PARTS, LANES), 0)
    want = (row % PARTS) * SHARE + row // PARTS
    wide = jnp.where(lane_index(2 * PARTS) % WIDTH == want, both, 0.0)
    wide = group_sum(wide)
    return unfold(wide[:PARTS]), unfold(wide[PARTS:])


def silu(values):
    return values / (1.0 + jnp.exp(-values))


def block_kernel(
    tiles,
    heads,
    lat_hbm,
    *refs,
):
    vec_hbm, mat_hbm, refs = refs[:VECTORS], refs[VECTORS : VECTORS + 6], refs[VECTORS + 6 :]
    (
        out_ref,
        lat_ref,
        vec,
        w1,
        w2,
        wp,
        act,
        shifted,
        hid,
        row_in,
        row_out,
        col_in,
        col_out,
        corner_in,
        stat_out,
        stat_in,
        norm,
        res,
        kv,
        kn,
        kt,
        qn,
        qp,
        acc,
        top,
        low,
        o_out,
        o_in,
        l_out,
        l_in,
        lat_sem,
        v_sem,
        w_sem,
        s_send,
        s_recv,
        h_send,
        h_recv,
        z_send,
        z_recv,
        c_send,
        c_recv,
        q_send,
        q_recv,
        o_send,
        o_recv,
        l_send,
        l_recv,
    ) = refs
    rows, cols, _ = lat_ref.shape
    n = rows * cols
    total = tiles * heads
    half = tiles // 2
    pairs = half // 2
    tile, head = lax.axis_index("tile"), lax.axis_index("head")
    me = tile * heads + head
    partner = (tile + 1 - 2 * lax.rem(tile, 2), head)

    barrier = pltpu.get_barrier_semaphore()

    def greet(k, carry):
        peer = lax.rem(me + k, total)
        pl.semaphore_signal(
            barrier, inc=1, device_id=(peer // heads, lax.rem(peer, heads)), device_id_type=MESH
        )
        return carry

    latent_copy = pltpu.make_async_copy(lat_hbm, lat_ref, lat_sem)
    latent_copy.start()
    lax.fori_loop(1, total, greet, 0)
    vectors = [
        pltpu.make_async_copy(src, vec.at[i], v_sem.at[i]) for i, src in enumerate(vec_hbm)
    ]
    targets = [w1, w2] + [wp.at[i] for i in range(4)]
    weights = [
        pltpu.make_async_copy(src, dst, w_sem.at[i])
        for i, (src, dst) in enumerate(zip(mat_hbm, targets))
    ]
    for copy in vectors + weights:
        copy.start()
    n1g, n1s, c1b, n2g, n2s, c2b, n3g, n3s, qb, vb, ob = [vec.at[i] for i in range(VECTORS)]

    def remote(src, dst, send, recv, device):
        return pltpu.make_async_remote_copy(
            src_ref=src,
            dst_ref=dst,
            send_sem=send,
            recv_sem=recv,
            device_id=device,
            device_id_type=MESH,
        )

    def stat_copy(phase, k):
        peer = lax.rem(me + k, total)
        return remote(
            stat_out.at[phase],
            stat_in.at[phase, k],
            s_send.at[phase],
            s_recv.at[phase],
            (peer // heads, lax.rem(peer, heads)),
        )

    def stats_start(phase):
        def begin(k, carry):
            stat_copy(phase, k).start()
            return carry

        lax.fori_loop(1, total, begin, 0)

    def stats_finish(phase, gain, shift):
        others = stat_in.at[phase, pl.ds(1, total - 1)]
        for sem in (s_send, s_recv):
            pltpu.make_async_copy(others, others, sem.at[phase]).wait()
        mean, inverse = merged_stats(stat_in[phase], n * WIDTH)
        norm[0:1] = mean
        norm[1:2] = inverse * gain[...]
        norm[2:3] = shift[...]

    def put_stats(phase, values):
        packed = local_stats(values)
        stat_out[phase] = packed
        stat_in[phase, 0] = packed

    def normalize(values):
        return (values - norm[0:1]) * norm[1:2] + norm[2:3]

    def halo_plan(phase, first_row, last_row):
        first, last = col_out.at[phase, 0], col_out.at[phase, 1]
        plan = [
            (first_row, row_in.at[phase, 1], -1, 0),
            (last_row, row_in.at[phase, 0], 1, 0),
            (first, col_in.at[phase, 1], 0, -1),
            (last, col_in.at[phase, 0], 0, 1),
            (first.at[0], corner_in.at[phase, 3], -1, -1),
            (last.at[0], corner_in.at[phase, 2], -1, 1),
            (first.at[rows - 1], corner_in.at[phase, 1], 1, -1),
            (last.at[rows - 1], corner_in.at[phase, 0], 1, 1),
        ]
        return plan

    def there(dt, dh):
        inside = None
        for place, delta, size in ((tile, dt, tiles), (head, dh, heads)):
            if delta:
                one = place + delta < size if delta > 0 else place + delta >= 0
                inside = one if inside is None else jnp.logical_and(inside, one)
        return inside

    def halo_copy(phase, i, src, dst, dt, dh):
        return remote(
            src, dst, h_send.at[phase, i], h_recv.at[phase, i], (tile + dt, head + dh)
        )

    def halo_start(phase, plan):
        for i, (src, dst, dt, dh) in enumerate(plan):

            @pl.when(there(dt, dh))
            def _(i=i, src=src, dst=dst, dt=dt, dh=dh):
                halo_copy(phase, i, src, dst, dt, dh).start()

    def halo_finish(phase, plan):
        for i, (src, dst, dt, dh) in enumerate(plan):

            @pl.when(there(dt, dh))
            def _(i=i, src=src, dst=dst, dt=dt, dh=dh):
                halo_copy(phase, i, src, dst, dt, dh).wait_send()

            @pl.when(there(-dt, -dh))
            def _(i=i, src=src, dst=dst, dt=dt, dh=dh):
                halo_copy(phase, i, src, dst, dt, dh).wait_recv()

    def put_columns(phase, values):
        for r in range(rows):
            col_out[phase, 0, r] = values[r, 0:1]
            col_out[phase, 1, r] = values[r, cols - 1 : cols]

    def activate(phase, values):
        left, right = head > 0, head < heads - 1
        up, down = tile > 0, tile < tiles - 1

        def active(x):
            return silu(normalize(x))

        for r in range(rows):
            act[1 + r, PAD : PAD + cols] = active(values(r))
            for side, at, inside in ((0, PAD - 1, left), (1, PAD + cols, right)):
                one = active(col_in[phase, side, r])
                act[1 + r, at : at + 1] = jnp.where(inside, one, 0.0)
        for side, at, inside in ((0, 0, up), (1, rows + 1, down)):
            one = active(row_in[phase, side].astype(jnp.float32))
            act[at, PAD : PAD + cols] = jnp.where(inside, one, 0.0)
            for k, place, beside in ((0, PAD - 1, left), (1, PAD + cols, right)):
                one = active(corner_in[phase, 2 * side + k])
                both = jnp.logical_and(inside, beside)
                act[at, place : place + 1] = jnp.where(both, one, 0.0)
        for dj in range(3):
            start = PAD - 1 + dj
            for r in range(rows + 2):
                shifted[dj, r] = act[r, start : start + cols].astype(jnp.bfloat16)

    def conv(weight):
        result = None
        for di in range(3):
            for dj in range(3):
                tap = 3 * di + dj
                lhs = shifted[dj, di : di + rows].reshape(n, C)
                one = nn_dot(lhs, weight[tap * C : (tap + 1) * C])
                result = one if result is None else result + one
        return result

    with jax.named_scope("stats0"):
        latent_copy.wait()
        put_columns(0, lat_ref[...].astype(jnp.float32))
        put_stats(0, lat_ref[...].astype(jnp.float32).reshape(n, C))
    with jax.named_scope("barrier"):
        pl.semaphore_wait(barrier, total - 1)
    with jax.named_scope("send0"):
        plan = halo_plan(0, lat_ref.at[0], lat_ref.at[rows - 1])
        stats_start(0)
        halo_start(0, plan)
    with jax.named_scope("halo0"):
        halo_finish(0, plan)
    with jax.named_scope("norm0"):
        for copy in vectors:
            copy.wait()
        stats_finish(0, n1g, n1s)
    with jax.named_scope("act0"):
        activate(0, lambda r: lat_ref[r].astype(jnp.float32))
    with jax.named_scope("w0"):
        weights[0].wait()
    with jax.named_scope("conv0"):
        hid[...] = (conv(w1) + c1b[...]).reshape(rows, cols, C)

    with jax.named_scope("stats1"):
        put_stats(1, hid[...].reshape(n, C))
        put_columns(1, hid[...])
        row_out[0] = hid[0].astype(jnp.bfloat16)
        row_out[1] = hid[rows - 1].astype(jnp.bfloat16)
    with jax.named_scope("send1"):
        plan = halo_plan(1, row_out.at[0], row_out.at[1])
        stats_start(1)
        halo_start(1, plan)
    with jax.named_scope("halo1"):
        halo_finish(1, plan)
    with jax.named_scope("norm1"):
        stats_finish(1, n2g, n2s)
    with jax.named_scope("act1"):
        activate(1, lambda r: hid[r])
    with jax.named_scope("conv1"):
        weights[1].wait()
        res[...] = (
            lat_ref[...].astype(jnp.float32).reshape(n, C) + (conv(w2) + c2b[...])
        ).astype(jnp.bfloat16)

    with jax.named_scope("stats2"):
        put_stats(2, res[...].astype(jnp.float32))
        stats_start(2)

    def piece(ref, ch):
        return ref.at[pl.ds(ch * (n // CHUNKS), n // CHUNKS)]

    def z_copy(source, src, way, distance, ch):
        return remote(
            piece(src, ch),
            piece(kv.at[0, source], ch),
            z_send.at[way, distance, ch],
            z_recv.at[source, ch],
            (tile, head + (1 if way else -1) * (distance if distance <= DIRECT else 1)),
        )

    def reachable(way, distance):
        return head + distance < heads if way else head - distance >= 0

    def straight(fn):
        at_end = jnp.logical_or(head == 0, head == heads - 1)
        farther = tuple(range(2, min(DIRECT, heads - 1) + 1))
        for distances, chosen in ((farther, at_end), ((1,), True), (farther, ~at_end)):
            for distance in distances:
                for ch in range(CHUNKS):
                    for way in (0, 1):

                        @pl.when(jnp.logical_and(reachable(way, distance), chosen))
                        def _(way=way, distance=distance, ch=ch):
                            fn(z_copy(head, res, way, distance, ch))

    def onward(distance, fn, chunks=tuple(range(CHUNKS))):
        for ch in chunks:
            for way in (0, 1):

                @pl.when(jnp.logical_and(reachable(1 - way, distance), reachable(way, 1)))
                def _(way=way, ch=ch):
                    source = head + (-distance if way else distance)
                    fn(z_copy(source, kv.at[0, source], way, distance + 1, ch))

    def z_arrived(source, distance, way):
        def wait():
            for ch in range(CHUNKS):
                z_copy(source, res, way, 1, ch).wait_recv()

        if heads - 1 > DIRECT:
            passed = jnp.logical_and(distance >= DIRECT, reachable(1 - way, 1))
            pl.when(jnp.logical_not(passed))(wait)
        else:
            wait()

    def c_copy(source, src):
        return remote(
            src, kv.at[1, source], c_send.at[source], c_recv.at[source], partner
        )

    def q_copy(j):
        return remote(
            res, qn.at[j], q_send.at[j], q_recv.at[j], (lax.rem(tile + 2 * j, tiles), head)
        )

    def q_begin(j, carry):
        q_copy(j).start()
        return carry

    c_copy(head, res).start()
    with jax.named_scope("norm2"):
        straight(lambda copy: copy.start())
        lax.fori_loop(1, half, q_begin, 0)
        stats_finish(2, n3g, n3s)
        for copy in weights[2:]:
            copy.wait()

    def normed(values):
        return normalize(values.astype(jnp.float32)).astype(jnp.bfloat16)

    scale = LOG2E / C**0.5

    def make_query(pair, at, source):
        query = (nn_dot(normed(source), wp[0]) + qb[...]).astype(jnp.bfloat16)
        qp[pair, :, at * n : (at + 1) * n] = (nt_dot(wp[1], query) * scale).astype(jnp.bfloat16)

    def clear(pair):
        top[pair] = jnp.full((1, 2 * n), -jnp.inf, jnp.float32)
        low[pair] = jnp.zeros((1, 2 * n), jnp.float32)
        acc[pair] = jnp.zeros((C, 2 * n), jnp.float32)

    def prepare(core, source, values):
        keys = normed(values)
        kn[core, source] = keys
        kt[core, source] = jnp.transpose(keys)

    def attend(pair, core, source):
        scores = nn_dot(kn[core, source], qp[pair])
        before = top[pair]
        peak = jnp.maximum(before, jnp.max(scores, axis=0, keepdims=True))
        expo = jnp.exp2(scores - peak).astype(jnp.bfloat16)
        fade = jnp.exp2(before - peak)
        top[pair] = peak
        low[pair] = low[pair] * fade + jnp.sum(
            expo.astype(jnp.float32), axis=0, keepdims=True
        )
        acc[pair] = acc[pair] * fade + nn_dot(kt[core, source], expo)

    def columns(fn, distances, inner):
        for distance in distances:
            for way in (0, 1):
                source = head + (distance if way else -distance)
                chosen = reachable(way, distance)
                if inner is not None:
                    within = jnp.logical_and(source > 0, source < heads - 1)
                    chosen = jnp.logical_and(chosen, within if inner else ~within)

                @pl.when(chosen)
                def _(distance=distance, way=way, source=source):
                    fn(source, distance, way)

    far = tuple(range(2, heads))

    def pass_on(ch):
        def go(copy):
            copy.wait_recv()
            copy.start()

        with jax.named_scope("relay"):
            for distance in range(DIRECT, heads - 1):
                onward(distance, go, (ch,))

    with jax.named_scope("query0"):
        clear(0)
        make_query(0, 0, res[...])
        prepare(0, head, res[...])
    with jax.named_scope("q_wait0"):
        q_copy(1).wait()
    for ch in range(CHUNKS - 1):
        pass_on(ch)
    with jax.named_scope("query1"):
        make_query(0, 1, qn[1])
    with jax.named_scope("attend_own"):
        attend(0, 0, head)
    with jax.named_scope("c_own"):
        c_copy(head, res).wait()
        prepare(1, head, kv[1, head])
    with jax.named_scope("attend_partner"):
        attend(0, 1, head)

    def fetch(source, distance, way, work):
        with jax.named_scope("z_wait"):
            z_arrived(source, distance, way)
            c_copy(source, kv.at[0, source]).start()
        with jax.named_scope("z_attend0"):
            prepare(0, source, kv[0, source])
            work(0, source)
        with jax.named_scope("c_wait"):
            c_copy(source, kv.at[0, source]).wait()
        with jax.named_scope("z_attend1"):
            prepare(1, source, kv[1, source])
            work(1, source)

    def near(source, distance, way):
        fetch(source, distance, way, lambda core, place: attend(0, core, place))

    def far_pairs(core, source):
        def one(pair, carry):
            attend(pair, core, source)
            return carry

        if pairs == 2:
            attend(1, core, source)
        else:
            lax.fori_loop(1, pairs, one, 0)

    pass_on(CHUNKS - 1)
    columns(near, (1,), True)

    def rest(pair, carry):
        with jax.named_scope("q_wait1"):
            for at in range(2):
                q_copy(2 * pair + at).wait()
        with jax.named_scope("query2"):
            clear(pair)
            for at in range(2):
                make_query(pair, at, qn[2 * pair + at])
        with jax.named_scope("attend_rest"):
            attend(pair, 0, head)
            attend(pair, 1, head)
        return carry

    lax.fori_loop(1, pairs, rest, 0)

    def again(source, distance, way):
        with jax.named_scope("again"):
            far_pairs(0, source)
            far_pairs(1, source)

    def late(*place):
        fetch(*place, far_pairs)

    columns(again, (1,), True)
    columns(late, far, None)
    columns(late, (1,), False)

    def give_copies(j):
        owner = (lax.rem(tile + tiles - 2 * j, tiles), head)
        return [
            remote(o_out.at[j], o_in.at[j], o_send.at[j], o_recv.at[j], owner),
            remote(l_out.at[j], l_in.at[j], l_send.at[j], l_recv.at[j], owner),
        ]

    def finish(pair, at, o_to, l_to):
        lanes = slice(at * n, (at + 1) * n)
        sums = low[pair, :, lanes]
        l_to[2 * pair + at] = top[pair, :, lanes] + jnp.log2(sums)
        o_to[2 * pair + at] = (acc[pair, :, lanes] * (1.0 / sums)).astype(jnp.bfloat16)

    def send(j):
        for copy in give_copies(j):
            copy.start()

    def give(i, carry):
        pair = pairs - 1 - i
        for at in range(2):
            finish(pair, at, o_out, l_out)
            send(2 * pair + at)
        return carry

    with jax.named_scope("give"):
        lax.fori_loop(0, pairs - 1, give, 0)

    def own(source, distance, way):
        with jax.named_scope("own_far"):
            attend(0, 0, source)
            attend(0, 1, source)

    columns(own, far, None)
    columns(own, (1,), False)
    with jax.named_scope("give1"):
        finish(0, 1, o_out, l_out)
        send(1)
    with jax.named_scope("finish0"):
        finish(0, 0, o_in, l_in)
        straight(lambda copy: copy.wait_send())
        for distance in range(DIRECT, heads - 1):
            onward(distance, lambda copy: copy.wait_send())

    def take(j, carry):
        for copy in give_copies(j):
            copy.wait()
        return carry

    with jax.named_scope("take"):
        lax.fori_loop(1, half, take, 0)
    with jax.named_scope("last"):
        peak = l_in[0]
        for j in range(1, half):
            peak = jnp.maximum(peak, l_in[j])
        shares = [jnp.exp2(l_in[j] - peak) for j in range(half)]
        whole = shares[0]
        for j in range(1, half):
            whole = whole + shares[j]
        mixed = jnp.zeros((C, n), jnp.float32)
        for j in range(half):
            mixed = mixed + (shares[j] / whole) * o_in[j].astype(jnp.float32)
        mixed = jnp.transpose(mixed.astype(jnp.bfloat16))
        attended = (nn_dot(mixed, wp[2]) + vb[...]).astype(jnp.bfloat16)
        out = nn_dot(attended, wp[3]) + ob[...]
        out_ref[...] = (res[...].astype(jnp.float32) + out).astype(jnp.bfloat16)


def per_device(
    latent,
    norm1_gain,
    norm1_shift,
    conv1_weight,
    conv1_bias,
    norm2_gain,
    norm2_shift,
    conv2_weight,
    conv2_bias,
    norm3_gain,
    norm3_shift,
    query_weight,
    query_bias,
    key_weight,
    value_weight,
    value_bias,
    out_weight,
    out_bias,
):
    rows, cols, _ = latent.shape
    tiles, heads = lax.axis_size("tile"), lax.axis_size("head")
    n = rows * cols
    total = tiles * heads
    half = tiles // 2
    vectors = [
        v.reshape(1, C)
        for v in (
            norm1_gain,
            norm1_shift,
            conv1_bias,
            norm2_gain,
            norm2_shift,
            conv2_bias,
            norm3_gain,
            norm3_shift,
            query_bias,
            value_bias,
            out_bias,
        )
    ]
    matrices = [
        conv1_weight.reshape(9 * C, C),
        conv2_weight.reshape(9 * C, C),
        query_weight,
        key_weight,
        value_weight,
        out_weight,
    ]
    bf16, f32 = jnp.bfloat16, jnp.float32
    dma = pltpu.SemaphoreType.DMA
    out = pl.pallas_call(
        functools.partial(block_kernel, tiles, heads),
        out_shape=pltpu.VMEM((n, C), bf16),
        in_specs=[HBM] * (1 + len(vectors) + len(matrices)),
        out_specs=VMEM,
        scratch_shapes=[
            pltpu.VMEM((rows, cols, C), bf16),
            pltpu.VMEM((len(vectors), 1, C), f32),
            pltpu.VMEM((9 * C, C), bf16),
            pltpu.VMEM((9 * C, C), bf16),
            pltpu.VMEM((4, C, C), bf16),
            pltpu.VMEM((rows + 2, cols + 2 * PAD, C), f32),
            pltpu.VMEM((3, rows + 2, cols, C), bf16),
            pltpu.VMEM((rows, cols, C), f32),
            pltpu.VMEM((2, 2, cols, C), bf16),
            pltpu.VMEM((2, cols, C), bf16),
            pltpu.VMEM((2, 2, rows, 1, C), f32),
            pltpu.VMEM((2, 2, rows, 1, C), f32),
            pltpu.VMEM((2, 4, 1, C), f32),
            pltpu.VMEM((3, 1, LANES), f32),
            pltpu.VMEM((3, total, 1, LANES), f32),
            pltpu.VMEM((8, C), f32),
            pltpu.VMEM((n, C), bf16),
            pltpu.VMEM((2, heads, n, C), bf16),
            pltpu.VMEM((2, heads, n, C), bf16),
            pltpu.VMEM((2, heads, C, n), bf16),
            pltpu.VMEM((half, n, C), bf16),
            pltpu.VMEM((half // 2, C, 2 * n), bf16),
            pltpu.VMEM((half // 2, C, 2 * n), f32),
            pltpu.VMEM((half // 2, 1, 2 * n), f32),
            pltpu.VMEM((half // 2, 1, 2 * n), f32),
            pltpu.VMEM((half, C, n), bf16),
            pltpu.VMEM((half, C, n), bf16),
            pltpu.VMEM((half, 1, n), f32),
            pltpu.VMEM((half, 1, n), f32),
            dma,
            dma((len(vectors),)),
            dma((len(matrices),)),
            dma((3,)),
            dma((3,)),
            dma((2, 8)),
            dma((2, 8)),
            dma((2, heads, CHUNKS)),
            dma((heads, CHUNKS)),
            dma((heads,)),
            dma((heads,)),
            dma((half,)),
            dma((half,)),
            dma((half,)),
            dma((half,)),
            dma((half,)),
            dma((half,)),
        ],
        compiler_params=pltpu.CompilerParams(
            collective_id=1, has_side_effects=True, vmem_limit_bytes=VMEM_LIMIT
        ),
        name="middle_block",
    )(latent, *vectors, *matrices)
    return out.reshape(rows, cols, C)


def solution(mesh):
    return jax.shard_map(
        per_device,
        mesh=mesh,
        in_specs=(P("tile", "head", None),) + (P(),) * 17,
        out_specs=P("tile", "head", None),
        check_vma=False,
    )
```

```python
import functools
import math

import jax
import jax.numpy as jnp
from jax import lax
from jax.experimental import pallas as pl
from jax.experimental.pallas import tpu as pltpu
from jax.sharding import PartitionSpec as P

C = 512
GROUPS = 32
WIDTH = C // GROUPS
EPS = 1e-06
LANES = 128
PARTS = C // LANES
SHARE = WIDTH // PARTS
PAD = 8
LOG2E = math.log2(math.e)
MESH = pl.DeviceIdType.MESH
VMEM = pl.BlockSpec(memory_space=pltpu.VMEM)
HBM = pl.BlockSpec(memory_space=pltpu.HBM)
VECTORS = 11
CHUNKS = 4
SPLIT = 1
DIRECT = 2
VMEM_LIMIT = 56 * 1024 * 1024


def nt_dot(a, b):
    return lax.dot_general(a, b, (((1,), (1,)), ((), ())), preferred_element_type=jnp.float32)


def nn_dot(a, b):
    return jnp.dot(a, b, preferred_element_type=jnp.float32)


def lane_index(rows):
    return lax.broadcasted_iota(jnp.int32, (rows, LANES), 1)


def lane_partner(values, step):
    below = pltpu.roll(values, step, 1)
    above = pltpu.roll(values, LANES - step, 1)
    return jnp.where(lane_index(values.shape[0]) % (2 * step) >= step, below, above)


def group_sum(values):
    step = 1
    while step < WIDTH:
        values = values + lane_partner(values, step)
        step *= 2
    return values


def fold(row):
    return jnp.concatenate([row[:, i * LANES : (i + 1) * LANES] for i in range(PARTS)], axis=0)


def unfold(rows):
    return jnp.concatenate([rows[i : i + 1] for i in range(PARTS)], axis=1)


def local_stats(values):
    count = values.shape[0]
    mean = jnp.sum(values, axis=0, keepdims=True) / count
    deviation = values - mean
    square = jnp.sum(deviation * deviation, axis=0, keepdims=True)
    group_mean, square = fold(mean), fold(square)
    step = 1
    while step < WIDTH:
        other = lane_partner(group_mean, step)
        gap = group_mean - other
        square = square + lane_partner(square, step) + (0.5 * count * step) * (gap * gap)
        group_mean = 0.5 * (group_mean + other)
        step *= 2
    lane = lane_index(1)
    packed = jnp.zeros((1, LANES), jnp.float32)
    for i in range(PARTS):
        one = jnp.where(lane % 2 == 0, group_mean[i : i + 1], square[i : i + 1])
        packed = jnp.where((lane % WIDTH) // SHARE == i, one, packed)
    return packed


def merged_stats(slots, count):
    total = slots.shape[0]
    sums = jnp.sum(slots, axis=0)
    mean = sums / total
    gap = slots - mean[None]
    spread = jnp.sum(gap * gap, axis=0)
    variance = (sums + count * pltpu.roll(spread, 1, 1)) / (total * count)
    lane = lane_index(1)
    both = jnp.where(lane % 2 == 0, mean, lax.rsqrt(variance + EPS))
    row = lax.broadcasted_iota(jnp.int32, (2 * PARTS, LANES), 0)
    want = (row % PARTS) * SHARE + row // PARTS
    wide = jnp.where(lane_index(2 * PARTS) % WIDTH == want, both, 0.0)
    wide = group_sum(wide)
    return unfold(wide[:PARTS]), unfold(wide[PARTS:])


def silu(values):
    half = 0.5 * values
    return half + half * jnp.tanh(half)


def block_kernel(
    tiles,
    heads,
    lat_hbm,
    *refs,
):
    vec_hbm, mat_hbm, refs = refs[:VECTORS], refs[VECTORS : VECTORS + 6], refs[VECTORS + 6 :]
    (
        out_ref,
        lat_ref,
        vec,
        w1,
        w2,
        wp,
        act,
        shifted,
        hid,
        row_in,
        row_out,
        col_in,
        col_out,
        corner_in,
        stat_out,
        stat_in,
        norm,
        res,
        kv,
        kn,
        kt,
        qn,
        qp,
        acc,
        top,
        low,
        o_out,
        o_in,
        l_out,
        l_in,
        u_in,
        ul_in,
        m_out,
        ml_out,
        lat_sem,
        v_sem,
        w_sem,
        s_send,
        s_recv,
        h_send,
        h_recv,
        z_send,
        z_recv,
        c_send,
        c_recv,
        q_send,
        q_recv,
        o_send,
        o_recv,
        l_send,
        l_recv,
    ) = refs
    rows, cols, _ = lat_ref.shape
    n = rows * cols
    total = tiles * heads
    half = tiles // 2
    pairs = half // 2
    tile, head = lax.axis_index("tile"), lax.axis_index("head")
    me = tile * heads + head
    partner = (tile + 1 - 2 * lax.rem(tile, 2), head)

    def fellow(j):
        chip, bit, other = lax.div(tile, 2), 1, 0
        if half & (half - 1):
            return lax.rem(tile + 2 * j, tiles)
        while bit < half:
            mine, flip = lax.rem(lax.div(chip, bit), 2), (j // bit) % 2
            other = other + bit * (mine + flip - 2 * mine * flip)
            bit *= 2
        return 2 * other + lax.rem(tile, 2)

    def lender(j):
        return fellow(j) if half & (half - 1) == 0 else lax.rem(tile + tiles - 2 * j, tiles)

    barrier = pltpu.get_barrier_semaphore()

    def greet(k, carry):
        peer = lax.rem(me + k, total)
        pl.semaphore_signal(
            barrier, inc=1, device_id=(lax.div(peer, heads), lax.rem(peer, heads)), device_id_type=MESH
        )
        return carry

    latent_copy = pltpu.make_async_copy(lat_hbm, lat_ref, lat_sem)
    latent_copy.start()
    lax.fori_loop(1, total, greet, 0)
    vectors = [
        pltpu.make_async_copy(src, vec.at[i], v_sem.at[i]) for i, src in enumerate(vec_hbm)
    ]
    targets = [w1, w2] + [wp.at[i] for i in range(4)]
    weights = [
        pltpu.make_async_copy(src, dst, w_sem.at[i])
        for i, (src, dst) in enumerate(zip(mat_hbm, targets))
    ]
    for copy in vectors + weights:
        copy.start()
    n1g, n1s, c1b, n2g, n2s, c2b, n3g, n3s, qb, vb, ob = [vec.at[i] for i in range(VECTORS)]

    def remote(src, dst, send, recv, device):
        return pltpu.make_async_remote_copy(
            src_ref=src,
            dst_ref=dst,
            send_sem=send,
            recv_sem=recv,
            device_id=device,
            device_id_type=MESH,
        )

    def stat_copy(phase, k):
        peer = lax.rem(me + k, total)
        return remote(
            stat_out.at[phase],
            stat_in.at[phase, k],
            s_send.at[phase],
            s_recv.at[phase],
            (lax.div(peer, heads), lax.rem(peer, heads)),
        )

    def stats_start(phase):
        def begin(k, carry):
            stat_copy(phase, k).start()
            return carry

        lax.fori_loop(1, total, begin, 0)

    def stats_finish(phase, gain, shift):
        others = stat_in.at[phase, pl.ds(1, total - 1)]
        for sem in (s_send, s_recv):
            pltpu.make_async_copy(others, others, sem.at[phase]).wait()
        mean, inverse = merged_stats(stat_in[phase], n * WIDTH)
        norm[0:1] = mean
        norm[1:2] = inverse * gain[...]
        norm[2:3] = shift[...]

    def put_stats(phase, values):
        packed = local_stats(values)
        stat_out[phase] = packed
        stat_in[phase, 0] = packed

    def normalize(values):
        return (values - norm[0:1]) * norm[1:2] + norm[2:3]

    def halo_plan(phase, first_row, last_row):
        first, last = col_out.at[phase, 0], col_out.at[phase, 1]
        plan = [
            (first_row, row_in.at[phase, 1], -1, 0),
            (last_row, row_in.at[phase, 0], 1, 0),
            (first, col_in.at[phase, 1], 0, -1),
            (last, col_in.at[phase, 0], 0, 1),
            (first.at[0], corner_in.at[phase, 3], -1, -1),
            (last.at[0], corner_in.at[phase, 2], -1, 1),
            (first.at[rows - 1], corner_in.at[phase, 1], 1, -1),
            (last.at[rows - 1], corner_in.at[phase, 0], 1, 1),
        ]
        return plan

    def there(dt, dh):
        inside = None
        for place, delta, size in ((tile, dt, tiles), (head, dh, heads)):
            if delta:
                one = place + delta < size if delta > 0 else place + delta >= 0
                inside = one if inside is None else jnp.logical_and(inside, one)
        return inside

    def halo_copy(phase, i, src, dst, dt, dh):
        return remote(
            src, dst, h_send.at[phase, i], h_recv.at[phase, i], (tile + dt, head + dh)
        )

    def halo_start(phase, plan):
        for i, (src, dst, dt, dh) in enumerate(plan):

            @pl.when(there(dt, dh))
            def _(i=i, src=src, dst=dst, dt=dt, dh=dh):
                halo_copy(phase, i, src, dst, dt, dh).start()

    def halo_finish(phase, plan):
        for i, (src, dst, dt, dh) in enumerate(plan):

            @pl.when(there(dt, dh))
            def _(i=i, src=src, dst=dst, dt=dt, dh=dh):
                halo_copy(phase, i, src, dst, dt, dh).wait_send()

            @pl.when(there(-dt, -dh))
            def _(i=i, src=src, dst=dst, dt=dt, dh=dh):
                halo_copy(phase, i, src, dst, dt, dh).wait_recv()

    def put_columns(phase, values):
        for r in range(rows):
            col_out[phase, 0, r] = values[r, 0:1]
            col_out[phase, 1, r] = values[r, cols - 1 : cols]

    def activate(phase, values):
        left, right = head > 0, head < heads - 1
        up, down = tile > 0, tile < tiles - 1

        def active(x):
            return silu(normalize(x))

        for r in range(rows):
            act[1 + r, PAD : PAD + cols] = active(values(r))
            for side, at, inside in ((0, PAD - 1, left), (1, PAD + cols, right)):
                one = active(col_in[phase, side, r])
                act[1 + r, at : at + 1] = jnp.where(inside, one, 0.0)
        for side, at, inside in ((0, 0, up), (1, rows + 1, down)):
            one = active(row_in[phase, side].astype(jnp.float32))
            act[at, PAD : PAD + cols] = jnp.where(inside, one, 0.0)
            for k, place, beside in ((0, PAD - 1, left), (1, PAD + cols, right)):
                one = active(corner_in[phase, 2 * side + k])
                both = jnp.logical_and(inside, beside)
                act[at, place : place + 1] = jnp.where(both, one, 0.0)
        for dj in range(3):
            start = PAD - 1 + dj
            for r in range(rows + 2):
                shifted[dj, r] = act[r, start : start + cols].astype(jnp.bfloat16)

    def conv(weight):
        result = None
        for di in range(3):
            for dj in range(3):
                tap = 3 * di + dj
                lhs = shifted[dj, di : di + rows].reshape(n, C)
                one = nn_dot(lhs, weight[tap * C : (tap + 1) * C])
                result = one if result is None else result + one
        return result

    with jax.named_scope("stats0"):
        latent_copy.wait()
        put_columns(0, lat_ref[...].astype(jnp.float32))
        put_stats(0, lat_ref[...].astype(jnp.float32).reshape(n, C))
    with jax.named_scope("barrier"):
        pl.semaphore_wait(barrier, total - 1)
    with jax.named_scope("send0"):
        plan = halo_plan(0, lat_ref.at[0], lat_ref.at[rows - 1])
        stats_start(0)
        halo_start(0, plan)
    with jax.named_scope("halo0"):
        halo_finish(0, plan)
    with jax.named_scope("norm0"):
        for copy in vectors:
            copy.wait()
        stats_finish(0, n1g, n1s)
    with jax.named_scope("act0"):
        activate(0, lambda r: lat_ref[r].astype(jnp.float32))
    with jax.named_scope("w0"):
        weights[0].wait()
    with jax.named_scope("conv0"):
        hid[...] = (conv(w1) + c1b[...]).reshape(rows, cols, C)

    with jax.named_scope("stats1"):
        put_stats(1, hid[...].reshape(n, C))
        put_columns(1, hid[...])
        row_out[0] = hid[0].astype(jnp.bfloat16)
        row_out[1] = hid[rows - 1].astype(jnp.bfloat16)
    with jax.named_scope("send1"):
        plan = halo_plan(1, row_out.at[0], row_out.at[1])
        stats_start(1)
        halo_start(1, plan)
    with jax.named_scope("halo1"):
        halo_finish(1, plan)
    with jax.named_scope("norm1"):
        stats_finish(1, n2g, n2s)
    with jax.named_scope("act1"):
        activate(1, lambda r: hid[r])
    with jax.named_scope("conv1"):
        weights[1].wait()
        res[...] = (
            lat_ref[...].astype(jnp.float32).reshape(n, C) + (conv(w2) + c2b[...])
        ).astype(jnp.bfloat16)

    with jax.named_scope("stats2"):
        put_stats(2, res[...].astype(jnp.float32))
        stats_start(2)

    def piece(ref, ch):
        return ref.at[pl.ds(ch * (n // CHUNKS), n // CHUNKS)]

    def z_copy(source, src, way, distance, ch):
        return remote(
            piece(src, ch),
            piece(kv.at[0, source], ch),
            z_send.at[way, distance, ch],
            z_recv.at[source, ch],
            (tile, head + (1 if way else -1) * (distance if distance <= DIRECT else 1)),
        )

    def reachable(way, distance):
        return head + distance < heads if way else head - distance >= 0

    def straight(fn):
        at_end = jnp.logical_or(head == 0, head == heads - 1)
        farther = [(d, c) for d in range(2, min(DIRECT, heads - 1) + 1) for c in range(CHUNKS)]
        nearer = [(1, c) for c in range(CHUNKS)]
        for chosen, order in ((at_end, farther + nearer), (~at_end, nearer + farther)):
            for distance, ch in order:
                for way in (0, 1):

                    @pl.when(jnp.logical_and(reachable(way, distance), chosen))
                    def _(way=way, distance=distance, ch=ch):
                        fn(z_copy(head, res, way, distance, ch))

    def onward(distance, fn, chunks=tuple(range(CHUNKS))):
        for ch in chunks:
            for way in (0, 1):

                @pl.when(jnp.logical_and(reachable(1 - way, distance), reachable(way, 1)))
                def _(way=way, ch=ch):
                    source = head + (-distance if way else distance)
                    fn(z_copy(source, kv.at[0, source], way, distance + 1, ch))

    def z_arrived(source, distance, way, ch):
        def wait():
            z_copy(source, res, way, 1, ch).wait_recv()

        if heads - 1 > DIRECT:
            passed = jnp.logical_and(distance >= DIRECT, reachable(1 - way, 1))
            pl.when(jnp.logical_not(passed))(wait)
        else:
            wait()

    def c_copy(source, src, ch):
        return remote(
            piece(src, ch),
            piece(kv.at[1, source], ch),
            c_send.at[source, ch],
            c_recv.at[source, ch],
            partner,
        )

    def q_copy(j):
        return remote(
            res, qn.at[j], q_send.at[j], q_recv.at[j], (fellow(j), head)
        )

    def q_begin(j, carry):
        q_copy(j).start()
        return carry

    for ch in range(CHUNKS):
        c_copy(head, res, ch).start()
    def pass_on(ch):
        def go(copy):
            copy.wait_recv()
            copy.start()

        with jax.named_scope("relay"):
            for distance in range(DIRECT, heads - 1):
                onward(distance, go, (ch,))

    straight(lambda copy: copy.start())
    lax.fori_loop(1, half, q_begin, 0)
    pass_on(0)
    with jax.named_scope("norm2"):
        stats_finish(2, n3g, n3s)
        for copy in weights[2:]:
            copy.wait()

    def normed(values):
        return normalize(values.astype(jnp.float32)).astype(jnp.bfloat16)

    scale = LOG2E / C**0.5

    def make_query(pair, at, source):
        query = (nn_dot(normed(source), wp[0]) + qb[...]).astype(jnp.bfloat16)
        qp[pair, :, at * n : (at + 1) * n] = (nt_dot(wp[1], query) * scale).astype(jnp.bfloat16)

    def clear(pair):
        top[pair] = jnp.full((1, 2 * n), -jnp.inf, jnp.float32)
        low[pair] = jnp.zeros((1, 2 * n), jnp.float32)
        acc[pair] = jnp.zeros((C, 2 * n), jnp.float32)

    def prepare(core, source, values):
        keys = normed(values)
        kn[source, core] = keys
        kt[source, :, core * n : (core + 1) * n] = jnp.transpose(keys)

    def one_core(core, source):
        return kn.at[source, core], kt.at[source, :, pl.ds(core * n, n)]

    def both_cores(source):
        return kn.at[source], kt.at[source]

    def attend(pair, *blocks):
        for at in range(SPLIT):
            width = 2 * n // SPLIT
            attend_lanes(pair, slice(at * width, (at + 1) * width), blocks)

    def attend_lanes(pair, lanes, blocks):
        query = qp[pair, :, lanes]
        scores = [nn_dot(keys[...].reshape(-1, C), query) for keys, _ in blocks]
        before = top[pair, :, lanes]
        peak = before
        for one in scores:
            peak = jnp.maximum(peak, jnp.max(one, axis=0, keepdims=True))
        fade = jnp.exp2(before - peak)
        sums, values = low[pair, :, lanes] * fade, None
        for one, (_, turned) in zip(scores, blocks):
            expo = jnp.exp2(one - peak).astype(jnp.bfloat16)
            sums = sums + jnp.sum(expo.astype(jnp.float32), axis=0, keepdims=True)
            part = nn_dot(turned[...], expo)
            values = part if values is None else values + part
        top[pair, :, lanes] = peak
        low[pair, :, lanes] = sums
        acc[pair, :, lanes] = acc[pair, :, lanes] * fade + values

    def columns(fn, distances, inner=None, extra=None):
        for distance in distances:
            for way in (0, 1):
                source = head + (distance if way else -distance)
                chosen = reachable(way, distance)
                if inner is not None:
                    within = jnp.logical_and(source > 0, source < heads - 1)
                    chosen = jnp.logical_and(chosen, within if inner else ~within)
                if extra is not None:
                    chosen = jnp.logical_and(chosen, extra)

                @pl.when(chosen)
                def _(distance=distance, way=way, source=source):
                    fn(source, distance, way)

    far = tuple(range(2, heads))
    at_end = jnp.logical_or(head == 0, head == heads - 1)

    with jax.named_scope("query0"):
        clear(0)
        make_query(0, 0, res[...])
        prepare(0, head, res[...])
    pass_on(1)
    with jax.named_scope("q_wait0"):
        q_copy(1).wait()
    with jax.named_scope("query1"):
        make_query(0, 1, qn[1])
        for ch in range(CHUNKS):
            c_copy(head, res, ch).wait()
        prepare(1, head, kv[1, head])
    pass_on(2)
    with jax.named_scope("attend_own"):
        attend(0, both_cores(head))
    pass_on(3)

    def begin(source, distance, way):
        with jax.named_scope("z_wait"):
            for ch in range(CHUNKS):
                z_arrived(source, distance, way, ch)
                c_copy(source, kv.at[0, source], ch).start()
        with jax.named_scope("prepare0"):
            prepare(0, source, kv[0, source])

    def second(source):
        with jax.named_scope("c_wait"):
            for ch in range(CHUNKS):
                c_copy(source, kv.at[0, source], ch).wait()
        with jax.named_scope("prepare1"):
            prepare(1, source, kv[1, source])

    def other_pairs(*blocks):
        def one(pair, carry):
            attend(pair, *blocks)
            return carry

        if pairs == 2:
            attend(1, *blocks)
        else:
            lax.fori_loop(1, pairs, one, 0)

    def together(source, distance, way):
        second(source)
        with jax.named_scope("together"):
            other_pairs(both_cores(source))

    columns(begin, (1,), True)

    def rest(pair, carry):
        with jax.named_scope("q_wait1"):
            for at in range(2):
                q_copy(2 * pair + at).wait()
        with jax.named_scope("query2"):
            clear(pair)
            for at in range(2):
                make_query(pair, at, qn[2 * pair + at])
        with jax.named_scope("attend_rest"):
            attend(pair, both_cores(head))
        return carry

    lax.fori_loop(1, pairs, rest, 0)
    columns(begin, (2,), extra=~at_end)
    columns(together, (1,), True)
    columns(begin, (1,), False)
    columns(together, (2,), extra=~at_end)
    columns(together, (1,), False)
    def first_half(source, distance, way):
        begin(source, distance, way)
        with jax.named_scope("late0"):
            other_pairs(one_core(0, source))
        second(source)

    def second_half(source, distance, way):
        with jax.named_scope("late1"):
            other_pairs(one_core(1, source))

    columns(first_half, (2,), extra=at_end)
    columns(begin, far[1:])
    columns(second_half, (2,), extra=at_end)
    columns(together, far[1:])

    def both(src, dst, src_level, dst_level, sem, device):
        return [
            remote(src, dst, o_send.at[sem], o_recv.at[sem], device),
            remote(src_level, dst_level, l_send.at[sem], l_recv.at[sem], device),
        ]

    def give_copies(j):
        return both(o_out.at[j], o_in.at[j], l_out.at[j], l_in.at[j], j, (lender(j), head))

    def finish(pair, at, o_to, l_to):
        for part in range(2):
            lanes = slice((2 * at + part) * (n // 2), (2 * at + part + 1) * (n // 2))
            sums = low[pair, :, lanes]
            l_to[2 * pair + at, part] = top[pair, :, lanes] + jnp.log2(sums)
            o_to[2 * pair + at, part] = (acc[pair, :, lanes] * (1.0 / sums)).astype(jnp.bfloat16)

    def own(source, distance, way):
        with jax.named_scope("own_far"):
            attend(0, both_cores(source))

    def column_sent():
        straight(lambda copy: copy.wait_send())
        for distance in range(DIRECT, heads - 1):
            onward(distance, lambda copy: copy.wait_send())

    def begin_all(copies):
        for copy in copies:
            copy.start()

    def end_all(copies):
        for copy in copies:
            copy.wait()

    if half == 4:
        def hop(part):
            via = (fellow(2 - part), head)
            return both(
                o_out.at[3, part], u_in.at[part], l_out.at[3, part], ul_in.at[part], part, via
            )

        def direct(j):
            part = 2 - j
            return both(
                o_out.at[j, part],
                o_in.at[j, part],
                l_out.at[j, part],
                l_in.at[j, part],
                1 + j,
                (fellow(j), head),
            )

        def merged(j):
            part = j - 1
            return both(
                m_out.at[part],
                o_in.at[j, part],
                ml_out.at[part],
                l_in.at[j, part],
                3 + j,
                (fellow(j), head),
            )

        def merge(j):
            part = j - 1
            end_all(hop(part))
            mine, theirs = l_out[j, part], ul_in[part]
            level = jnp.maximum(mine, theirs)
            keep, add = jnp.exp2(mine - level), jnp.exp2(theirs - level)
            whole = keep + add
            ml_out[part] = level + jnp.log2(whole)
            values = o_out[j, part].astype(jnp.float32) * (keep / whole)
            values = values + u_in[part].astype(jnp.float32) * (add / whole)
            m_out[part] = values.astype(jnp.bfloat16)
            begin_all(merged(j))

        with jax.named_scope("give"):
            finish(1, 1, o_out, l_out)
            begin_all(hop(0))
            begin_all(hop(1))
            finish(1, 0, o_out, l_out)
            begin_all(direct(2))
        columns(own, tuple(range(1, heads)))
        with jax.named_scope("give1"):
            finish(0, 1, o_out, l_out)
            begin_all(direct(1))
        with jax.named_scope("finish0"):
            finish(0, 0, o_in, l_in)
            column_sent()
        with jax.named_scope("merge2"):
            merge(2)
        with jax.named_scope("merge1"):
            merge(1)
        with jax.named_scope("take"):
            for j in (1, 2):
                end_all(direct(j))
                end_all(merged(j))
        parts = 3
    else:

        def give(i, carry):
            pair = pairs - 1 - i
            for at in range(2):
                finish(pair, at, o_out, l_out)
                begin_all(give_copies(2 * pair + at))
            return carry

        def take(j, carry):
            end_all(give_copies(j))
            return carry

        lax.fori_loop(0, pairs - 1, give, 0)
        columns(own, tuple(range(1, heads)))
        finish(0, 1, o_out, l_out)
        begin_all(give_copies(1))
        finish(0, 0, o_in, l_in)
        column_sent()
        lax.fori_loop(1, half, take, 0)
        parts = half
    with jax.named_scope("last"):
        sides = []
        for part in range(2):
            peak = l_in[0, part]
            for j in range(1, parts):
                peak = jnp.maximum(peak, l_in[j, part])
            shares = [jnp.exp2(l_in[j, part] - peak) for j in range(parts)]
            whole = shares[0]
            for j in range(1, parts):
                whole = whole + shares[j]
            side = jnp.zeros((C, n // 2), jnp.float32)
            for j in range(parts):
                side = side + (shares[j] / whole) * o_in[j, part].astype(jnp.float32)
            sides.append(side)
        mixed = jnp.concatenate(sides, axis=1)
        mixed = jnp.transpose(mixed.astype(jnp.bfloat16))
        attended = (nn_dot(mixed, wp[2]) + vb[...]).astype(jnp.bfloat16)
        out = nn_dot(attended, wp[3]) + ob[...]
        out_ref[...] = (res[...].astype(jnp.float32) + out).astype(jnp.bfloat16)


def per_device(
    latent,
    norm1_gain,
    norm1_shift,
    conv1_weight,
    conv1_bias,
    norm2_gain,
    norm2_shift,
    conv2_weight,
    conv2_bias,
    norm3_gain,
    norm3_shift,
    query_weight,
    query_bias,
    key_weight,
    value_weight,
    value_bias,
    out_weight,
    out_bias,
):
    rows, cols, _ = latent.shape
    tiles, heads = lax.axis_size("tile"), lax.axis_size("head")
    n = rows * cols
    total = tiles * heads
    half = tiles // 2
    vectors = [
        v.reshape(1, C)
        for v in (
            norm1_gain,
            norm1_shift,
            conv1_bias,
            norm2_gain,
            norm2_shift,
            conv2_bias,
            norm3_gain,
            norm3_shift,
            query_bias,
            value_bias,
            out_bias,
        )
    ]
    matrices = [
        conv1_weight.reshape(9 * C, C),
        conv2_weight.reshape(9 * C, C),
        query_weight,
        key_weight,
        value_weight,
        out_weight,
    ]
    bf16, f32 = jnp.bfloat16, jnp.float32
    dma = pltpu.SemaphoreType.DMA
    out = pl.pallas_call(
        functools.partial(block_kernel, tiles, heads),
        out_shape=pltpu.VMEM((n, C), bf16),
        in_specs=[HBM] * (1 + len(vectors) + len(matrices)),
        out_specs=VMEM,
        scratch_shapes=[
            pltpu.VMEM((rows, cols, C), bf16),
            pltpu.VMEM((len(vectors), 1, C), f32),
            pltpu.VMEM((9 * C, C), bf16),
            pltpu.VMEM((9 * C, C), bf16),
            pltpu.VMEM((4, C, C), bf16),
            pltpu.VMEM((rows + 2, cols + 2 * PAD, C), f32),
            pltpu.VMEM((3, rows + 2, cols, C), bf16),
            pltpu.VMEM((rows, cols, C), f32),
            pltpu.VMEM((2, 2, cols, C), bf16),
            pltpu.VMEM((2, cols, C), bf16),
            pltpu.VMEM((2, 2, rows, 1, C), f32),
            pltpu.VMEM((2, 2, rows, 1, C), f32),
            pltpu.VMEM((2, 4, 1, C), f32),
            pltpu.VMEM((3, 1, LANES), f32),
            pltpu.VMEM((3, total, 1, LANES), f32),
            pltpu.VMEM((8, C), f32),
            pltpu.VMEM((n, C), bf16),
            pltpu.VMEM((2, heads, n, C), bf16),
            pltpu.VMEM((heads, 2, n, C), bf16),
            pltpu.VMEM((heads, C, 2 * n), bf16),
            pltpu.VMEM((half, n, C), bf16),
            pltpu.VMEM((half // 2, C, 2 * n), bf16),
            pltpu.VMEM((half // 2, C, 2 * n), f32),
            pltpu.VMEM((half // 2, 1, 2 * n), f32),
            pltpu.VMEM((half // 2, 1, 2 * n), f32),
            pltpu.VMEM((half, 2, C, n // 2), bf16),
            pltpu.VMEM((half, 2, C, n // 2), bf16),
            pltpu.VMEM((half, 2, 1, n // 2), f32),
            pltpu.VMEM((half, 2, 1, n // 2), f32),
            pltpu.VMEM((2, C, n // 2), bf16),
            pltpu.VMEM((2, 1, n // 2), f32),
            pltpu.VMEM((2, C, n // 2), bf16),
            pltpu.VMEM((2, 1, n // 2), f32),
            dma,
            dma((len(vectors),)),
            dma((len(matrices),)),
            dma((3,)),
            dma((3,)),
            dma((2, 8)),
            dma((2, 8)),
            dma((2, heads, CHUNKS)),
            dma((heads, CHUNKS)),
            dma((heads, CHUNKS)),
            dma((heads, CHUNKS)),
            dma((half,)),
            dma((half,)),
            dma((half + 2,)),
            dma((half + 2,)),
            dma((half + 2,)),
            dma((half + 2,)),
        ],
        compiler_params=pltpu.CompilerParams(
            collective_id=1, has_side_effects=True, vmem_limit_bytes=VMEM_LIMIT
        ),
        name="middle_block",
    )(latent, *vectors, *matrices)
    return out.reshape(rows, cols, C)


def solution(mesh):
    return jax.shard_map(
        per_device,
        mesh=mesh,
        in_specs=(P("tile", "head", None),) + (P(),) * 17,
        out_specs=P("tile", "head", None),
        check_vma=False,
    )
```

```python
import functools
import math

import jax
import jax.numpy as jnp
from jax import lax
from jax.experimental import pallas as pl
from jax.experimental.pallas import tpu as pltpu
from jax.sharding import PartitionSpec as P

C = 512
GROUPS = 32
WIDTH = C // GROUPS
EPS = 1e-06
LANES = 128
PARTS = C // LANES
SHARE = WIDTH // PARTS
PAD = 8
LOG2E = math.log2(math.e)
MESH = pl.DeviceIdType.MESH
VMEM = pl.BlockSpec(memory_space=pltpu.VMEM)
HBM = pl.BlockSpec(memory_space=pltpu.HBM)
VECTORS = 11
CHUNKS = 4
DIRECT = 2
VMEM_LIMIT = 56 * 1024 * 1024


def interleaved(far, near):
    order, rest, near = far[: len(far) // 2], far[len(far) // 2 :], list(near)
    for place in rest:
        order += near[:1] + [place]
        near = near[1:]
    return order + near


def nt_dot(a, b):
    return lax.dot_general(a, b, (((1,), (1,)), ((), ())), preferred_element_type=jnp.float32)


def nn_dot(a, b):
    return jnp.dot(a, b, preferred_element_type=jnp.float32)


def lane_index(rows):
    return lax.broadcasted_iota(jnp.int32, (rows, LANES), 1)


def lane_partner(values, step):
    below = pltpu.roll(values, step, 1)
    above = pltpu.roll(values, LANES - step, 1)
    return jnp.where(lane_index(values.shape[0]) % (2 * step) >= step, below, above)


def group_sum(values):
    step = 1
    while step < WIDTH:
        values = values + lane_partner(values, step)
        step *= 2
    return values


def fold(row):
    return jnp.concatenate([row[:, i * LANES : (i + 1) * LANES] for i in range(PARTS)], axis=0)


def unfold(rows):
    return jnp.concatenate([rows[i : i + 1] for i in range(PARTS)], axis=1)


def local_stats(values):
    count = values.shape[0]
    mean = jnp.sum(values, axis=0, keepdims=True) / count
    deviation = values - mean
    square = jnp.sum(deviation * deviation, axis=0, keepdims=True)
    group_mean, square = fold(mean), fold(square)
    step = 1
    while step < WIDTH:
        other = lane_partner(group_mean, step)
        gap = group_mean - other
        square = square + lane_partner(square, step) + (0.5 * count * step) * (gap * gap)
        group_mean = 0.5 * (group_mean + other)
        step *= 2
    lane = lane_index(1)
    packed = jnp.zeros((1, LANES), jnp.float32)
    for i in range(PARTS):
        one = jnp.where(lane % 2 == 0, group_mean[i : i + 1], square[i : i + 1])
        packed = jnp.where((lane % WIDTH) // SHARE == i, one, packed)
    return packed


def merged_stats(slots, count):
    total = slots.shape[0]
    sums = jnp.sum(slots, axis=0)
    mean = sums / total
    gap = slots - mean[None]
    spread = jnp.sum(gap * gap, axis=0)
    variance = (sums + count * pltpu.roll(spread, 1, 1)) / (total * count)
    lane = lane_index(1)
    both = jnp.where(lane % 2 == 0, mean, lax.rsqrt(variance + EPS))
    row = lax.broadcasted_iota(jnp.int32, (2 * PARTS, LANES), 0)
    want = (row % PARTS) * SHARE + row // PARTS
    wide = jnp.where(lane_index(2 * PARTS) % WIDTH == want, both, 0.0)
    wide = group_sum(wide)
    return unfold(wide[:PARTS]), unfold(wide[PARTS:])


def silu(values):
    half = 0.5 * values
    return half + half * jnp.tanh(half)


def block_kernel(
    tiles,
    heads,
    lat_hbm,
    *refs,
):
    vec_hbm, mat_hbm, refs = refs[:VECTORS], refs[VECTORS : VECTORS + 6], refs[VECTORS + 6 :]
    (
        out_ref,
        lat_ref,
        vec,
        w1,
        w2,
        wp,
        act,
        shifted,
        hid,
        row_in,
        row_out,
        col_in,
        col_out,
        corner_in,
        stat_out,
        stat_in,
        norm,
        res,
        kv,
        kn,
        kt,
        qn,
        qp,
        acc,
        top,
        low,
        o_out,
        o_in,
        l_out,
        l_in,
        u_in,
        ul_in,
        m_out,
        ml_out,
        lat_sem,
        v_sem,
        w_sem,
        s_send,
        s_recv,
        h_send,
        h_recv,
        z_send,
        z_recv,
        c_send,
        c_recv,
        q_send,
        q_recv,
        o_send,
        o_recv,
        l_send,
        l_recv,
    ) = refs
    rows, cols, _ = lat_ref.shape
    n = rows * cols
    total = tiles * heads
    half = tiles // 2
    pairs = half // 2
    tile, head = lax.axis_index("tile"), lax.axis_index("head")
    me = tile * heads + head
    partner = (tile + 1 - 2 * lax.rem(tile, 2), head)

    def fellow(j):
        chip, bit, other = lax.div(tile, 2), 1, 0
        if half & (half - 1):
            return lax.rem(tile + 2 * j, tiles)
        while bit < half:
            mine, flip = lax.rem(lax.div(chip, bit), 2), (j // bit) % 2
            other = other + bit * (mine + flip - 2 * mine * flip)
            bit *= 2
        return 2 * other + lax.rem(tile, 2)

    def lender(j):
        return fellow(j) if half & (half - 1) == 0 else lax.rem(tile + tiles - 2 * j, tiles)

    barrier = pltpu.get_barrier_semaphore()

    def greet(k, carry):
        peer = lax.rem(me + k, total)
        pl.semaphore_signal(
            barrier, inc=1, device_id=(lax.div(peer, heads), lax.rem(peer, heads)), device_id_type=MESH
        )
        return carry

    latent_copy = pltpu.make_async_copy(lat_hbm, lat_ref, lat_sem)
    latent_copy.start()
    lax.fori_loop(1, total, greet, 0)
    vectors = [
        pltpu.make_async_copy(src, vec.at[i], v_sem.at[i]) for i, src in enumerate(vec_hbm)
    ]
    targets = [w1, w2] + [wp.at[i] for i in range(4)]
    weights = [
        pltpu.make_async_copy(src, dst, w_sem.at[i])
        for i, (src, dst) in enumerate(zip(mat_hbm, targets))
    ]
    for copy in vectors + weights:
        copy.start()
    n1g, n1s, c1b, n2g, n2s, c2b, n3g, n3s, qb, vb, ob = [vec.at[i] for i in range(VECTORS)]

    def remote(src, dst, send, recv, device):
        return pltpu.make_async_remote_copy(
            src_ref=src,
            dst_ref=dst,
            send_sem=send,
            recv_sem=recv,
            device_id=device,
            device_id_type=MESH,
        )

    def stat_copy(phase, k):
        peer = lax.rem(me + k, total)
        return remote(
            stat_out.at[phase],
            stat_in.at[phase, k],
            s_send.at[phase],
            s_recv.at[phase],
            (lax.div(peer, heads), lax.rem(peer, heads)),
        )

    def stats_start(phase):
        def begin(k, carry):
            stat_copy(phase, k).start()
            return carry

        lax.fori_loop(1, total, begin, 0)

    def stats_finish(phase, gain, shift):
        others = stat_in.at[phase, pl.ds(1, total - 1)]
        for sem in (s_send, s_recv):
            pltpu.make_async_copy(others, others, sem.at[phase]).wait()
        mean, inverse = merged_stats(stat_in[phase], n * WIDTH)
        norm[0:1] = mean
        norm[1:2] = inverse * gain[...]
        norm[2:3] = shift[...]

    def put_stats(phase, values):
        packed = local_stats(values)
        stat_out[phase] = packed
        stat_in[phase, 0] = packed

    def normalize(values):
        return (values - norm[0:1]) * norm[1:2] + norm[2:3]

    def halo_plan(phase, first_row, last_row):
        first, last = col_out.at[phase, 0], col_out.at[phase, 1]
        plan = [
            (first_row, row_in.at[phase, 1], -1, 0),
            (last_row, row_in.at[phase, 0], 1, 0),
            (first, col_in.at[phase, 1], 0, -1),
            (last, col_in.at[phase, 0], 0, 1),
            (first.at[0], corner_in.at[phase, 3], -1, -1),
            (last.at[0], corner_in.at[phase, 2], -1, 1),
            (first.at[rows - 1], corner_in.at[phase, 1], 1, -1),
            (last.at[rows - 1], corner_in.at[phase, 0], 1, 1),
        ]
        return plan

    def there(dt, dh):
        inside = None
        for place, delta, size in ((tile, dt, tiles), (head, dh, heads)):
            if delta:
                one = place + delta < size if delta > 0 else place + delta >= 0
                inside = one if inside is None else jnp.logical_and(inside, one)
        return inside

    def halo_copy(phase, i, src, dst, dt, dh):
        return remote(
            src, dst, h_send.at[phase, i], h_recv.at[phase, i], (tile + dt, head + dh)
        )

    def halo_start(phase, plan):
        for i, (src, dst, dt, dh) in enumerate(plan):

            @pl.when(there(dt, dh))
            def _(i=i, src=src, dst=dst, dt=dt, dh=dh):
                halo_copy(phase, i, src, dst, dt, dh).start()

    def halo_finish(phase, plan):
        for i, (src, dst, dt, dh) in enumerate(plan):

            @pl.when(there(dt, dh))
            def _(i=i, src=src, dst=dst, dt=dt, dh=dh):
                halo_copy(phase, i, src, dst, dt, dh).wait_send()

            @pl.when(there(-dt, -dh))
            def _(i=i, src=src, dst=dst, dt=dt, dh=dh):
                halo_copy(phase, i, src, dst, dt, dh).wait_recv()

    def put_columns(phase, values):
        for r in range(rows):
            col_out[phase, 0, r] = values[r, 0:1]
            col_out[phase, 1, r] = values[r, cols - 1 : cols]

    def activate(phase, values):
        left, right = head > 0, head < heads - 1
        up, down = tile > 0, tile < tiles - 1

        def active(x):
            return silu(normalize(x))

        for r in range(rows):
            act[1 + r, PAD : PAD + cols] = active(values(r))
            for side, at, inside in ((0, PAD - 1, left), (1, PAD + cols, right)):
                one = active(col_in[phase, side, r])
                act[1 + r, at : at + 1] = jnp.where(inside, one, 0.0)
        for side, at, inside in ((0, 0, up), (1, rows + 1, down)):
            one = active(row_in[phase, side].astype(jnp.float32))
            act[at, PAD : PAD + cols] = jnp.where(inside, one, 0.0)
            for k, place, beside in ((0, PAD - 1, left), (1, PAD + cols, right)):
                one = active(corner_in[phase, 2 * side + k])
                both = jnp.logical_and(inside, beside)
                act[at, place : place + 1] = jnp.where(both, one, 0.0)
        for dj in range(3):
            start = PAD - 1 + dj
            for r in range(rows + 2):
                shifted[dj, r] = act[r, start : start + cols].astype(jnp.bfloat16)

    def conv(weight):
        result = None
        for di in range(3):
            for dj in range(3):
                tap = 3 * di + dj
                lhs = shifted[dj, di : di + rows].reshape(n, C)
                one = nn_dot(lhs, weight[tap * C : (tap + 1) * C])
                result = one if result is None else result + one
        return result

    with jax.named_scope("stats0"):
        latent_copy.wait()
        put_stats(0, lat_ref[...].astype(jnp.float32).reshape(n, C))
    with jax.named_scope("barrier"):
        pl.semaphore_wait(barrier, total - 1)
    with jax.named_scope("send0"):
        plan = halo_plan(0, lat_ref.at[0], lat_ref.at[rows - 1])
        stats_start(0)
        put_columns(0, lat_ref[...].astype(jnp.float32))
        halo_start(0, plan)
    with jax.named_scope("halo0"):
        halo_finish(0, plan)
    with jax.named_scope("norm0"):
        for copy in vectors:
            copy.wait()
        stats_finish(0, n1g, n1s)
    with jax.named_scope("act0"):
        activate(0, lambda r: lat_ref[r].astype(jnp.float32))
    with jax.named_scope("w0"):
        weights[0].wait()
    with jax.named_scope("conv0"):
        hid[...] = (conv(w1) + c1b[...]).reshape(rows, cols, C)

    with jax.named_scope("stats1"):
        put_stats(1, hid[...].reshape(n, C))
    with jax.named_scope("send1"):
        plan = halo_plan(1, row_out.at[0], row_out.at[1])
        stats_start(1)
        row_out[0] = hid[0].astype(jnp.bfloat16)
        row_out[1] = hid[rows - 1].astype(jnp.bfloat16)
        put_columns(1, hid[...])
        halo_start(1, plan)
    with jax.named_scope("halo1"):
        halo_finish(1, plan)
    with jax.named_scope("norm1"):
        stats_finish(1, n2g, n2s)
    with jax.named_scope("act1"):
        activate(1, lambda r: hid[r])
    with jax.named_scope("conv1"):
        weights[1].wait()
        res[...] = (
            lat_ref[...].astype(jnp.float32).reshape(n, C) + (conv(w2) + c2b[...])
        ).astype(jnp.bfloat16)

    with jax.named_scope("stats2"):
        put_stats(2, res[...].astype(jnp.float32))
        stats_start(2)

    def piece(ref, ch):
        return ref.at[pl.ds(ch * (n // CHUNKS), n // CHUNKS)]

    def z_copy(source, src, way, distance, ch):
        return remote(
            piece(src, ch),
            piece(kv.at[0, source], ch),
            z_send.at[way, distance, ch],
            z_recv.at[source, ch],
            (tile, head + (1 if way else -1) * (distance if distance <= DIRECT else 1)),
        )

    def reachable(way, distance):
        return head + distance < heads if way else head - distance >= 0

    at_end = jnp.logical_or(head == 0, head == heads - 1)

    def straight(fn):
        nearer = [(1, ch) for ch in range(CHUNKS)]
        farther = [(d, ch) for d in range(2, min(DIRECT, heads - 1) + 1) for ch in range(CHUNKS)]
        for chosen, order in ((at_end, interleaved(farther, nearer)), (~at_end, farther + nearer)):
            for distance, ch in order:
                for way in (0, 1):

                    @pl.when(jnp.logical_and(reachable(way, distance), chosen))
                    def _(way=way, distance=distance, ch=ch):
                        fn(z_copy(head, res, way, distance, ch))

    def onward(distance, fn, chunks=tuple(range(CHUNKS))):
        for ch in chunks:
            for way in (0, 1):

                @pl.when(jnp.logical_and(reachable(1 - way, distance), reachable(way, 1)))
                def _(way=way, ch=ch):
                    source = head + (-distance if way else distance)
                    fn(z_copy(source, kv.at[0, source], way, distance + 1, ch))

    def z_arrived(source, distance, way, ch):
        def wait():
            z_copy(source, res, way, 1, ch).wait_recv()

        if heads - 1 > DIRECT:
            passed = jnp.logical_and(distance >= DIRECT, reachable(1 - way, 1))
            pl.when(jnp.logical_not(passed))(wait)
        else:
            wait()

    def c_copy(source, src, ch):
        return remote(
            piece(src, ch),
            piece(kv.at[1, source], ch),
            c_send.at[source, ch],
            c_recv.at[source, ch],
            partner,
        )

    def q_copy(j):
        return remote(
            res, qn.at[j], q_send.at[j], q_recv.at[j], (fellow(j), head)
        )

    def q_begin(j, carry):
        q_copy(j).start()
        return carry

    for ch in range(CHUNKS):
        c_copy(head, res, ch).start()

    def pass_on(ch):
        def go(copy):
            copy.wait_recv()
            copy.start()

        with jax.named_scope("relay"):
            for distance in range(DIRECT, heads - 1):
                onward(distance, go, (ch,))

    straight(lambda copy: copy.start())
    lax.fori_loop(1, half, q_begin, 0)
    pass_on(0)
    pass_on(1)
    with jax.named_scope("norm2"):
        stats_finish(2, n3g, n3s)
        for copy in weights[2:]:
            copy.wait()

    def normed(values):
        return normalize(values.astype(jnp.float32)).astype(jnp.bfloat16)

    scale = LOG2E / C**0.5

    def make_query(pair, at, source):
        query = (nn_dot(normed(source), wp[0]) + qb[...]).astype(jnp.bfloat16)
        qp[pair, :, at * n : (at + 1) * n] = (nt_dot(wp[1], query) * scale).astype(jnp.bfloat16)

    def clear(pair):
        top[pair] = jnp.full((1, 2 * n), -jnp.inf, jnp.float32)
        low[pair] = jnp.zeros((1, 2 * n), jnp.float32)
        acc[pair] = jnp.zeros((C, 2 * n), jnp.float32)

    def prepare(core, source, values):
        keys = normed(values)
        kn[source, core] = keys
        kt[source, :, core * n : (core + 1) * n] = jnp.transpose(keys)

    def one_core(core, source):
        return kn.at[source, core], kt.at[source, :, pl.ds(core * n, n)]

    def both_cores(source):
        return kn.at[source], kt.at[source]

    def attend(pair, *blocks):
        query = qp[pair]
        scores = [nn_dot(keys[...].reshape(-1, C), query) for keys, _ in blocks]
        before = top[pair]
        peak = before
        for one in scores:
            peak = jnp.maximum(peak, jnp.max(one, axis=0, keepdims=True))
        fade = jnp.exp2(before - peak)
        sums, values = low[pair] * fade, None
        for one, (_, turned) in zip(scores, blocks):
            expo = jnp.exp2(one - peak).astype(jnp.bfloat16)
            sums = sums + jnp.sum(expo.astype(jnp.float32), axis=0, keepdims=True)
            part = nn_dot(turned[...], expo)
            values = part if values is None else values + part
        top[pair] = peak
        low[pair] = sums
        acc[pair] = acc[pair] * fade + values

    def columns(fn, distances, chosen=None):
        for distance in distances:
            for way in (0, 1):
                present = reachable(way, distance)
                if chosen is not None:
                    present = jnp.logical_and(present, chosen)

                @pl.when(present)
                def _(distance=distance, way=way):
                    fn(head + (distance if way else -distance), distance, way)

    far = tuple(range(2, heads))

    with jax.named_scope("query0"):
        clear(0)
        make_query(0, 0, res[...])
        prepare(0, head, res[...])
    with jax.named_scope("q_wait0"):
        q_copy(1).wait()
    pass_on(2)
    with jax.named_scope("query1"):
        make_query(0, 1, qn[1])
        for ch in range(CHUNKS):
            c_copy(head, res, ch).wait()
        prepare(1, head, kv[1, head])
    pass_on(3)
    with jax.named_scope("attend_own"):
        attend(0, both_cores(head))

    def begin(source, distance, way):
        with jax.named_scope("z_wait"):
            for ch in range(CHUNKS):
                z_arrived(source, distance, way, ch)
                c_copy(source, kv.at[0, source], ch).start()
        with jax.named_scope("prepare0"):
            prepare(0, source, kv[0, source])

    def second(source):
        with jax.named_scope("c_wait"):
            for ch in range(CHUNKS):
                c_copy(source, kv.at[0, source], ch).wait()
        with jax.named_scope("prepare1"):
            prepare(1, source, kv[1, source])

    def other_pairs(*blocks):
        def one(pair, carry):
            attend(pair, *blocks)
            return carry

        if pairs == 2:
            attend(1, *blocks)
        else:
            lax.fori_loop(1, pairs, one, 0)

    def together(source, distance, way):
        second(source)
        with jax.named_scope("together"):
            other_pairs(both_cores(source))

    def own(source, distance, way):
        with jax.named_scope("own_far"):
            attend(0, both_cores(source))

    columns(begin, (1,), at_end)

    def rest(pair, carry):
        with jax.named_scope("q_wait1"):
            for at in range(2):
                q_copy(2 * pair + at).wait()
        with jax.named_scope("query2"):
            clear(pair)
            for at in range(2):
                make_query(pair, at, qn[2 * pair + at])
        return carry

    lax.fori_loop(1, pairs, rest, 0)
    columns(begin, (2,), ~at_end)
    with jax.named_scope("attend_rest"):
        other_pairs(both_cores(head))
    columns(begin, (2,), at_end)
    columns(together, (1,), at_end)
    columns(together, (2,))

    def apart(*places):
        sources = [source for source, _, _ in places]
        for place in places:
            begin(*place)
        with jax.named_scope("late0"):
            other_pairs(*[one_core(0, source) for source in sources])
        for source in sources:
            second(source)
        with jax.named_scope("late1"):
            other_pairs(*[one_core(1, source) for source in sources])

    @pl.when(~at_end)
    def _():
        apart((head - 1, 1, 0), (head + 1, 1, 1))

    columns(lambda *place: apart(place), far[1:])

    def both(src, dst, src_level, dst_level, sem, device):
        return [
            remote(src, dst, o_send.at[sem], o_recv.at[sem], device),
            remote(src_level, dst_level, l_send.at[sem], l_recv.at[sem], device),
        ]

    def give_copies(j):
        return both(o_out.at[j], o_in.at[j], l_out.at[j], l_in.at[j], j, (lender(j), head))

    def finish(pair, at, o_to, l_to):
        for part in range(2):
            lanes = slice((2 * at + part) * (n // 2), (2 * at + part + 1) * (n // 2))
            sums = low[pair, :, lanes]
            l_to[2 * pair + at, part] = top[pair, :, lanes] + jnp.log2(sums)
            o_to[2 * pair + at, part] = (acc[pair, :, lanes] * (1.0 / sums)).astype(jnp.bfloat16)

    def column_sent():
        straight(lambda copy: copy.wait_send())
        for distance in range(DIRECT, heads - 1):
            onward(distance, lambda copy: copy.wait_send())

    def begin_all(copies):
        for copy in copies:
            copy.start()

    def end_all(copies):
        for copy in copies:
            copy.wait()

    if half == 4:
        def hop(part):
            via = (fellow(2 - part), head)
            return both(
                o_out.at[3, part], u_in.at[part], l_out.at[3, part], ul_in.at[part], part, via
            )

        def direct(j):
            part = 2 - j
            return both(
                o_out.at[j, part],
                o_in.at[j, part],
                l_out.at[j, part],
                l_in.at[j, part],
                1 + j,
                (fellow(j), head),
            )

        def merged(j):
            part = j - 1
            return both(
                m_out.at[part],
                o_in.at[j, part],
                ml_out.at[part],
                l_in.at[j, part],
                3 + j,
                (fellow(j), head),
            )

        def merge(j):
            part = j - 1
            end_all(hop(part))
            mine, theirs = l_out[j, part], ul_in[part]
            level = jnp.maximum(mine, theirs)
            keep, add = jnp.exp2(mine - level), jnp.exp2(theirs - level)
            whole = keep + add
            ml_out[part] = level + jnp.log2(whole)
            values = o_out[j, part].astype(jnp.float32) * (keep / whole)
            values = values + u_in[part].astype(jnp.float32) * (add / whole)
            m_out[part] = values.astype(jnp.bfloat16)
            begin_all(merged(j))

        with jax.named_scope("give"):
            finish(1, 1, o_out, l_out)
            begin_all(hop(0))
            begin_all(hop(1))
            finish(1, 0, o_out, l_out)
            begin_all(direct(2))
        columns(own, tuple(range(1, heads)))
        with jax.named_scope("give1"):
            finish(0, 1, o_out, l_out)
            begin_all(direct(1))
        with jax.named_scope("finish0"):
            finish(0, 0, o_in, l_in)
            column_sent()
        with jax.named_scope("merge2"):
            merge(2)
        with jax.named_scope("merge1"):
            merge(1)
        with jax.named_scope("take"):
            for j in (1, 2):
                end_all(direct(j))
                end_all(merged(j))
        parts = 3
    else:

        def give(i, carry):
            pair = pairs - 1 - i
            for at in range(2):
                finish(pair, at, o_out, l_out)
                begin_all(give_copies(2 * pair + at))
            return carry

        def take(j, carry):
            end_all(give_copies(j))
            return carry

        lax.fori_loop(0, pairs - 1, give, 0)
        columns(own, tuple(range(1, heads)))
        finish(0, 1, o_out, l_out)
        begin_all(give_copies(1))
        finish(0, 0, o_in, l_in)
        column_sent()
        lax.fori_loop(1, half, take, 0)
        parts = half
    with jax.named_scope("last"):
        sides = []
        for part in range(2):
            peak = l_in[0, part]
            for j in range(1, parts):
                peak = jnp.maximum(peak, l_in[j, part])
            shares = [jnp.exp2(l_in[j, part] - peak) for j in range(parts)]
            whole = shares[0]
            for j in range(1, parts):
                whole = whole + shares[j]
            side = jnp.zeros((C, n // 2), jnp.float32)
            for j in range(parts):
                side = side + (shares[j] / whole) * o_in[j, part].astype(jnp.float32)
            sides.append(side)
        mixed = jnp.concatenate(sides, axis=1)
        mixed = jnp.transpose(mixed.astype(jnp.bfloat16))
        attended = (nn_dot(mixed, wp[2]) + vb[...]).astype(jnp.bfloat16)
        out = nn_dot(attended, wp[3]) + ob[...]
        out_ref[...] = (res[...].astype(jnp.float32) + out).astype(jnp.bfloat16)


def per_device(
    latent,
    norm1_gain,
    norm1_shift,
    conv1_weight,
    conv1_bias,
    norm2_gain,
    norm2_shift,
    conv2_weight,
    conv2_bias,
    norm3_gain,
    norm3_shift,
    query_weight,
    query_bias,
    key_weight,
    value_weight,
    value_bias,
    out_weight,
    out_bias,
):
    rows, cols, _ = latent.shape
    tiles, heads = lax.axis_size("tile"), lax.axis_size("head")
    n = rows * cols
    total = tiles * heads
    half = tiles // 2
    vectors = [
        v.reshape(1, C)
        for v in (
            norm1_gain,
            norm1_shift,
            conv1_bias,
            norm2_gain,
            norm2_shift,
            conv2_bias,
            norm3_gain,
            norm3_shift,
            query_bias,
            value_bias,
            out_bias,
        )
    ]
    matrices = [
        conv1_weight.reshape(9 * C, C),
        conv2_weight.reshape(9 * C, C),
        query_weight,
        key_weight,
        value_weight,
        out_weight,
    ]
    bf16, f32 = jnp.bfloat16, jnp.float32
    dma = pltpu.SemaphoreType.DMA
    out = pl.pallas_call(
        functools.partial(block_kernel, tiles, heads),
        out_shape=pltpu.VMEM((n, C), bf16),
        in_specs=[HBM] * (1 + len(vectors) + len(matrices)),
        out_specs=VMEM,
        scratch_shapes=[
            pltpu.VMEM((rows, cols, C), bf16),
            pltpu.VMEM((len(vectors), 1, C), f32),
            pltpu.VMEM((9 * C, C), bf16),
            pltpu.VMEM((9 * C, C), bf16),
            pltpu.VMEM((4, C, C), bf16),
            pltpu.VMEM((rows + 2, cols + 2 * PAD, C), f32),
            pltpu.VMEM((3, rows + 2, cols, C), bf16),
            pltpu.VMEM((rows, cols, C), f32),
            pltpu.VMEM((2, 2, cols, C), bf16),
            pltpu.VMEM((2, cols, C), bf16),
            pltpu.VMEM((2, 2, rows, 1, C), f32),
            pltpu.VMEM((2, 2, rows, 1, C), f32),
            pltpu.VMEM((2, 4, 1, C), f32),
            pltpu.VMEM((3, 1, LANES), f32),
            pltpu.VMEM((3, total, 1, LANES), f32),
            pltpu.VMEM((8, C), f32),
            pltpu.VMEM((n, C), bf16),
            pltpu.VMEM((2, heads, n, C), bf16),
            pltpu.VMEM((heads, 2, n, C), bf16),
            pltpu.VMEM((heads, C, 2 * n), bf16),
            pltpu.VMEM((half, n, C), bf16),
            pltpu.VMEM((half // 2, C, 2 * n), bf16),
            pltpu.VMEM((half // 2, C, 2 * n), f32),
            pltpu.VMEM((half // 2, 1, 2 * n), f32),
            pltpu.VMEM((half // 2, 1, 2 * n), f32),
            pltpu.VMEM((half, 2, C, n // 2), bf16),
            pltpu.VMEM((half, 2, C, n // 2), bf16),
            pltpu.VMEM((half, 2, 1, n // 2), f32),
            pltpu.VMEM((half, 2, 1, n // 2), f32),
            pltpu.VMEM((2, C, n // 2), bf16),
            pltpu.VMEM((2, 1, n // 2), f32),
            pltpu.VMEM((2, C, n // 2), bf16),
            pltpu.VMEM((2, 1, n // 2), f32),
            dma,
            dma((len(vectors),)),
            dma((len(matrices),)),
            dma((3,)),
            dma((3,)),
            dma((2, 8)),
            dma((2, 8)),
            dma((2, heads, CHUNKS)),
            dma((heads, CHUNKS)),
            dma((heads, CHUNKS)),
            dma((heads, CHUNKS)),
            dma((half,)),
            dma((half,)),
            dma((half + 2,)),
            dma((half + 2,)),
            dma((half + 2,)),
            dma((half + 2,)),
        ],
        compiler_params=pltpu.CompilerParams(
            collective_id=1, has_side_effects=True, vmem_limit_bytes=VMEM_LIMIT
        ),
        name="middle_block",
    )(latent, *vectors, *matrices)
    return out.reshape(rows, cols, C)


def solution(mesh):
    return jax.shard_map(
        per_device,
        mesh=mesh,
        in_specs=(P("tile", "head", None),) + (P(),) * 17,
        out_specs=P("tile", "head", None),
        check_vma=False,
    )
```

```python
import functools
import math

import jax
import jax.numpy as jnp
from jax import lax
from jax.experimental import pallas as pl
from jax.experimental.pallas import tpu as pltpu
from jax.sharding import PartitionSpec as P

C = 512
GROUPS = 32
WIDTH = C // GROUPS
EPS = 1e-06
LANES = 128
PARTS = C // LANES
SHARE = WIDTH // PARTS
PAD = 8
LOG2E = math.log2(math.e)
MESH = pl.DeviceIdType.MESH
VMEM = pl.BlockSpec(memory_space=pltpu.VMEM)
HBM = pl.BlockSpec(memory_space=pltpu.HBM)
VECTORS = 11
CHUNKS = 4
DIRECT = 2
VMEM_LIMIT = 56 * 1024 * 1024


def interleaved(far, near):
    order, rest, near = far[: len(far) // 2], far[len(far) // 2 :], list(near)
    for place in rest:
        order += near[:1] + [place]
        near = near[1:]
    return order + near


def nt_dot(a, b):
    return lax.dot_general(a, b, (((1,), (1,)), ((), ())), preferred_element_type=jnp.float32)


def nn_dot(a, b):
    return jnp.dot(a, b, preferred_element_type=jnp.float32)


def lane_index(rows):
    return lax.broadcasted_iota(jnp.int32, (rows, LANES), 1)


def lane_partner(values, step):
    below = pltpu.roll(values, step, 1)
    above = pltpu.roll(values, LANES - step, 1)
    return jnp.where(lane_index(values.shape[0]) % (2 * step) >= step, below, above)


def group_sum(values):
    step = 1
    while step < WIDTH:
        values = values + lane_partner(values, step)
        step *= 2
    return values


def fold(row):
    return jnp.concatenate([row[:, i * LANES : (i + 1) * LANES] for i in range(PARTS)], axis=0)


def unfold(rows):
    return jnp.concatenate([rows[i : i + 1] for i in range(PARTS)], axis=1)


def local_stats(values):
    count = values.shape[0]
    mean = jnp.sum(values, axis=0, keepdims=True) / count
    deviation = values - mean
    square = jnp.sum(deviation * deviation, axis=0, keepdims=True)
    group_mean, square = fold(mean), fold(square)
    step = 1
    while step < WIDTH:
        other = lane_partner(group_mean, step)
        gap = group_mean - other
        square = square + lane_partner(square, step) + (0.5 * count * step) * (gap * gap)
        group_mean = 0.5 * (group_mean + other)
        step *= 2
    lane = lane_index(1)
    packed = jnp.zeros((1, LANES), jnp.float32)
    for i in range(PARTS):
        one = jnp.where(lane % 2 == 0, group_mean[i : i + 1], square[i : i + 1])
        packed = jnp.where((lane % WIDTH) // SHARE == i, one, packed)
    return packed


def merged_stats(slots, count):
    total = slots.shape[0]
    sums = jnp.sum(slots, axis=0)
    mean = sums / total
    gap = slots - mean[None]
    spread = jnp.sum(gap * gap, axis=0)
    variance = (sums + count * pltpu.roll(spread, 1, 1)) / (total * count)
    lane = lane_index(1)
    both = jnp.where(lane % 2 == 0, mean, lax.rsqrt(variance + EPS))
    row = lax.broadcasted_iota(jnp.int32, (2 * PARTS, LANES), 0)
    want = (row % PARTS) * SHARE + row // PARTS
    wide = jnp.where(lane_index(2 * PARTS) % WIDTH == want, both, 0.0)
    wide = group_sum(wide)
    return unfold(wide[:PARTS]), unfold(wide[PARTS:])


def silu_of_double(values):
    return values + values * jnp.tanh(values)


def block_kernel(
    tiles,
    heads,
    lat_hbm,
    *refs,
):
    vec_hbm, mat_hbm, refs = refs[:VECTORS], refs[VECTORS : VECTORS + 6], refs[VECTORS + 6 :]
    (
        out_ref,
        lat_ref,
        vec,
        w1,
        w2,
        wp,
        act,
        shifted,
        hid,
        row_in,
        row_out,
        col_in,
        col_out,
        corner_in,
        stat_out,
        stat_in,
        norm,
        res,
        kv,
        kn,
        kt,
        qn,
        qp,
        acc,
        top,
        low,
        o_out,
        o_in,
        l_out,
        l_in,
        u_in,
        ul_in,
        m_out,
        ml_out,
        lat_sem,
        v_sem,
        w_sem,
        s_send,
        s_recv,
        h_send,
        h_recv,
        z_send,
        z_recv,
        c_send,
        c_recv,
        q_send,
        q_recv,
        o_send,
        o_recv,
        l_send,
        l_recv,
    ) = refs
    rows, cols, _ = lat_ref.shape
    n = rows * cols
    total = tiles * heads
    half = tiles // 2
    pairs = half // 2
    tile, head = lax.axis_index("tile"), lax.axis_index("head")
    me = tile * heads + head
    partner = (tile + 1 - 2 * lax.rem(tile, 2), head)

    def fellow(j):
        chip, bit, other = lax.div(tile, 2), 1, 0
        if half & (half - 1):
            return lax.rem(tile + 2 * j, tiles)
        while bit < half:
            mine, flip = lax.rem(lax.div(chip, bit), 2), (j // bit) % 2
            other = other + bit * (mine + flip - 2 * mine * flip)
            bit *= 2
        return 2 * other + lax.rem(tile, 2)

    def lender(j):
        return fellow(j) if half & (half - 1) == 0 else lax.rem(tile + tiles - 2 * j, tiles)

    barrier = pltpu.get_barrier_semaphore()

    def greet(k, carry):
        peer = lax.rem(me + k, total)
        pl.semaphore_signal(
            barrier, inc=1, device_id=(lax.div(peer, heads), lax.rem(peer, heads)), device_id_type=MESH
        )
        return carry

    latent_copy = pltpu.make_async_copy(lat_hbm, lat_ref, lat_sem)
    latent_copy.start()
    lax.fori_loop(1, total, greet, 0)
    vectors = [
        pltpu.make_async_copy(src, vec.at[i], v_sem.at[i]) for i, src in enumerate(vec_hbm)
    ]
    targets = [w1, w2] + [wp.at[i] for i in range(4)]
    weights = [
        pltpu.make_async_copy(src, dst, w_sem.at[i])
        for i, (src, dst) in enumerate(zip(mat_hbm, targets))
    ]
    for copy in vectors + weights:
        copy.start()
    n1g, n1s, c1b, n2g, n2s, c2b, n3g, n3s, qb, vb, ob = [vec.at[i] for i in range(VECTORS)]

    def remote(src, dst, send, recv, device):
        return pltpu.make_async_remote_copy(
            src_ref=src,
            dst_ref=dst,
            send_sem=send,
            recv_sem=recv,
            device_id=device,
            device_id_type=MESH,
        )

    def stat_copy(phase, k):
        peer = lax.rem(me + k, total)
        return remote(
            stat_out.at[phase],
            stat_in.at[phase, k],
            s_send.at[phase],
            s_recv.at[phase],
            (lax.div(peer, heads), lax.rem(peer, heads)),
        )

    def stats_start(phase):
        def begin(k, carry):
            stat_copy(phase, k).start()
            return carry

        lax.fori_loop(1, total, begin, 0)

    def stats_finish(phase, gain, shift):
        others = stat_in.at[phase, pl.ds(1, total - 1)]
        for sem in (s_send, s_recv):
            pltpu.make_async_copy(others, others, sem.at[phase]).wait()
        mean, inverse = merged_stats(stat_in[phase], n * WIDTH)
        norm[0:1] = inverse * gain[...]
        norm[1:2] = shift[...] - mean * (inverse * gain[...])

    def put_stats(phase, values):
        packed = local_stats(values)
        stat_out[phase] = packed
        stat_in[phase, 0] = packed

    def normalize(values):
        return values * norm[0:1] + norm[1:2]

    def halo_plan(phase, first_row, last_row):
        first, last = col_out.at[phase, 0], col_out.at[phase, 1]
        plan = [
            (first_row, row_in.at[phase, 1], -1, 0),
            (last_row, row_in.at[phase, 0], 1, 0),
            (first, col_in.at[phase, 1], 0, -1),
            (last, col_in.at[phase, 0], 0, 1),
            (first.at[0], corner_in.at[phase, 3], -1, -1),
            (last.at[0], corner_in.at[phase, 2], -1, 1),
            (first.at[rows - 1], corner_in.at[phase, 1], 1, -1),
            (last.at[rows - 1], corner_in.at[phase, 0], 1, 1),
        ]
        return plan

    def there(dt, dh):
        inside = None
        for place, delta, size in ((tile, dt, tiles), (head, dh, heads)):
            if delta:
                one = place + delta < size if delta > 0 else place + delta >= 0
                inside = one if inside is None else jnp.logical_and(inside, one)
        return inside

    def halo_copy(phase, i, src, dst, dt, dh):
        return remote(
            src, dst, h_send.at[phase, i], h_recv.at[phase, i], (tile + dt, head + dh)
        )

    def halo_start(phase, plan):
        for i, (src, dst, dt, dh) in enumerate(plan):

            @pl.when(there(dt, dh))
            def _(i=i, src=src, dst=dst, dt=dt, dh=dh):
                halo_copy(phase, i, src, dst, dt, dh).start()

    def halo_finish(phase, plan):
        for i, (src, dst, dt, dh) in enumerate(plan):

            @pl.when(there(dt, dh))
            def _(i=i, src=src, dst=dst, dt=dt, dh=dh):
                halo_copy(phase, i, src, dst, dt, dh).wait_send()

            @pl.when(there(-dt, -dh))
            def _(i=i, src=src, dst=dst, dt=dt, dh=dh):
                halo_copy(phase, i, src, dst, dt, dh).wait_recv()

    def put_columns(phase, values):
        for r in range(rows):
            col_out[phase, 0, r] = values[r, 0:1]
            col_out[phase, 1, r] = values[r, cols - 1 : cols]

    def activate(phase, values):
        left, right = head > 0, head < heads - 1
        up, down = tile > 0, tile < tiles - 1

        slope, level = 0.5 * norm[0:1], 0.5 * norm[1:2]

        def active(x):
            return silu_of_double(x * slope + level)

        for r in range(rows):
            one = active(values(r))
            act[1 + r, PAD : PAD + cols] = one
            shifted[1, 1 + r] = one.astype(jnp.bfloat16)
            for side, at, inside in ((0, PAD - 1, left), (1, PAD + cols, right)):
                one = active(col_in[phase, side, r])
                act[1 + r, at : at + 1] = jnp.where(inside, one, 0.0)
        for side, at, inside in ((0, 0, up), (1, rows + 1, down)):
            one = active(row_in[phase, side].astype(jnp.float32))
            one = jnp.where(inside, one, 0.0)
            act[at, PAD : PAD + cols] = one
            shifted[1, at] = one.astype(jnp.bfloat16)
            for k, place, beside in ((0, PAD - 1, left), (1, PAD + cols, right)):
                one = active(corner_in[phase, 2 * side + k])
                both = jnp.logical_and(inside, beside)
                act[at, place : place + 1] = jnp.where(both, one, 0.0)
        for dj in (0, 2):
            start = PAD - 1 + dj
            for r in range(rows + 2):
                shifted[dj, r] = act[r, start : start + cols].astype(jnp.bfloat16)

    def conv(weight, first=0, many=rows):
        result = None
        for di in range(3):
            for dj in range(3):
                tap = 3 * di + dj
                lhs = shifted[dj, first + di : first + di + many].reshape(many * cols, C)
                one = nn_dot(lhs, weight[tap * C : (tap + 1) * C])
                result = one if result is None else result + one
        return result

    with jax.named_scope("stats0"):
        latent_copy.wait()
        put_stats(0, lat_ref[...].astype(jnp.float32).reshape(n, C))
    with jax.named_scope("barrier"):
        pl.semaphore_wait(barrier, total - 1)
    with jax.named_scope("send0"):
        plan = halo_plan(0, lat_ref.at[0], lat_ref.at[rows - 1])
        stats_start(0)
        put_columns(0, lat_ref[...].astype(jnp.float32))
        halo_start(0, plan)
    with jax.named_scope("halo0"):
        halo_finish(0, plan)
    with jax.named_scope("norm0"):
        for copy in vectors:
            copy.wait()
        stats_finish(0, n1g, n1s)
    with jax.named_scope("act0"):
        activate(0, lambda r: lat_ref[r].astype(jnp.float32))
    with jax.named_scope("w0"):
        weights[0].wait()
    with jax.named_scope("conv0"):
        hid[...] = (conv(w1) + c1b[...]).reshape(rows, cols, C)

    with jax.named_scope("stats1"):
        put_stats(1, hid[...].reshape(n, C))
    with jax.named_scope("send1"):
        plan = halo_plan(1, row_out.at[0], row_out.at[1])
        stats_start(1)
        row_out[0] = hid[0].astype(jnp.bfloat16)
        row_out[1] = hid[rows - 1].astype(jnp.bfloat16)
        put_columns(1, hid[...])
        halo_start(1, plan)
    with jax.named_scope("halo1"):
        halo_finish(1, plan)
    with jax.named_scope("norm1"):
        stats_finish(1, n2g, n2s)
    with jax.named_scope("act1"):
        activate(1, lambda r: hid[r])
    with jax.named_scope("conv1"):
        weights[1].wait()

    def residual(r):
        with jax.named_scope("conv1"):
            new = lat_ref[r].astype(jnp.float32) + (conv(w2, r, 1) + c2b[...])
            res[r * cols : (r + 1) * cols] = new.astype(jnp.bfloat16)

    def piece(ref, ch):
        return ref.at[pl.ds(ch * (n // CHUNKS), n // CHUNKS)]

    def z_copy(source, src, way, distance, ch):
        return remote(
            piece(src, ch),
            piece(kv.at[0, source], ch),
            z_send.at[way, distance, ch],
            z_recv.at[source, ch],
            (tile, head + (1 if way else -1) * (distance if distance <= DIRECT else 1)),
        )

    def reachable(way, distance):
        return head + distance < heads if way else head - distance >= 0

    at_end = jnp.logical_or(head == 0, head == heads - 1)

    def straight(fn, opening=None):
        nearer = [(1, ch) for ch in range(CHUNKS)]
        farther = [(d, ch) for d in range(2, min(DIRECT, heads - 1) + 1) for ch in range(CHUNKS)]
        for chosen, order in ((at_end, interleaved(farther, nearer)), (~at_end, farther + nearer)):
            for distance, ch in order:
                for way in (0, 1):
                    present = jnp.logical_and(reachable(way, distance), chosen)
                    if opening is not None:
                        opens = ch == 0 and distance <= 2
                        if opens and distance == 1:
                            alone = ~reachable(way, 2)
                            present = jnp.logical_and(present, alone if opening else ~alone)
                        elif opens != opening:
                            continue

                    @pl.when(present)
                    def _(way=way, distance=distance, ch=ch):
                        fn(z_copy(head, res, way, distance, ch))

    def onward(distance, fn, chunks=tuple(range(CHUNKS))):
        for ch in chunks:
            for way in (0, 1):

                @pl.when(jnp.logical_and(reachable(1 - way, distance), reachable(way, 1)))
                def _(way=way, ch=ch):
                    source = head + (-distance if way else distance)
                    fn(z_copy(source, kv.at[0, source], way, distance + 1, ch))

    def z_arrived(source, distance, way, ch):
        def wait():
            z_copy(source, res, way, 1, ch).wait_recv()

        if heads - 1 > DIRECT:
            passed = jnp.logical_and(distance >= DIRECT, reachable(1 - way, 1))
            pl.when(jnp.logical_not(passed))(wait)
        else:
            wait()

    def c_copy(source, src, ch):
        return remote(
            piece(src, ch),
            piece(kv.at[1, source], ch),
            c_send.at[source, ch],
            c_recv.at[source, ch],
            partner,
        )

    def q_copy(j, part):
        rows_of = pl.ds(0, n // 4) if part == 0 else pl.ds(n // 4, n - n // 4)
        return remote(
            res.at[rows_of],
            qn.at[j, rows_of],
            q_send.at[j, part],
            q_recv.at[j, part],
            (fellow(j), head),
        )

    residual(0)
    straight(lambda copy: copy.start(), True)
    for j in (1, 2):
        if j < half:
            q_copy(j, 0).start()
    for r in range(1, rows):
        residual(r)
    for ch in range(CHUNKS):
        c_copy(head, res, ch).start()
    with jax.named_scope("stats2"):
        put_stats(2, res[...].astype(jnp.float32))
        stats_start(2)

    def pass_on(ch):
        def go(copy):
            copy.wait_recv()
            copy.start()

        with jax.named_scope("relay"):
            for distance in range(DIRECT, heads - 1):
                onward(distance, go, (ch,))

    straight(lambda copy: copy.start(), False)
    for j in (1, 2):
        if j < half:
            q_copy(j, 1).start()

    def q_begin(j, carry):
        for part in range(2):
            q_copy(j, part).start()
        return carry

    lax.fori_loop(3, half, q_begin, 0)
    pass_on(0)
    pass_on(1)
    with jax.named_scope("norm2"):
        stats_finish(2, n3g, n3s)
        for copy in weights[2:]:
            copy.wait()

    def normed(values):
        return normalize(values.astype(jnp.float32)).astype(jnp.bfloat16)

    scale = LOG2E / C**0.5

    def make_query(pair, at, source):
        query = (nn_dot(normed(source), wp[0]) + qb[...]).astype(jnp.bfloat16)
        qp[pair, :, at * n : (at + 1) * n] = (nt_dot(wp[1], query) * scale).astype(jnp.bfloat16)

    def clear(pair):
        top[pair] = jnp.full((1, 2 * n), -jnp.inf, jnp.float32)
        low[pair] = jnp.zeros((1, 2 * n), jnp.float32)
        acc[pair] = jnp.zeros((C, 2 * n), jnp.float32)

    def prepare(core, source, values):
        keys = normed(values)
        kn[source, core] = keys
        kt[source, :, core * n : (core + 1) * n] = jnp.transpose(keys)

    def one_core(core, source):
        return kn.at[source, core], kt.at[source, :, pl.ds(core * n, n)]

    def both_cores(source):
        return kn.at[source], kt.at[source]

    def attend(pair, *blocks):
        query = qp[pair]
        scores = [nn_dot(keys[...].reshape(-1, C), query) for keys, _ in blocks]
        before = top[pair]
        peak = before
        for one in scores:
            peak = jnp.maximum(peak, jnp.max(one, axis=0, keepdims=True))
        fade = jnp.exp2(before - peak)
        sums, values = low[pair] * fade, None
        for one, (_, turned) in zip(scores, blocks):
            expo = jnp.exp2(one - peak)
            sums = sums + jnp.sum(expo, axis=0, keepdims=True)
            part = nn_dot(turned[...], expo.astype(jnp.bfloat16))
            values = part if values is None else values + part
        top[pair] = peak
        low[pair] = sums
        acc[pair] = acc[pair] * fade + values

    def columns(fn, distances, chosen=None):
        for distance in distances:
            for way in (0, 1):
                present = reachable(way, distance)
                if chosen is not None:
                    present = jnp.logical_and(present, chosen)

                @pl.when(present)
                def _(distance=distance, way=way):
                    fn(head + (distance if way else -distance), distance, way)

    far = tuple(range(2, heads))

    with jax.named_scope("query0"):
        clear(0)
        make_query(0, 0, res[...])
        prepare(0, head, res[...])
    with jax.named_scope("q_wait0"):
        for part in range(2):
            q_copy(1, part).wait()
    pass_on(2)
    with jax.named_scope("query1"):
        make_query(0, 1, qn[1])
        for ch in range(CHUNKS):
            c_copy(head, res, ch).wait()
        prepare(1, head, kv[1, head])
    pass_on(3)
    with jax.named_scope("attend_own"):
        attend(0, both_cores(head))

    def begin(source, distance, way):
        with jax.named_scope("z_wait"):
            for ch in range(CHUNKS):
                z_arrived(source, distance, way, ch)
                c_copy(source, kv.at[0, source], ch).start()
        with jax.named_scope("prepare0"):
            prepare(0, source, kv[0, source])

    def second(source):
        with jax.named_scope("c_wait"):
            for ch in range(CHUNKS):
                c_copy(source, kv.at[0, source], ch).wait()
        with jax.named_scope("prepare1"):
            prepare(1, source, kv[1, source])

    def other_pairs(*blocks):
        def one(pair, carry):
            attend(pair, *blocks)
            return carry

        if pairs == 2:
            attend(1, *blocks)
        else:
            lax.fori_loop(1, pairs, one, 0)

    def together(source, distance, way):
        second(source)
        with jax.named_scope("together"):
            other_pairs(both_cores(source))

    def own_pair():
        with jax.named_scope("own_far"):
            attend(0, *[both_cores(lax.rem(head + k, heads)) for k in range(1, heads)])

    columns(begin, (1,), at_end)

    def rest(pair, carry):
        with jax.named_scope("q_wait1"):
            for at in range(2):
                for part in range(2):
                    q_copy(2 * pair + at, part).wait()
        with jax.named_scope("query2"):
            clear(pair)
            for at in range(2):
                make_query(pair, at, qn[2 * pair + at])
        return carry

    lax.fori_loop(1, pairs, rest, 0)
    columns(begin, (2,), ~at_end)
    with jax.named_scope("attend_rest"):
        other_pairs(both_cores(head))
    columns(begin, (2,), at_end)
    columns(together, (1,), at_end)
    columns(together, (2,))

    def apart(*place):
        begin(*place)
        with jax.named_scope("late0"):
            other_pairs(one_core(0, place[0]))
        second(place[0])
        with jax.named_scope("late1"):
            other_pairs(one_core(1, place[0]))

    def two_near(first, last):
        begin(*first)
        with jax.named_scope("late0"):
            other_pairs(one_core(0, first[0]))
        second(first[0])
        begin(*last)
        with jax.named_scope("late01"):
            other_pairs(one_core(1, first[0]), one_core(0, last[0]))
        second(last[0])
        with jax.named_scope("late1"):
            other_pairs(one_core(1, last[0]))

    below, above = (head - 1, 1, 0), (head + 1, 1, 1)
    lower = 2 * head < heads - 1
    pl.when(jnp.logical_and(~at_end, lower))(lambda: two_near(below, above))
    pl.when(jnp.logical_and(~at_end, ~lower))(lambda: two_near(above, below))

    columns(apart, far[1:])

    def both(src, dst, src_level, dst_level, sem, device):
        return [
            remote(src, dst, o_send.at[sem], o_recv.at[sem], device),
            remote(src_level, dst_level, l_send.at[sem], l_recv.at[sem], device),
        ]

    def give_copies(j):
        return both(o_out.at[j], o_in.at[j], l_out.at[j], l_in.at[j], j, (lender(j), head))

    def finish(pair, at, o_to, l_to):
        for part in range(2):
            lanes = slice((2 * at + part) * (n // 2), (2 * at + part + 1) * (n // 2))
            sums = low[pair, :, lanes]
            l_to[2 * pair + at, part] = top[pair, :, lanes] + jnp.log2(sums)
            o_to[2 * pair + at, part] = (acc[pair, :, lanes] * (1.0 / sums)).astype(jnp.bfloat16)

    def column_sent():
        straight(lambda copy: copy.wait_send())
        for distance in range(DIRECT, heads - 1):
            onward(distance, lambda copy: copy.wait_send())

    def begin_all(copies):
        for copy in copies:
            copy.start()

    def end_all(copies):
        for copy in copies:
            copy.wait()

    if half == 4:
        def hop(part):
            via = (fellow(2 - part), head)
            return both(
                o_out.at[3, part], u_in.at[part], l_out.at[3, part], ul_in.at[part], part, via
            )

        def direct(j):
            part = 2 - j
            return both(
                o_out.at[j, part],
                o_in.at[j, part],
                l_out.at[j, part],
                l_in.at[j, part],
                1 + j,
                (fellow(j), head),
            )

        def merged(j):
            part = j - 1
            return both(
                m_out.at[part],
                o_in.at[j, part],
                ml_out.at[part],
                l_in.at[j, part],
                3 + j,
                (fellow(j), head),
            )

        def merge(j):
            part = j - 1
            end_all(hop(part))
            mine, theirs = l_out[j, part], ul_in[part]
            level = jnp.maximum(mine, theirs)
            keep, add = jnp.exp2(mine - level), jnp.exp2(theirs - level)
            whole = keep + add
            ml_out[part] = level + jnp.log2(whole)
            values = o_out[j, part].astype(jnp.float32) * (keep / whole)
            values = values + u_in[part].astype(jnp.float32) * (add / whole)
            m_out[part] = values.astype(jnp.bfloat16)
            begin_all(merged(j))

        with jax.named_scope("give"):
            finish(1, 1, o_out, l_out)
            begin_all(hop(0))
            begin_all(hop(1))
            finish(1, 0, o_out, l_out)
            begin_all(direct(2))
        own_pair()
        with jax.named_scope("give1"):
            finish(0, 1, o_out, l_out)
            begin_all(direct(1))
        with jax.named_scope("finish0"):
            finish(0, 0, o_in, l_in)
            column_sent()
        with jax.named_scope("merge2"):
            merge(2)
        with jax.named_scope("merge1"):
            merge(1)
        with jax.named_scope("take"):
            for j in (1, 2):
                end_all(direct(j))
                end_all(merged(j))
        parts = 3
    else:

        def give(i, carry):
            pair = pairs - 1 - i
            for at in range(2):
                finish(pair, at, o_out, l_out)
                begin_all(give_copies(2 * pair + at))
            return carry

        def take(j, carry):
            end_all(give_copies(j))
            return carry

        lax.fori_loop(0, pairs - 1, give, 0)
        own_pair()
        finish(0, 1, o_out, l_out)
        begin_all(give_copies(1))
        finish(0, 0, o_in, l_in)
        column_sent()
        lax.fori_loop(1, half, take, 0)
        parts = half
    with jax.named_scope("last"):
        sides = []
        for part in range(2):
            peak = l_in[0, part]
            for j in range(1, parts):
                peak = jnp.maximum(peak, l_in[j, part])
            shares = [jnp.exp2(l_in[j, part] - peak) for j in range(parts)]
            whole = shares[0]
            for j in range(1, parts):
                whole = whole + shares[j]
            side = jnp.zeros((C, n // 2), jnp.float32)
            for j in range(parts):
                side = side + (shares[j] / whole) * o_in[j, part].astype(jnp.float32)
            sides.append(side)
        mixed = jnp.concatenate(sides, axis=1)
        mixed = jnp.transpose(mixed.astype(jnp.bfloat16))
        attended = (nn_dot(mixed, wp[2]) + vb[...]).astype(jnp.bfloat16)
        out = nn_dot(attended, wp[3]) + ob[...]
        out_ref[...] = (res[...].astype(jnp.float32) + out).astype(jnp.bfloat16)


def per_device(
    latent,
    norm1_gain,
    norm1_shift,
    conv1_weight,
    conv1_bias,
    norm2_gain,
    norm2_shift,
    conv2_weight,
    conv2_bias,
    norm3_gain,
    norm3_shift,
    query_weight,
    query_bias,
    key_weight,
    value_weight,
    value_bias,
    out_weight,
    out_bias,
):
    rows, cols, _ = latent.shape
    tiles, heads = lax.axis_size("tile"), lax.axis_size("head")
    n = rows * cols
    total = tiles * heads
    half = tiles // 2
    vectors = [
        v.reshape(1, C)
        for v in (
            norm1_gain,
            norm1_shift,
            conv1_bias,
            norm2_gain,
            norm2_shift,
            conv2_bias,
            norm3_gain,
            norm3_shift,
            query_bias,
            value_bias,
            out_bias,
        )
    ]
    matrices = [
        conv1_weight.reshape(9 * C, C),
        conv2_weight.reshape(9 * C, C),
        query_weight,
        key_weight,
        value_weight,
        out_weight,
    ]
    bf16, f32 = jnp.bfloat16, jnp.float32
    dma = pltpu.SemaphoreType.DMA
    out = pl.pallas_call(
        functools.partial(block_kernel, tiles, heads),
        out_shape=pltpu.VMEM((n, C), bf16),
        in_specs=[HBM] * (1 + len(vectors) + len(matrices)),
        out_specs=VMEM,
        scratch_shapes=[
            pltpu.VMEM((rows, cols, C), bf16),
            pltpu.VMEM((len(vectors), 1, C), f32),
            pltpu.VMEM((9 * C, C), bf16),
            pltpu.VMEM((9 * C, C), bf16),
            pltpu.VMEM((4, C, C), bf16),
            pltpu.VMEM((rows + 2, cols + 2 * PAD, C), f32),
            pltpu.VMEM((3, rows + 2, cols, C), bf16),
            pltpu.VMEM((rows, cols, C), f32),
            pltpu.VMEM((2, 2, cols, C), bf16),
            pltpu.VMEM((2, cols, C), bf16),
            pltpu.VMEM((2, 2, rows, 1, C), f32),
            pltpu.VMEM((2, 2, rows, 1, C), f32),
            pltpu.VMEM((2, 4, 1, C), f32),
            pltpu.VMEM((3, 1, LANES), f32),
            pltpu.VMEM((3, total, 1, LANES), f32),
            pltpu.VMEM((8, C), f32),
            pltpu.VMEM((n, C), bf16),
            pltpu.VMEM((2, heads, n, C), bf16),
            pltpu.VMEM((heads, 2, n, C), bf16),
            pltpu.VMEM((heads, C, 2 * n), bf16),
            pltpu.VMEM((half, n, C), bf16),
            pltpu.VMEM((half // 2, C, 2 * n), bf16),
            pltpu.VMEM((half // 2, C, 2 * n), f32),
            pltpu.VMEM((half // 2, 1, 2 * n), f32),
            pltpu.VMEM((half // 2, 1, 2 * n), f32),
            pltpu.VMEM((half, 2, C, n // 2), bf16),
            pltpu.VMEM((half, 2, C, n // 2), bf16),
            pltpu.VMEM((half, 2, 1, n // 2), f32),
            pltpu.VMEM((half, 2, 1, n // 2), f32),
            pltpu.VMEM((2, C, n // 2), bf16),
            pltpu.VMEM((2, 1, n // 2), f32),
            pltpu.VMEM((2, C, n // 2), bf16),
            pltpu.VMEM((2, 1, n // 2), f32),
            dma,
            dma((len(vectors),)),
            dma((len(matrices),)),
            dma((3,)),
            dma((3,)),
            dma((2, 8)),
            dma((2, 8)),
            dma((2, heads, CHUNKS)),
            dma((heads, CHUNKS)),
            dma((heads, CHUNKS)),
            dma((heads, CHUNKS)),
            dma((half, 2)),
            dma((half, 2)),
            dma((half + 2,)),
            dma((half + 2,)),
            dma((half + 2,)),
            dma((half + 2,)),
        ],
        compiler_params=pltpu.CompilerParams(
            collective_id=1, has_side_effects=True, vmem_limit_bytes=VMEM_LIMIT
        ),
        name="middle_block",
    )(latent, *vectors, *matrices)
    return out.reshape(rows, cols, C)


def solution(mesh):
    return jax.shard_map(
        per_device,
        mesh=mesh,
        in_specs=(P("tile", "head", None),) + (P(),) * 17,
        out_specs=P("tile", "head", None),
        check_vma=False,
    )
```

```python
import functools
import math

import jax
import jax.numpy as jnp
from jax import lax
from jax.experimental import pallas as pl
from jax.experimental.pallas import tpu as pltpu
from jax.sharding import PartitionSpec as P

C = 512
GROUPS = 32
WIDTH = C // GROUPS
EPS = 1e-06
LANES = 128
PARTS = C // LANES
SHARE = WIDTH // PARTS
PAD = 8
LOG2E = math.log2(math.e)
MESH = pl.DeviceIdType.MESH
VMEM = pl.BlockSpec(memory_space=pltpu.VMEM)
HBM = pl.BlockSpec(memory_space=pltpu.HBM)
VECTORS = 11
CHUNKS = 4
DIRECT = 2
VMEM_LIMIT = 56 * 1024 * 1024


def interleaved(far, near):
    order, rest, near = far[: len(far) // 2], far[len(far) // 2 :], list(near)
    for place in rest:
        order += near[:1] + [place]
        near = near[1:]
    return order + near


def nt_dot(a, b):
    return lax.dot_general(a, b, (((1,), (1,)), ((), ())), preferred_element_type=jnp.float32)


def nn_dot(a, b):
    return jnp.dot(a, b, preferred_element_type=jnp.float32)


def lane_index(rows):
    return lax.broadcasted_iota(jnp.int32, (rows, LANES), 1)


def lane_partner(values, step):
    below = pltpu.roll(values, step, 1)
    above = pltpu.roll(values, LANES - step, 1)
    return jnp.where(lane_index(values.shape[0]) % (2 * step) >= step, below, above)


def group_sum(values):
    step = 1
    while step < WIDTH:
        values = values + lane_partner(values, step)
        step *= 2
    return values


def fold(row):
    return jnp.concatenate([row[:, i * LANES : (i + 1) * LANES] for i in range(PARTS)], axis=0)


def unfold(rows):
    return jnp.concatenate([rows[i : i + 1] for i in range(PARTS)], axis=1)


def local_stats(values):
    count = values.shape[0]
    mean = jnp.sum(values, axis=0, keepdims=True) / count
    deviation = values - mean
    square = jnp.sum(deviation * deviation, axis=0, keepdims=True)
    group_mean, square = fold(mean), fold(square)
    step = 1
    while step < WIDTH:
        other = lane_partner(group_mean, step)
        gap = group_mean - other
        square = square + lane_partner(square, step) + (0.5 * count * step) * (gap * gap)
        group_mean = 0.5 * (group_mean + other)
        step *= 2
    lane = lane_index(1)
    packed = jnp.zeros((1, LANES), jnp.float32)
    for i in range(PARTS):
        one = jnp.where(lane % 2 == 0, group_mean[i : i + 1], square[i : i + 1])
        packed = jnp.where((lane % WIDTH) // SHARE == i, one, packed)
    return packed


def merged_stats(slots, count):
    total = slots.shape[0]
    sums = jnp.sum(slots, axis=0)
    mean = sums / total
    gap = slots - mean[None]
    spread = jnp.sum(gap * gap, axis=0)
    variance = (sums + count * pltpu.roll(spread, 1, 1)) / (total * count)
    lane = lane_index(1)
    both = jnp.where(lane % 2 == 0, mean, lax.rsqrt(variance + EPS))
    row = lax.broadcasted_iota(jnp.int32, (2 * PARTS, LANES), 0)
    want = (row % PARTS) * SHARE + row // PARTS
    wide = jnp.where(lane_index(2 * PARTS) % WIDTH == want, both, 0.0)
    wide = group_sum(wide)
    return unfold(wide[:PARTS]), unfold(wide[PARTS:])


def silu_of_double(values):
    return values + values * jnp.tanh(values)


def block_kernel(
    tiles,
    heads,
    lat_hbm,
    *refs,
):
    vec_hbm, mat_hbm, refs = refs[:VECTORS], refs[VECTORS : VECTORS + 6], refs[VECTORS + 6 :]
    (
        out_ref,
        lat_ref,
        vec,
        w1,
        w2,
        wp,
        act,
        shifted,
        hid,
        row_in,
        row_out,
        col_in,
        col_out,
        corner_in,
        stat_out,
        stat_in,
        norm,
        res,
        kv,
        kn,
        kt,
        qn,
        qp,
        acc,
        top,
        low,
        o_out,
        o_in,
        l_out,
        l_in,
        u_in,
        ul_in,
        m_out,
        ml_out,
        lat_sem,
        v_sem,
        w_sem,
        s_send,
        s_recv,
        h_send,
        h_recv,
        z_send,
        z_recv,
        c_send,
        c_recv,
        q_send,
        q_recv,
        o_send,
        o_recv,
        l_send,
        l_recv,
    ) = refs
    rows, cols, _ = lat_ref.shape
    n = rows * cols
    total = tiles * heads
    half = tiles // 2
    pairs = half // 2
    tile, head = lax.axis_index("tile"), lax.axis_index("head")
    me = tile * heads + head
    partner = (tile + 1 - 2 * lax.rem(tile, 2), head)

    def fellow(j):
        chip, bit, other = lax.div(tile, 2), 1, 0
        if half & (half - 1):
            return lax.rem(tile + 2 * j, tiles)
        while bit < half:
            mine, flip = lax.rem(lax.div(chip, bit), 2), (j // bit) % 2
            other = other + bit * (mine + flip - 2 * mine * flip)
            bit *= 2
        return 2 * other + lax.rem(tile, 2)

    def lender(j):
        return fellow(j) if half & (half - 1) == 0 else lax.rem(tile + tiles - 2 * j, tiles)

    barrier = pltpu.get_barrier_semaphore()

    def greet(k, carry):
        peer = lax.rem(me + k, total)
        pl.semaphore_signal(
            barrier, inc=1, device_id=(lax.div(peer, heads), lax.rem(peer, heads)), device_id_type=MESH
        )
        return carry

    latent_copy = pltpu.make_async_copy(lat_hbm, lat_ref, lat_sem)
    latent_copy.start()
    lax.fori_loop(1, total, greet, 0)
    vectors = [
        pltpu.make_async_copy(src, vec.at[i], v_sem.at[i]) for i, src in enumerate(vec_hbm)
    ]
    targets = [w1, w2] + [wp.at[i] for i in range(4)]
    weights = [
        pltpu.make_async_copy(src, dst, w_sem.at[i])
        for i, (src, dst) in enumerate(zip(mat_hbm, targets))
    ]
    for copy in vectors + weights:
        copy.start()
    n1g, n1s, c1b, n2g, n2s, c2b, n3g, n3s, qb, vb, ob = [vec.at[i] for i in range(VECTORS)]

    def remote(src, dst, send, recv, device):
        return pltpu.make_async_remote_copy(
            src_ref=src,
            dst_ref=dst,
            send_sem=send,
            recv_sem=recv,
            device_id=device,
            device_id_type=MESH,
        )

    def stat_copy(phase, k):
        peer = lax.rem(me + k, total)
        return remote(
            stat_out.at[phase],
            stat_in.at[phase, k],
            s_send.at[phase],
            s_recv.at[phase],
            (lax.div(peer, heads), lax.rem(peer, heads)),
        )

    def stats_start(phase):
        def begin(k, carry):
            stat_copy(phase, k).start()
            return carry

        lax.fori_loop(1, total, begin, 0)

    def stats_finish(phase, gain, shift):
        others = stat_in.at[phase, pl.ds(1, total - 1)]
        for sem in (s_send, s_recv):
            pltpu.make_async_copy(others, others, sem.at[phase]).wait()
        mean, inverse = merged_stats(stat_in[phase], n * WIDTH)
        norm[0:1] = inverse * gain[...]
        norm[1:2] = shift[...] - mean * (inverse * gain[...])

    def put_stats(phase, values):
        packed = local_stats(values)
        stat_out[phase] = packed
        stat_in[phase, 0] = packed

    def normalize(values):
        return values * norm[0:1] + norm[1:2]

    def halo_plan(phase, first_row, last_row):
        first, last = col_out.at[phase, 0], col_out.at[phase, 1]
        plan = [
            (first_row, row_in.at[phase, 1], -1, 0),
            (last_row, row_in.at[phase, 0], 1, 0),
            (first, col_in.at[phase, 1], 0, -1),
            (last, col_in.at[phase, 0], 0, 1),
            (first.at[0], corner_in.at[phase, 3], -1, -1),
            (last.at[0], corner_in.at[phase, 2], -1, 1),
            (first.at[rows - 1], corner_in.at[phase, 1], 1, -1),
            (last.at[rows - 1], corner_in.at[phase, 0], 1, 1),
        ]
        return plan

    def there(dt, dh):
        inside = None
        for place, delta, size in ((tile, dt, tiles), (head, dh, heads)):
            if delta:
                one = place + delta < size if delta > 0 else place + delta >= 0
                inside = one if inside is None else jnp.logical_and(inside, one)
        return inside

    def halo_copy(phase, i, src, dst, dt, dh):
        return remote(
            src, dst, h_send.at[phase, i], h_recv.at[phase, i], (tile + dt, head + dh)
        )

    def halo_start(phase, plan):
        for i, (src, dst, dt, dh) in enumerate(plan):

            @pl.when(there(dt, dh))
            def _(i=i, src=src, dst=dst, dt=dt, dh=dh):
                halo_copy(phase, i, src, dst, dt, dh).start()

    def halo_finish(phase, plan):
        for i, (src, dst, dt, dh) in enumerate(plan):

            @pl.when(there(dt, dh))
            def _(i=i, src=src, dst=dst, dt=dt, dh=dh):
                halo_copy(phase, i, src, dst, dt, dh).wait_send()

            @pl.when(there(-dt, -dh))
            def _(i=i, src=src, dst=dst, dt=dt, dh=dh):
                halo_copy(phase, i, src, dst, dt, dh).wait_recv()

    def put_columns(phase, values):
        for r in range(rows):
            col_out[phase, 0, r] = values[r, 0:1]
            col_out[phase, 1, r] = values[r, cols - 1 : cols]

    def activate(phase, values):
        left, right = head > 0, head < heads - 1
        up, down = tile > 0, tile < tiles - 1

        slope, level = 0.5 * norm[0:1], 0.5 * norm[1:2]

        def active(x):
            return silu_of_double(x * slope + level)

        for r in range(rows):
            one = active(values(r))
            act[1 + r, PAD : PAD + cols] = one
            shifted[1, 1 + r] = one.astype(jnp.bfloat16)
            for side, at, inside in ((0, PAD - 1, left), (1, PAD + cols, right)):
                one = active(col_in[phase, side, r])
                act[1 + r, at : at + 1] = jnp.where(inside, one, 0.0)
        for side, at, inside in ((0, 0, up), (1, rows + 1, down)):
            one = active(row_in[phase, side].astype(jnp.float32))
            one = jnp.where(inside, one, 0.0)
            act[at, PAD : PAD + cols] = one
            shifted[1, at] = one.astype(jnp.bfloat16)
            for k, place, beside in ((0, PAD - 1, left), (1, PAD + cols, right)):
                one = active(corner_in[phase, 2 * side + k])
                both = jnp.logical_and(inside, beside)
                act[at, place : place + 1] = jnp.where(both, one, 0.0)
        for dj in (0, 2):
            start = PAD - 1 + dj
            for r in range(rows + 2):
                shifted[dj, r] = act[r, start : start + cols].astype(jnp.bfloat16)

    def conv(weight, first=0, many=rows):
        result = None
        for di in range(3):
            for dj in range(3):
                tap = 3 * di + dj
                lhs = shifted[dj, first + di : first + di + many].reshape(many * cols, C)
                one = nn_dot(lhs, weight[tap * C : (tap + 1) * C])
                result = one if result is None else result + one
        return result

    with jax.named_scope("stats0"):
        latent_copy.wait()
        put_stats(0, lat_ref[...].astype(jnp.float32).reshape(n, C))
    with jax.named_scope("barrier"):
        pl.semaphore_wait(barrier, total - 1)
    with jax.named_scope("send0"):
        plan = halo_plan(0, lat_ref.at[0], lat_ref.at[rows - 1])
        stats_start(0)
        put_columns(0, lat_ref[...].astype(jnp.float32))
        halo_start(0, plan)
    with jax.named_scope("halo0"):
        halo_finish(0, plan)
    with jax.named_scope("norm0"):
        for copy in vectors:
            copy.wait()
        stats_finish(0, n1g, n1s)
    with jax.named_scope("act0"):
        activate(0, lambda r: lat_ref[r].astype(jnp.float32))
    with jax.named_scope("w0"):
        weights[0].wait()
    with jax.named_scope("conv0"):
        hid[...] = (conv(w1) + c1b[...]).reshape(rows, cols, C)

    with jax.named_scope("stats1"):
        put_stats(1, hid[...].reshape(n, C))
    with jax.named_scope("send1"):
        plan = halo_plan(1, row_out.at[0], row_out.at[1])
        stats_start(1)
        row_out[0] = hid[0].astype(jnp.bfloat16)
        row_out[1] = hid[rows - 1].astype(jnp.bfloat16)
        put_columns(1, hid[...])
        halo_start(1, plan)
    with jax.named_scope("halo1"):
        halo_finish(1, plan)
    with jax.named_scope("norm1"):
        stats_finish(1, n2g, n2s)
    with jax.named_scope("act1"):
        activate(1, lambda r: hid[r])
    with jax.named_scope("conv1"):
        weights[1].wait()

    def residual(r):
        with jax.named_scope("conv1"):
            new = lat_ref[r].astype(jnp.float32) + (conv(w2, r, 1) + c2b[...])
            res[r * cols : (r + 1) * cols] = new.astype(jnp.bfloat16)

    def piece(ref, ch):
        return ref.at[pl.ds(ch * (n // CHUNKS), n // CHUNKS)]

    def z_copy(source, src, way, distance, ch):
        return remote(
            piece(src, ch),
            piece(kv.at[0, source], ch),
            z_send.at[way, distance, ch],
            z_recv.at[source, ch],
            (tile, head + (1 if way else -1) * (distance if distance <= DIRECT else 1)),
        )

    def reachable(way, distance):
        return head + distance < heads if way else head - distance >= 0

    at_end = jnp.logical_or(head == 0, head == heads - 1)

    def straight(fn, opening=None):
        nearer = [(1, ch) for ch in range(CHUNKS)]
        farther = [(d, ch) for d in range(2, min(DIRECT, heads - 1) + 1) for ch in range(CHUNKS)]
        for chosen, order in ((at_end, interleaved(farther, nearer)), (~at_end, farther + nearer)):
            for distance, ch in order:
                for way in (0, 1):
                    present = jnp.logical_and(reachable(way, distance), chosen)
                    if opening is not None:
                        opens = ch == 0 and distance <= 2
                        if opens and distance == 1:
                            alone = ~reachable(way, 2)
                            present = jnp.logical_and(present, alone if opening else ~alone)
                        elif opens != opening:
                            continue

                    @pl.when(present)
                    def _(way=way, distance=distance, ch=ch):
                        fn(z_copy(head, res, way, distance, ch))

    def onward(distance, fn, chunks=tuple(range(CHUNKS))):
        for ch in chunks:
            for way in (0, 1):

                @pl.when(jnp.logical_and(reachable(1 - way, distance), reachable(way, 1)))
                def _(way=way, ch=ch):
                    source = head + (-distance if way else distance)
                    fn(z_copy(source, kv.at[0, source], way, distance + 1, ch))

    def z_arrived(source, distance, way, ch):
        def wait():
            z_copy(source, res, way, 1, ch).wait_recv()

        if heads - 1 > DIRECT:
            passed = jnp.logical_and(distance >= DIRECT, reachable(1 - way, 1))
            pl.when(jnp.logical_not(passed))(wait)
        else:
            wait()

    def c_copy(source, src, ch):
        return remote(
            piece(src, ch),
            piece(kv.at[1, source], ch),
            c_send.at[source, ch],
            c_recv.at[source, ch],
            partner,
        )

    def q_copy(j, part):
        rows_of = pl.ds(0, n // 2) if part == 0 else pl.ds(n // 2, n - n // 2)
        return remote(
            res.at[rows_of],
            qn.at[j, rows_of],
            q_send.at[j, part],
            q_recv.at[j, part],
            (fellow(j), head),
        )

    residual(0)
    straight(lambda copy: copy.start(), True)
    for j in (1, 2):
        if j < half:
            q_copy(j, 0).start()
    for r in range(1, rows):
        residual(r)
    for ch in range(CHUNKS):
        c_copy(head, res, ch).start()
    with jax.named_scope("stats2"):
        put_stats(2, res[...].astype(jnp.float32))
        stats_start(2)

    def pass_on(ch):
        def go(copy):
            copy.wait_recv()
            copy.start()

        with jax.named_scope("relay"):
            for distance in range(DIRECT, heads - 1):
                onward(distance, go, (ch,))

    straight(lambda copy: copy.start(), False)
    for j in (1, 2):
        if j < half:
            q_copy(j, 1).start()

    def q_begin(j, carry):
        for part in range(2):
            q_copy(j, part).start()
        return carry

    lax.fori_loop(3, half, q_begin, 0)
    pass_on(0)
    pass_on(1)
    with jax.named_scope("norm2"):
        stats_finish(2, n3g, n3s)
        for copy in weights[2:]:
            copy.wait()

    def normed(values):
        return normalize(values.astype(jnp.float32)).astype(jnp.bfloat16)

    scale = LOG2E / C**0.5

    def make_query(pair, at, source):
        query = (nn_dot(normed(source), wp[0]) + qb[...]).astype(jnp.bfloat16)
        qp[pair, :, at * n : (at + 1) * n] = (nt_dot(wp[1], query) * scale).astype(jnp.bfloat16)

    def clear(pair):
        top[pair] = jnp.full((1, 2 * n), -jnp.inf, jnp.float32)
        low[pair] = jnp.zeros((1, 2 * n), jnp.float32)
        acc[pair] = jnp.zeros((C, 2 * n), jnp.float32)

    def prepare(core, source, values):
        keys = normed(values)
        kn[source, core] = keys
        kt[source, :, core * n : (core + 1) * n] = jnp.transpose(keys)

    def one_core(core, source):
        return kn.at[source, core], kt.at[source, :, pl.ds(core * n, n)]

    def both_cores(source):
        return kn.at[source], kt.at[source]

    def attend(pair, *blocks):
        query = qp[pair]
        scores = [nn_dot(keys[...].reshape(-1, C), query) for keys, _ in blocks]
        before = top[pair]
        peak = before
        for one in scores:
            peak = jnp.maximum(peak, jnp.max(one, axis=0, keepdims=True))
        fade = jnp.exp2(before - peak)
        sums, values = low[pair] * fade, None
        for one, (_, turned) in zip(scores, blocks):
            expo = jnp.exp2(one - peak)
            sums = sums + jnp.sum(expo, axis=0, keepdims=True)
            part = nn_dot(turned[...], expo.astype(jnp.bfloat16))
            values = part if values is None else values + part
        top[pair] = peak
        low[pair] = sums
        acc[pair] = acc[pair] * fade + values

    def columns(fn, distances, chosen=None):
        for distance in distances:
            for way in (0, 1):
                present = reachable(way, distance)
                if chosen is not None:
                    present = jnp.logical_and(present, chosen)

                @pl.when(present)
                def _(distance=distance, way=way):
                    fn(head + (distance if way else -distance), distance, way)

    far = tuple(range(2, heads))

    with jax.named_scope("query0"):
        clear(0)
        make_query(0, 0, res[...])
        prepare(0, head, res[...])
    with jax.named_scope("q_wait0"):
        for part in range(2):
            q_copy(1, part).wait()
    pass_on(2)
    with jax.named_scope("query1"):
        make_query(0, 1, qn[1])
        for ch in range(CHUNKS):
            c_copy(head, res, ch).wait()
        prepare(1, head, kv[1, head])
    pass_on(3)
    with jax.named_scope("attend_own"):
        attend(0, both_cores(head))

    def begin(source, distance, way):
        with jax.named_scope("z_wait"):
            for ch in range(CHUNKS):
                z_arrived(source, distance, way, ch)
                c_copy(source, kv.at[0, source], ch).start()
        with jax.named_scope("prepare0"):
            prepare(0, source, kv[0, source])

    def second(source):
        with jax.named_scope("c_wait"):
            for ch in range(CHUNKS):
                c_copy(source, kv.at[0, source], ch).wait()
        with jax.named_scope("prepare1"):
            prepare(1, source, kv[1, source])

    def other_pairs(*blocks):
        def one(pair, carry):
            attend(pair, *blocks)
            return carry

        if pairs == 2:
            attend(1, *blocks)
        else:
            lax.fori_loop(1, pairs, one, 0)

    def together(source, distance, way):
        second(source)
        with jax.named_scope("together"):
            other_pairs(both_cores(source))

    def own_pair():
        with jax.named_scope("own_far"):
            attend(0, *[both_cores(lax.rem(head + k, heads)) for k in range(1, heads)])

    columns(begin, (1,), at_end)

    def rest(pair, carry):
        with jax.named_scope("q_wait1"):
            for at in range(2):
                for part in range(2):
                    q_copy(2 * pair + at, part).wait()
        with jax.named_scope("query2"):
            clear(pair)
            for at in range(2):
                make_query(pair, at, qn[2 * pair + at])
        return carry

    lax.fori_loop(1, pairs, rest, 0)
    columns(begin, (2,), ~at_end)
    with jax.named_scope("attend_rest"):
        other_pairs(both_cores(head))
    columns(begin, (2,), at_end)
    columns(together, (1,), at_end)
    columns(together, (2,))

    def apart(*place):
        begin(*place)
        with jax.named_scope("late0"):
            other_pairs(one_core(0, place[0]))
        second(place[0])
        with jax.named_scope("late1"):
            other_pairs(one_core(1, place[0]))

    def two_near(first, last):
        begin(*first)
        with jax.named_scope("late0"):
            other_pairs(one_core(0, first[0]))
        second(first[0])
        begin(*last)
        with jax.named_scope("late01"):
            other_pairs(one_core(1, first[0]), one_core(0, last[0]))
        second(last[0])
        with jax.named_scope("late1"):
            other_pairs(one_core(1, last[0]))

    below, above = (head - 1, 1, 0), (head + 1, 1, 1)
    lower = 2 * head < heads - 1
    pl.when(jnp.logical_and(~at_end, lower))(lambda: two_near(below, above))
    pl.when(jnp.logical_and(~at_end, ~lower))(lambda: two_near(above, below))

    columns(apart, far[1:])

    def both(src, dst, src_level, dst_level, sem, device):
        return [
            remote(src, dst, o_send.at[sem], o_recv.at[sem], device),
            remote(src_level, dst_level, l_send.at[sem], l_recv.at[sem], device),
        ]

    def give_copies(j):
        return both(o_out.at[j], o_in.at[j], l_out.at[j], l_in.at[j], j, (lender(j), head))

    def finish(pair, at, o_to, l_to):
        for part in range(2):
            lanes = slice((2 * at + part) * (n // 2), (2 * at + part + 1) * (n // 2))
            sums = low[pair, :, lanes]
            l_to[2 * pair + at, part] = top[pair, :, lanes] + jnp.log2(sums)
            o_to[2 * pair + at, part] = (acc[pair, :, lanes] * (1.0 / sums)).astype(jnp.bfloat16)

    def column_sent():
        straight(lambda copy: copy.wait_send())
        for distance in range(DIRECT, heads - 1):
            onward(distance, lambda copy: copy.wait_send())

    def begin_all(copies):
        for copy in copies:
            copy.start()

    def end_all(copies):
        for copy in copies:
            copy.wait()

    if half == 4:
        def hop(part):
            via = (fellow(2 - part), head)
            return both(
                o_out.at[3, part], u_in.at[part], l_out.at[3, part], ul_in.at[part], part, via
            )

        def direct(j):
            part = 2 - j
            return both(
                o_out.at[j, part],
                o_in.at[j, part],
                l_out.at[j, part],
                l_in.at[j, part],
                1 + j,
                (fellow(j), head),
            )

        def merged(j):
            part = j - 1
            return both(
                m_out.at[part],
                o_in.at[j, part],
                ml_out.at[part],
                l_in.at[j, part],
                3 + j,
                (fellow(j), head),
            )

        def merge(j):
            part = j - 1
            end_all(hop(part))
            mine, theirs = l_out[j, part], ul_in[part]
            level = jnp.maximum(mine, theirs)
            keep, add = jnp.exp2(mine - level), jnp.exp2(theirs - level)
            whole = keep + add
            ml_out[part] = level + jnp.log2(whole)
            values = o_out[j, part].astype(jnp.float32) * (keep / whole)
            values = values + u_in[part].astype(jnp.float32) * (add / whole)
            m_out[part] = values.astype(jnp.bfloat16)
            begin_all(merged(j))

        with jax.named_scope("give"):
            finish(1, 1, o_out, l_out)
            begin_all(hop(0))
            begin_all(hop(1))
            finish(1, 0, o_out, l_out)
            begin_all(direct(2))
        own_pair()
        with jax.named_scope("give1"):
            finish(0, 1, o_out, l_out)
            begin_all(direct(1))
        with jax.named_scope("finish0"):
            finish(0, 0, o_in, l_in)
            column_sent()
        with jax.named_scope("merge2"):
            merge(2)
        with jax.named_scope("merge1"):
            merge(1)
        with jax.named_scope("take"):
            for j in (1, 2):
                end_all(direct(j))
                end_all(merged(j))
        parts = 3
    else:

        def give(i, carry):
            pair = pairs - 1 - i
            for at in range(2):
                finish(pair, at, o_out, l_out)
                begin_all(give_copies(2 * pair + at))
            return carry

        def take(j, carry):
            end_all(give_copies(j))
            return carry

        lax.fori_loop(0, pairs - 1, give, 0)
        own_pair()
        finish(0, 1, o_out, l_out)
        begin_all(give_copies(1))
        finish(0, 0, o_in, l_in)
        column_sent()
        lax.fori_loop(1, half, take, 0)
        parts = half
    with jax.named_scope("last"):
        sides = []
        for part in range(2):
            peak = l_in[0, part]
            for j in range(1, parts):
                peak = jnp.maximum(peak, l_in[j, part])
            shares = [jnp.exp2(l_in[j, part] - peak) for j in range(parts)]
            whole = shares[0]
            for j in range(1, parts):
                whole = whole + shares[j]
            side = jnp.zeros((C, n // 2), jnp.float32)
            for j in range(parts):
                side = side + (shares[j] / whole) * o_in[j, part].astype(jnp.float32)
            sides.append(side)
        mixed = jnp.concatenate(sides, axis=1)
        mixed = jnp.transpose(mixed.astype(jnp.bfloat16))
        attended = (nn_dot(mixed, wp[2]) + vb[...]).astype(jnp.bfloat16)
        out = nn_dot(attended, wp[3]) + ob[...]
        out_ref[...] = (res[...].astype(jnp.float32) + out).astype(jnp.bfloat16)


def per_device(
    latent,
    norm1_gain,
    norm1_shift,
    conv1_weight,
    conv1_bias,
    norm2_gain,
    norm2_shift,
    conv2_weight,
    conv2_bias,
    norm3_gain,
    norm3_shift,
    query_weight,
    query_bias,
    key_weight,
    value_weight,
    value_bias,
    out_weight,
    out_bias,
):
    rows, cols, _ = latent.shape
    tiles, heads = lax.axis_size("tile"), lax.axis_size("head")
    n = rows * cols
    total = tiles * heads
    half = tiles // 2
    vectors = [
        v.reshape(1, C)
        for v in (
            norm1_gain,
            norm1_shift,
            conv1_bias,
            norm2_gain,
            norm2_shift,
            conv2_bias,
            norm3_gain,
            norm3_shift,
            query_bias,
            value_bias,
            out_bias,
        )
    ]
    matrices = [
        conv1_weight.reshape(9 * C, C),
        conv2_weight.reshape(9 * C, C),
        query_weight,
        key_weight,
        value_weight,
        out_weight,
    ]
    bf16, f32 = jnp.bfloat16, jnp.float32
    dma = pltpu.SemaphoreType.DMA
    out = pl.pallas_call(
        functools.partial(block_kernel, tiles, heads),
        out_shape=pltpu.VMEM((n, C), bf16),
        in_specs=[HBM] * (1 + len(vectors) + len(matrices)),
        out_specs=VMEM,
        scratch_shapes=[
            pltpu.VMEM((rows, cols, C), bf16),
            pltpu.VMEM((len(vectors), 1, C), f32),
            pltpu.VMEM((9 * C, C), bf16),
            pltpu.VMEM((9 * C, C), bf16),
            pltpu.VMEM((4, C, C), bf16),
            pltpu.VMEM((rows + 2, cols + 2 * PAD, C), f32),
            pltpu.VMEM((3, rows + 2, cols, C), bf16),
            pltpu.VMEM((rows, cols, C), f32),
            pltpu.VMEM((2, 2, cols, C), bf16),
            pltpu.VMEM((2, cols, C), bf16),
            pltpu.VMEM((2, 2, rows, 1, C), f32),
            pltpu.VMEM((2, 2, rows, 1, C), f32),
            pltpu.VMEM((2, 4, 1, C), f32),
            pltpu.VMEM((3, 1, LANES), f32),
            pltpu.VMEM((3, total, 1, LANES), f32),
            pltpu.VMEM((8, C), f32),
            pltpu.VMEM((n, C), bf16),
            pltpu.VMEM((2, heads, n, C), bf16),
            pltpu.VMEM((heads, 2, n, C), bf16),
            pltpu.VMEM((heads, C, 2 * n), bf16),
            pltpu.VMEM((half, n, C), bf16),
            pltpu.VMEM((half // 2, C, 2 * n), bf16),
            pltpu.VMEM((half // 2, C, 2 * n), f32),
            pltpu.VMEM((half // 2, 1, 2 * n), f32),
            pltpu.VMEM((half // 2, 1, 2 * n), f32),
            pltpu.VMEM((half, 2, C, n // 2), bf16),
            pltpu.VMEM((half, 2, C, n // 2), bf16),
            pltpu.VMEM((half, 2, 1, n // 2), f32),
            pltpu.VMEM((half, 2, 1, n // 2), f32),
            pltpu.VMEM((2, C, n // 2), bf16),
            pltpu.VMEM((2, 1, n // 2), f32),
            pltpu.VMEM((2, C, n // 2), bf16),
            pltpu.VMEM((2, 1, n // 2), f32),
            dma,
            dma((len(vectors),)),
            dma((len(matrices),)),
            dma((3,)),
            dma((3,)),
            dma((2, 8)),
            dma((2, 8)),
            dma((2, heads, CHUNKS)),
            dma((heads, CHUNKS)),
            dma((heads, CHUNKS)),
            dma((heads, CHUNKS)),
            dma((half, 2)),
            dma((half, 2)),
            dma((half + 2,)),
            dma((half + 2,)),
            dma((half + 2,)),
            dma((half + 2,)),
        ],
        compiler_params=pltpu.CompilerParams(
            collective_id=1, has_side_effects=True, vmem_limit_bytes=VMEM_LIMIT
        ),
        name="middle_block",
    )(latent, *vectors, *matrices)
    return out.reshape(rows, cols, C)


def solution(mesh):
    return jax.shard_map(
        per_device,
        mesh=mesh,
        in_specs=(P("tile", "head", None),) + (P(),) * 17,
        out_specs=P("tile", "head", None),
        check_vma=False,
    )
```

```python
import functools
import math

import jax
import jax.numpy as jnp
from jax import lax
from jax.experimental import pallas as pl
from jax.experimental.pallas import tpu as pltpu
from jax.sharding import PartitionSpec as P

C = 512
GROUPS = 32
WIDTH = C // GROUPS
EPS = 1e-06
LANES = 128
PARTS = C // LANES
SHARE = WIDTH // PARTS
PAD = 8
LOG2E = math.log2(math.e)
MESH = pl.DeviceIdType.MESH
VMEM = pl.BlockSpec(memory_space=pltpu.VMEM)
HBM = pl.BlockSpec(memory_space=pltpu.HBM)
VECTORS = 11
CHUNKS = 4
DIRECT = 2
VMEM_LIMIT = 56 * 1024 * 1024


def interleaved(far, near):
    order, rest, near = far[: len(far) // 2], far[len(far) // 2 :], list(near)
    for place in rest:
        order += near[:1] + [place]
        near = near[1:]
    return order + near


def nt_dot(a, b):
    return lax.dot_general(a, b, (((1,), (1,)), ((), ())), preferred_element_type=jnp.float32)


def nn_dot(a, b):
    return jnp.dot(a, b, preferred_element_type=jnp.float32)


def lane_index(rows):
    return lax.broadcasted_iota(jnp.int32, (rows, LANES), 1)


def lane_partner(values, step):
    below = pltpu.roll(values, step, 1)
    above = pltpu.roll(values, LANES - step, 1)
    return jnp.where(lane_index(values.shape[0]) % (2 * step) >= step, below, above)


def group_sum(values):
    step = 1
    while step < WIDTH:
        values = values + lane_partner(values, step)
        step *= 2
    return values


def fold(row):
    return jnp.concatenate([row[:, i * LANES : (i + 1) * LANES] for i in range(PARTS)], axis=0)


def unfold(rows):
    return jnp.concatenate([rows[i : i + 1] for i in range(PARTS)], axis=1)


def local_stats(values):
    count = values.shape[0]
    mean = jnp.sum(values, axis=0, keepdims=True) / count
    deviation = values - mean
    square = jnp.sum(deviation * deviation, axis=0, keepdims=True)
    group_mean, square = fold(mean), fold(square)
    step = 1
    while step < WIDTH:
        other = lane_partner(group_mean, step)
        gap = group_mean - other
        square = square + lane_partner(square, step) + (0.5 * count * step) * (gap * gap)
        group_mean = 0.5 * (group_mean + other)
        step *= 2
    lane = lane_index(1)
    packed = jnp.zeros((1, LANES), jnp.float32)
    for i in range(PARTS):
        one = jnp.where(lane % 2 == 0, group_mean[i : i + 1], square[i : i + 1])
        packed = jnp.where((lane % WIDTH) // SHARE == i, one, packed)
    return packed


def merged_stats(slots, count):
    total = slots.shape[0]
    sums = jnp.sum(slots, axis=0)
    mean = sums / total
    gap = slots - mean[None]
    spread = jnp.sum(gap * gap, axis=0)
    variance = (sums + count * pltpu.roll(spread, 1, 1)) / (total * count)
    lane = lane_index(1)
    both = jnp.where(lane % 2 == 0, mean, lax.rsqrt(variance + EPS))
    row = lax.broadcasted_iota(jnp.int32, (2 * PARTS, LANES), 0)
    want = (row % PARTS) * SHARE + row // PARTS
    wide = jnp.where(lane_index(2 * PARTS) % WIDTH == want, both, 0.0)
    wide = group_sum(wide)
    return unfold(wide[:PARTS]), unfold(wide[PARTS:])


def silu_of_double(values):
    return values + values * jnp.tanh(values)


def block_kernel(
    tiles,
    heads,
    lat_hbm,
    *refs,
):
    vec_hbm, mat_hbm, refs = refs[:VECTORS], refs[VECTORS : VECTORS + 6], refs[VECTORS + 6 :]
    (
        out_ref,
        lat_ref,
        vec,
        w1,
        w2,
        wp,
        act,
        shifted,
        hid,
        row_in,
        row_out,
        col_in,
        col_out,
        corner_in,
        stat_out,
        stat_in,
        norm,
        res,
        kv,
        kn,
        kt,
        qn,
        qp,
        acc,
        top,
        low,
        o_out,
        o_in,
        l_out,
        l_in,
        u_in,
        ul_in,
        m_out,
        ml_out,
        lat_sem,
        v_sem,
        w_sem,
        s_send,
        s_recv,
        h_send,
        h_recv,
        z_send,
        z_recv,
        c_send,
        c_recv,
        q_send,
        q_recv,
        o_send,
        o_recv,
        l_send,
        l_recv,
    ) = refs
    rows, cols, _ = lat_ref.shape
    n = rows * cols
    total = tiles * heads
    half = tiles // 2
    pairs = half // 2
    tile, head = lax.axis_index("tile"), lax.axis_index("head")
    me = tile * heads + head
    partner = (tile + 1 - 2 * lax.rem(tile, 2), head)

    def fellow(j):
        chip, bit, other = lax.div(tile, 2), 1, 0
        if half & (half - 1):
            return lax.rem(tile + 2 * j, tiles)
        while bit < half:
            mine, flip = lax.rem(lax.div(chip, bit), 2), (j // bit) % 2
            other = other + bit * (mine + flip - 2 * mine * flip)
            bit *= 2
        return 2 * other + lax.rem(tile, 2)

    def lender(j):
        return fellow(j) if half & (half - 1) == 0 else lax.rem(tile + tiles - 2 * j, tiles)

    barrier = pltpu.get_barrier_semaphore()

    def greet(k, carry):
        peer = lax.rem(me + k, total)
        pl.semaphore_signal(
            barrier, inc=1, device_id=(lax.div(peer, heads), lax.rem(peer, heads)), device_id_type=MESH
        )
        return carry

    latent_copy = pltpu.make_async_copy(lat_hbm, lat_ref, lat_sem)
    latent_copy.start()
    lax.fori_loop(1, total, greet, 0)
    vectors = [
        pltpu.make_async_copy(src, vec.at[i], v_sem.at[i]) for i, src in enumerate(vec_hbm)
    ]
    targets = [w1, w2] + [wp.at[i] for i in range(4)]
    weights = [
        pltpu.make_async_copy(src, dst, w_sem.at[i])
        for i, (src, dst) in enumerate(zip(mat_hbm, targets))
    ]
    for copy in vectors + weights:
        copy.start()
    n1g, n1s, c1b, n2g, n2s, c2b, n3g, n3s, qb, vb, ob = [vec.at[i] for i in range(VECTORS)]

    def remote(src, dst, send, recv, device):
        return pltpu.make_async_remote_copy(
            src_ref=src,
            dst_ref=dst,
            send_sem=send,
            recv_sem=recv,
            device_id=device,
            device_id_type=MESH,
        )

    def stat_copy(phase, k):
        peer = lax.rem(me + k, total)
        return remote(
            stat_out.at[phase],
            stat_in.at[phase, k],
            s_send.at[phase],
            s_recv.at[phase],
            (lax.div(peer, heads), lax.rem(peer, heads)),
        )

    def stats_start(phase):
        def begin(k, carry):
            stat_copy(phase, k).start()
            return carry

        lax.fori_loop(1, total, begin, 0)

    def stats_finish(phase, gain, shift):
        others = stat_in.at[phase, pl.ds(1, total - 1)]
        for sem in (s_send, s_recv):
            pltpu.make_async_copy(others, others, sem.at[phase]).wait()
        mean, inverse = merged_stats(stat_in[phase], n * WIDTH)
        norm[0:1] = inverse * gain[...]
        norm[1:2] = shift[...] - mean * (inverse * gain[...])

    def put_stats(phase, values):
        packed = local_stats(values)
        stat_out[phase] = packed
        stat_in[phase, 0] = packed

    def normalize(values):
        return values * norm[0:1] + norm[1:2]

    def halo_plan(phase, first_row, last_row):
        first, last = col_out.at[phase, 0], col_out.at[phase, 1]
        plan = [
            (first_row, row_in.at[phase, 1], -1, 0),
            (last_row, row_in.at[phase, 0], 1, 0),
            (first, col_in.at[phase, 1], 0, -1),
            (last, col_in.at[phase, 0], 0, 1),
            (first.at[0], corner_in.at[phase, 3], -1, -1),
            (last.at[0], corner_in.at[phase, 2], -1, 1),
            (first.at[rows - 1], corner_in.at[phase, 1], 1, -1),
            (last.at[rows - 1], corner_in.at[phase, 0], 1, 1),
        ]
        return plan

    def there(dt, dh):
        inside = None
        for place, delta, size in ((tile, dt, tiles), (head, dh, heads)):
            if delta:
                one = place + delta < size if delta > 0 else place + delta >= 0
                inside = one if inside is None else jnp.logical_and(inside, one)
        return inside

    def halo_copy(phase, i, src, dst, dt, dh):
        return remote(
            src, dst, h_send.at[phase, i], h_recv.at[phase, i], (tile + dt, head + dh)
        )

    def halo_start(phase, plan):
        for i, (src, dst, dt, dh) in enumerate(plan):

            @pl.when(there(dt, dh))
            def _(i=i, src=src, dst=dst, dt=dt, dh=dh):
                halo_copy(phase, i, src, dst, dt, dh).start()

    def halo_finish(phase, plan):
        for i, (src, dst, dt, dh) in enumerate(plan):

            @pl.when(there(dt, dh))
            def _(i=i, src=src, dst=dst, dt=dt, dh=dh):
                halo_copy(phase, i, src, dst, dt, dh).wait_send()

            @pl.when(there(-dt, -dh))
            def _(i=i, src=src, dst=dst, dt=dt, dh=dh):
                halo_copy(phase, i, src, dst, dt, dh).wait_recv()

    def put_columns(phase, values):
        for r in range(rows):
            col_out[phase, 0, r] = values[r, 0:1]
            col_out[phase, 1, r] = values[r, cols - 1 : cols]

    def activate(phase, values):
        left, right = head > 0, head < heads - 1
        up, down = tile > 0, tile < tiles - 1

        slope, level = 0.5 * norm[0:1], 0.5 * norm[1:2]

        def active(x):
            return silu_of_double(x * slope + level)

        for r in range(rows):
            one = active(values(r))
            act[1 + r, PAD : PAD + cols] = one
            shifted[1, 1 + r] = one.astype(jnp.bfloat16)
            for side, at, inside in ((0, PAD - 1, left), (1, PAD + cols, right)):
                one = active(col_in[phase, side, r])
                act[1 + r, at : at + 1] = jnp.where(inside, one, 0.0)
        for side, at, inside in ((0, 0, up), (1, rows + 1, down)):
            one = active(row_in[phase, side].astype(jnp.float32))
            one = jnp.where(inside, one, 0.0)
            act[at, PAD : PAD + cols] = one
            shifted[1, at] = one.astype(jnp.bfloat16)
            for k, place, beside in ((0, PAD - 1, left), (1, PAD + cols, right)):
                one = active(corner_in[phase, 2 * side + k])
                both = jnp.logical_and(inside, beside)
                act[at, place : place + 1] = jnp.where(both, one, 0.0)
        for dj in (0, 2):
            start = PAD - 1 + dj
            for r in range(rows + 2):
                shifted[dj, r] = act[r, start : start + cols].astype(jnp.bfloat16)

    def conv(weight, first=0, many=rows):
        result = None
        for di in range(3):
            for dj in range(3):
                tap = 3 * di + dj
                lhs = shifted[dj, first + di : first + di + many].reshape(many * cols, C)
                one = nn_dot(lhs, weight[tap * C : (tap + 1) * C])
                result = one if result is None else result + one
        return result

    with jax.named_scope("stats0"):
        latent_copy.wait()
        put_stats(0, lat_ref[...].astype(jnp.float32).reshape(n, C))
    with jax.named_scope("barrier"):
        pl.semaphore_wait(barrier, total - 1)
    with jax.named_scope("send0"):
        plan = halo_plan(0, lat_ref.at[0], lat_ref.at[rows - 1])
        stats_start(0)
        put_columns(0, lat_ref[...].astype(jnp.float32))
        halo_start(0, plan)
    with jax.named_scope("halo0"):
        halo_finish(0, plan)
    with jax.named_scope("norm0"):
        for copy in vectors:
            copy.wait()
        stats_finish(0, n1g, n1s)
    with jax.named_scope("act0"):
        activate(0, lambda r: lat_ref[r].astype(jnp.float32))
    with jax.named_scope("w0"):
        weights[0].wait()
    with jax.named_scope("conv0"):
        hid[...] = (conv(w1) + c1b[...]).reshape(rows, cols, C)

    with jax.named_scope("stats1"):
        put_stats(1, hid[...].reshape(n, C))
    with jax.named_scope("send1"):
        plan = halo_plan(1, row_out.at[0], row_out.at[1])
        stats_start(1)
        row_out[0] = hid[0].astype(jnp.bfloat16)
        row_out[1] = hid[rows - 1].astype(jnp.bfloat16)
        put_columns(1, hid[...])
        halo_start(1, plan)
    with jax.named_scope("halo1"):
        halo_finish(1, plan)
    with jax.named_scope("norm1"):
        stats_finish(1, n2g, n2s)
    with jax.named_scope("act1"):
        activate(1, lambda r: hid[r])
    with jax.named_scope("conv1"):
        weights[1].wait()

    def residual(r):
        with jax.named_scope("conv1"):
            new = lat_ref[r].astype(jnp.float32) + (conv(w2, r, 1) + c2b[...])
            res[r * cols : (r + 1) * cols] = new.astype(jnp.bfloat16)

    def piece(ref, ch):
        return ref.at[pl.ds(ch * (n // CHUNKS), n // CHUNKS)]

    def z_copy(source, src, way, distance, ch):
        return remote(
            piece(src, ch),
            piece(kv.at[0, source], ch),
            z_send.at[way, distance, ch],
            z_recv.at[source, ch],
            (tile, head + (1 if way else -1) * (distance if distance <= DIRECT else 1)),
        )

    def reachable(way, distance):
        return head + distance < heads if way else head - distance >= 0

    at_end = jnp.logical_or(head == 0, head == heads - 1)

    def straight(fn, opening=None):
        nearer = [(1, ch) for ch in range(CHUNKS)]
        farther = [(d, ch) for d in range(2, min(DIRECT, heads - 1) + 1) for ch in range(CHUNKS)]
        for chosen, order in ((at_end, interleaved(farther, nearer)), (~at_end, farther + nearer)):
            for distance, ch in order:
                for way in (0, 1):
                    present = jnp.logical_and(reachable(way, distance), chosen)
                    if opening is not None:
                        opens = ch == 0 and distance <= 2
                        if opens and distance == 1:
                            alone = ~reachable(way, 2)
                            present = jnp.logical_and(present, alone if opening else ~alone)
                        elif opens != opening:
                            continue

                    @pl.when(present)
                    def _(way=way, distance=distance, ch=ch):
                        fn(z_copy(head, res, way, distance, ch))

    def onward(distance, fn, chunks=tuple(range(CHUNKS))):
        for ch in chunks:
            for way in (0, 1):

                @pl.when(jnp.logical_and(reachable(1 - way, distance), reachable(way, 1)))
                def _(way=way, ch=ch):
                    source = head + (-distance if way else distance)
                    fn(z_copy(source, kv.at[0, source], way, distance + 1, ch))

    def z_arrived(source, distance, way, ch):
        def wait():
            z_copy(source, res, way, 1, ch).wait_recv()

        if heads - 1 > DIRECT:
            passed = jnp.logical_and(distance >= DIRECT, reachable(1 - way, 1))
            pl.when(jnp.logical_not(passed))(wait)
        else:
            wait()

    def c_copy(source, src, ch):
        return remote(
            piece(src, ch),
            piece(kv.at[1, source], ch),
            c_send.at[source, ch],
            c_recv.at[source, ch],
            partner,
        )

    def q_copy(j, part):
        rows_of = pl.ds(0, n // 2) if part == 0 else pl.ds(n // 2, n - n // 2)
        return remote(
            res.at[rows_of],
            qn.at[j, rows_of],
            q_send.at[j, part],
            q_recv.at[j, part],
            (fellow(j), head),
        )

    residual(0)
    straight(lambda copy: copy.start(), True)
    for j in (1, 2):
        if j < half:
            q_copy(j, 0).start()
    for r in range(1, rows):
        residual(r)
    for ch in range(CHUNKS):
        c_copy(head, res, ch).start()
    with jax.named_scope("stats2"):
        put_stats(2, res[...].astype(jnp.float32))
        stats_start(2)

    def pass_on(ch):
        def go(copy):
            copy.wait_recv()
            copy.start()

        with jax.named_scope("relay"):
            for distance in range(DIRECT, heads - 1):
                onward(distance, go, (ch,))

    straight(lambda copy: copy.start(), False)
    for j in (1, 2):
        if j < half:
            q_copy(j, 1).start()

    def q_begin(j, carry):
        for part in range(2):
            q_copy(j, part).start()
        return carry

    lax.fori_loop(3, half, q_begin, 0)
    pass_on(0)
    pass_on(1)
    with jax.named_scope("norm2"):
        stats_finish(2, n3g, n3s)
        for copy in weights[2:]:
            copy.wait()

    def normed(values):
        return normalize(values.astype(jnp.float32)).astype(jnp.bfloat16)

    scale = LOG2E / C**0.5

    def make_query(pair, at, source):
        query = (nn_dot(normed(source), wp[0]) + qb[...]).astype(jnp.bfloat16)
        qp[pair, :, at * n : (at + 1) * n] = (nt_dot(wp[1], query) * scale).astype(jnp.bfloat16)

    def clear(pair):
        top[pair] = jnp.full((1, 2 * n), -jnp.inf, jnp.float32)
        low[pair] = jnp.zeros((1, 2 * n), jnp.float32)
        acc[pair] = jnp.zeros((C, 2 * n), jnp.float32)

    def prepare(core, source, values):
        keys = normed(values)
        kn[source, core] = keys
        kt[source, :, core * n : (core + 1) * n] = jnp.transpose(keys)

    def one_core(core, source):
        return kn.at[source, core], kt.at[source, :, pl.ds(core * n, n)]

    def both_cores(source):
        return kn.at[source], kt.at[source]

    def attend(pair, *blocks):
        query = qp[pair]
        scores = [nn_dot(keys[...].reshape(-1, C), query) for keys, _ in blocks]
        before = top[pair]
        peak = before
        for one in scores:
            peak = jnp.maximum(peak, jnp.max(one, axis=0, keepdims=True))
        fade = jnp.exp2(before - peak)
        sums, values = low[pair] * fade, None
        for one, (_, turned) in zip(scores, blocks):
            expo = jnp.exp2(one - peak)
            sums = sums + jnp.sum(expo, axis=0, keepdims=True)
            part = nn_dot(turned[...], expo.astype(jnp.bfloat16))
            values = part if values is None else values + part
        top[pair] = peak
        low[pair] = sums
        acc[pair] = acc[pair] * fade + values

    def columns(fn, distances, chosen=None):
        for distance in distances:
            for way in (0, 1):
                present = reachable(way, distance)
                if chosen is not None:
                    present = jnp.logical_and(present, chosen)

                @pl.when(present)
                def _(distance=distance, way=way):
                    fn(head + (distance if way else -distance), distance, way)

    far = tuple(range(2, heads))

    with jax.named_scope("query0"):
        clear(0)
        make_query(0, 0, res[...])
        prepare(0, head, res[...])
    with jax.named_scope("q_wait0"):
        for part in range(2):
            q_copy(1, part).wait()
    pass_on(2)
    with jax.named_scope("query1"):
        make_query(0, 1, qn[1])
        for ch in range(CHUNKS):
            c_copy(head, res, ch).wait()
        prepare(1, head, kv[1, head])
    pass_on(3)
    with jax.named_scope("attend_own"):
        attend(0, both_cores(head))

    def begin(source, distance, way):
        with jax.named_scope("z_wait"):
            for ch in range(CHUNKS):
                z_arrived(source, distance, way, ch)
                c_copy(source, kv.at[0, source], ch).start()
        with jax.named_scope("prepare0"):
            prepare(0, source, kv[0, source])

    def second(source):
        with jax.named_scope("c_wait"):
            for ch in range(CHUNKS):
                c_copy(source, kv.at[0, source], ch).wait()
        with jax.named_scope("prepare1"):
            prepare(1, source, kv[1, source])

    def other_pairs(*blocks):
        def one(pair, carry):
            attend(pair, *blocks)
            return carry

        if pairs == 2:
            attend(1, *blocks)
        else:
            lax.fori_loop(1, pairs, one, 0)

    def together(source, distance, way):
        second(source)
        with jax.named_scope("together"):
            other_pairs(both_cores(source))

    def own_pair():
        with jax.named_scope("own_far"):
            attend(0, *[both_cores(lax.rem(head + k, heads)) for k in range(1, heads)])

    columns(begin, (1,), at_end)

    def rest(pair, carry):
        with jax.named_scope("q_wait1"):
            for at in range(2):
                for part in range(2):
                    q_copy(2 * pair + at, part).wait()
        with jax.named_scope("query2"):
            clear(pair)
            for at in range(2):
                make_query(pair, at, qn[2 * pair + at])
        return carry

    lax.fori_loop(1, pairs, rest, 0)
    columns(begin, (2,), ~at_end)
    with jax.named_scope("attend_rest"):
        other_pairs(both_cores(head))
    columns(begin, (2,), at_end)
    columns(together, (1,), at_end)
    columns(together, (2,))

    def apart(*place):
        begin(*place)
        with jax.named_scope("late0"):
            other_pairs(one_core(0, place[0]))
        second(place[0])
        with jax.named_scope("late1"):
            other_pairs(one_core(1, place[0]))

    def two_near(first, last):
        begin(*first)
        with jax.named_scope("late0"):
            other_pairs(one_core(0, first[0]))
        second(first[0])
        begin(*last)
        with jax.named_scope("late01"):
            other_pairs(one_core(1, first[0]), one_core(0, last[0]))
        second(last[0])
        with jax.named_scope("late1"):
            other_pairs(one_core(1, last[0]))

    below, above = (head - 1, 1, 0), (head + 1, 1, 1)
    lower = 2 * head < heads - 1
    pl.when(jnp.logical_and(~at_end, lower))(lambda: two_near(below, above))
    pl.when(jnp.logical_and(~at_end, ~lower))(lambda: two_near(above, below))

    columns(apart, far[1:])

    def both(src, dst, src_level, dst_level, sem, device):
        return [
            remote(src, dst, o_send.at[sem], o_recv.at[sem], device),
            remote(src_level, dst_level, l_send.at[sem], l_recv.at[sem], device),
        ]

    def give_copies(j):
        return both(o_out.at[j], o_in.at[j], l_out.at[j], l_in.at[j], j, (lender(j), head))

    def finish(pair, at, o_to, l_to):
        for part in range(2):
            lanes = slice((2 * at + part) * (n // 2), (2 * at + part + 1) * (n // 2))
            sums = low[pair, :, lanes]
            l_to[2 * pair + at, part] = top[pair, :, lanes] + jnp.log2(sums)
            o_to[2 * pair + at, part] = (acc[pair, :, lanes] * (1.0 / sums)).astype(jnp.bfloat16)

    def column_sent():
        straight(lambda copy: copy.wait_send())
        for distance in range(DIRECT, heads - 1):
            onward(distance, lambda copy: copy.wait_send())

    def fold_weights():
        value_bias = jnp.broadcast_to(vb[...], (8, C)).astype(jnp.bfloat16)
        norm[2:3] = nn_dot(value_bias, wp[3])[:1] + ob[...]
        wp[0] = nn_dot(wp[2], wp[3]).astype(jnp.bfloat16)

    def begin_all(copies):
        for copy in copies:
            copy.start()

    def end_all(copies):
        for copy in copies:
            copy.wait()

    if half == 4:
        def hop(part):
            via = (fellow(2 - part), head)
            return both(
                o_out.at[3, part], u_in.at[part], l_out.at[3, part], ul_in.at[part], part, via
            )

        def direct(j):
            part = 2 - j
            return both(
                o_out.at[j, part],
                o_in.at[j, part],
                l_out.at[j, part],
                l_in.at[j, part],
                1 + j,
                (fellow(j), head),
            )

        def merged(j):
            part = j - 1
            return both(
                m_out.at[part],
                o_in.at[j, part],
                ml_out.at[part],
                l_in.at[j, part],
                3 + j,
                (fellow(j), head),
            )

        def merge(j):
            part = j - 1
            end_all(hop(part))
            mine, theirs = l_out[j, part], ul_in[part]
            level = jnp.maximum(mine, theirs)
            keep, add = jnp.exp2(mine - level), jnp.exp2(theirs - level)
            whole = keep + add
            ml_out[part] = level + jnp.log2(whole)
            values = o_out[j, part].astype(jnp.float32) * (keep / whole)
            values = values + u_in[part].astype(jnp.float32) * (add / whole)
            m_out[part] = values.astype(jnp.bfloat16)
            begin_all(merged(j))

        with jax.named_scope("give"):
            finish(1, 1, o_out, l_out)
            begin_all(hop(0))
            begin_all(hop(1))
            finish(1, 0, o_out, l_out)
            begin_all(direct(2))
        own_pair()
        with jax.named_scope("give1"):
            finish(0, 1, o_out, l_out)
            begin_all(direct(1))
        with jax.named_scope("finish0"):
            finish(0, 0, o_in, l_in)
            column_sent()
            fold_weights()
        with jax.named_scope("merge2"):
            merge(2)
        with jax.named_scope("merge1"):
            merge(1)
        with jax.named_scope("take"):
            for j in (1, 2):
                end_all(direct(j))
                end_all(merged(j))
        parts = 3
    else:

        def give(i, carry):
            pair = pairs - 1 - i
            for at in range(2):
                finish(pair, at, o_out, l_out)
                begin_all(give_copies(2 * pair + at))
            return carry

        def take(j, carry):
            end_all(give_copies(j))
            return carry

        lax.fori_loop(0, pairs - 1, give, 0)
        own_pair()
        finish(0, 1, o_out, l_out)
        begin_all(give_copies(1))
        finish(0, 0, o_in, l_in)
        column_sent()
        fold_weights()
        lax.fori_loop(1, half, take, 0)
        parts = half
    with jax.named_scope("last"):
        sides = []
        for part in range(2):
            peak = l_in[0, part]
            for j in range(1, parts):
                peak = jnp.maximum(peak, l_in[j, part])
            shares = [jnp.exp2(l_in[j, part] - peak) for j in range(parts)]
            whole = shares[0]
            for j in range(1, parts):
                whole = whole + shares[j]
            side = jnp.zeros((C, n // 2), jnp.float32)
            for j in range(parts):
                side = side + (shares[j] / whole) * o_in[j, part].astype(jnp.float32)
            sides.append(side)
        mixed = jnp.concatenate(sides, axis=1)
        mixed = jnp.transpose(mixed.astype(jnp.bfloat16))
        out = nn_dot(mixed, wp[0]) + norm[2:3]
        out_ref[...] = (res[...].astype(jnp.float32) + out).astype(jnp.bfloat16)


def per_device(
    latent,
    norm1_gain,
    norm1_shift,
    conv1_weight,
    conv1_bias,
    norm2_gain,
    norm2_shift,
    conv2_weight,
    conv2_bias,
    norm3_gain,
    norm3_shift,
    query_weight,
    query_bias,
    key_weight,
    value_weight,
    value_bias,
    out_weight,
    out_bias,
):
    rows, cols, _ = latent.shape
    tiles, heads = lax.axis_size("tile"), lax.axis_size("head")
    n = rows * cols
    total = tiles * heads
    half = tiles // 2
    vectors = [
        v.reshape(1, C)
        for v in (
            norm1_gain,
            norm1_shift,
            conv1_bias,
            norm2_gain,
            norm2_shift,
            conv2_bias,
            norm3_gain,
            norm3_shift,
            query_bias,
            value_bias,
            out_bias,
        )
    ]
    matrices = [
        conv1_weight.reshape(9 * C, C),
        conv2_weight.reshape(9 * C, C),
        query_weight,
        key_weight,
        value_weight,
        out_weight,
    ]
    bf16, f32 = jnp.bfloat16, jnp.float32
    dma = pltpu.SemaphoreType.DMA
    out = pl.pallas_call(
        functools.partial(block_kernel, tiles, heads),
        out_shape=pltpu.VMEM((n, C), bf16),
        in_specs=[HBM] * (1 + len(vectors) + len(matrices)),
        out_specs=VMEM,
        scratch_shapes=[
            pltpu.VMEM((rows, cols, C), bf16),
            pltpu.VMEM((len(vectors), 1, C), f32),
            pltpu.VMEM((9 * C, C), bf16),
            pltpu.VMEM((9 * C, C), bf16),
            pltpu.VMEM((4, C, C), bf16),
            pltpu.VMEM((rows + 2, cols + 2 * PAD, C), f32),
            pltpu.VMEM((3, rows + 2, cols, C), bf16),
            pltpu.VMEM((rows, cols, C), f32),
            pltpu.VMEM((2, 2, cols, C), bf16),
            pltpu.VMEM((2, cols, C), bf16),
            pltpu.VMEM((2, 2, rows, 1, C), f32),
            pltpu.VMEM((2, 2, rows, 1, C), f32),
            pltpu.VMEM((2, 4, 1, C), f32),
            pltpu.VMEM((3, 1, LANES), f32),
            pltpu.VMEM((3, total, 1, LANES), f32),
            pltpu.VMEM((8, C), f32),
            pltpu.VMEM((n, C), bf16),
            pltpu.VMEM((2, heads, n, C), bf16),
            pltpu.VMEM((heads, 2, n, C), bf16),
            pltpu.VMEM((heads, C, 2 * n), bf16),
            pltpu.VMEM((half, n, C), bf16),
            pltpu.VMEM((half // 2, C, 2 * n), bf16),
            pltpu.VMEM((half // 2, C, 2 * n), f32),
            pltpu.VMEM((half // 2, 1, 2 * n), f32),
            pltpu.VMEM((half // 2, 1, 2 * n), f32),
            pltpu.VMEM((half, 2, C, n // 2), bf16),
            pltpu.VMEM((half, 2, C, n // 2), bf16),
            pltpu.VMEM((half, 2, 1, n // 2), f32),
            pltpu.VMEM((half, 2, 1, n // 2), f32),
            pltpu.VMEM((2, C, n // 2), bf16),
            pltpu.VMEM((2, 1, n // 2), f32),
            pltpu.VMEM((2, C, n // 2), bf16),
            pltpu.VMEM((2, 1, n // 2), f32),
            dma,
            dma((len(vectors),)),
            dma((len(matrices),)),
            dma((3,)),
            dma((3,)),
            dma((2, 8)),
            dma((2, 8)),
            dma((2, heads, CHUNKS)),
            dma((heads, CHUNKS)),
            dma((heads, CHUNKS)),
            dma((heads, CHUNKS)),
            dma((half, 2)),
            dma((half, 2)),
            dma((half + 2,)),
            dma((half + 2,)),
            dma((half + 2,)),
            dma((half + 2,)),
        ],
        compiler_params=pltpu.CompilerParams(
            collective_id=1, has_side_effects=True, vmem_limit_bytes=VMEM_LIMIT
        ),
        name="middle_block",
    )(latent, *vectors, *matrices)
    return out.reshape(rows, cols, C)


def solution(mesh):
    return jax.shard_map(
        per_device,
        mesh=mesh,
        in_specs=(P("tile", "head", None),) + (P(),) * 17,
        out_specs=P("tile", "head", None),
        check_vma=False,
    )
```
